32 devices in a mesh: rep: 2 (over z, core), dp: 16 (over x, y).
Axes of the slice: x: 4, y: 4, z: 1, core: 2. Of those that a mesh axis runs over, the one named last changes fastest.
The devices are a block of a 4x4x8 slice.
Arguments:
- x: bfloat16 [32, 1024, 1024], P(('rep', 'dp')), parts along dimension 0
- dy: bfloat16 [32, 1024, 1024], P(('rep', 'dp')), parts along dimension 0
- wq: bfloat16 [2, 1024, 1024], P(None, 'dp')
- wk: bfloat16 [2, 1024, 256], P(None, 'dp')
- wv: bfloat16 [2, 1024, 256], P(None, 'dp')
- wo: bfloat16 [2, 1024, 1024], P(None, 'dp')
- w_gate: bfloat16 [2, 1024, 3200], P(None, 'dp')
- w_up: bfloat16 [2, 1024, 3200], P(None, 'dp')
- w_down: bfloat16 [2, 3200, 1024], P(None, 'dp')
- m_wq: float32 [2, 1024, 1024], P(None, 'dp')
- m_wk: float32 [2, 1024, 256], P(None, 'dp')
- m_wv: float32 [2, 1024, 256], P(None, 'dp')
- m_wo: float32 [2, 1024, 1024], P(None, 'dp')
- m_w_gate: float32 [2, 1024, 3200], P(None, 'dp')
- m_w_up: float32 [2, 1024, 3200], P(None, 'dp')
- m_w_down: float32 [2, 3200, 1024], P(None, 'dp')
- v_wq: float32 [2, 1024, 1024], P(None, 'dp')
- v_wk: float32 [2, 1024, 256], P(None, 'dp')
- v_wv: float32 [2, 1024, 256], P(None, 'dp')
- v_wo: float32 [2, 1024, 1024], P(None, 'dp')
- v_w_gate: float32 [2, 1024, 3200], P(None, 'dp')
- v_w_up: float32 [2, 1024, 3200], P(None, 'dp')
- v_w_down: float32 [2, 3200, 1024], P(None, 'dp')
Outputs:
- output 1: bfloat16 [4, 1024, 1024], P('rep', 'dp'), parts along dimension 0
- output 2: bfloat16 [4, 1024, 256], P('rep', 'dp'), parts along dimension 0
- output 3: bfloat16 [4, 1024, 256], P('rep', 'dp'), parts along dimension 0
- output 4: bfloat16 [4, 1024, 1024], P('rep', 'dp'), parts along dimension 0
- output 5: bfloat16 [4, 1024, 3200], P('rep', 'dp'), parts along dimension 0
- output 6: bfloat16 [4, 1024, 3200], P('rep', 'dp'), parts along dimension 0
- output 7: bfloat16 [4, 3200, 1024], P('rep', 'dp'), parts along dimension 0
- output 8: float32 [4, 1024, 1024], P('rep', 'dp'), parts along dimension 0
- output 9: float32 [4, 1024, 256], P('rep', 'dp'), parts along dimension 0
- output 10: float32 [4, 1024, 256], P('rep', 'dp'), parts along dimension 0
- output 11: float32 [4, 1024, 1024], P('rep', 'dp'), parts along dimension 0
- output 12: float32 [4, 1024, 3200], P('rep', 'dp'), parts along dimension 0
- output 13: float32 [4, 1024, 3200], P('rep', 'dp'), parts along dimension 0
- output 14: float32 [4, 3200, 1024], P('rep', 'dp'), parts along dimension 0
- output 15: float32 [4, 1024, 1024], P('rep', 'dp'), parts along dimension 0
- output 16: float32 [4, 1024, 256], P('rep', 'dp'), parts along dimension 0
- output 17: float32 [4, 1024, 256], P('rep', 'dp'), parts along dimension 0
- output 18: float32 [4, 1024, 1024], P('rep', 'dp'), parts along dimension 0
- output 19: float32 [4, 1024, 3200], P('rep', 'dp'), parts along dimension 0
- output 20: float32 [4, 1024, 3200], P('rep', 'dp'), parts along dimension 0
- output 21: float32 [4, 3200, 1024], P('rep', 'dp'), parts along dimension 0
There are 2 independent parts. The reference program is written for one: setup_inputs(seed, part) draws one part's arguments, and reference() takes and returns one part's arrays. A program takes and returns all parts, laid end to end along the dimension named above; an argument that names none is the same for every part.
All inputs are finite; a program needn't handle non-finite values.
Results may differ from the reference program's by a relative error of at most 0.0289.
Values are sent between devices in bfloat16 or wider.
A program may use at most 768 MiB of HBM per device.

```python
import jax
import jax.numpy as jnp
from jax import lax

SEQUENCES = 16
TOKENS = 1024
D = 1024
HEADS = 8
KV_HEADS = 2
HEAD = 128
FF = 3200
LAYERS = 2
THETA = 10000
NAMES = ("wq", "wk", "wv", "wo", "w_gate", "w_up", "w_down")
SHAPES = {
    "wq": (LAYERS, D, HEADS * HEAD),
    "wk": (LAYERS, D, KV_HEADS * HEAD),
    "wv": (LAYERS, D, KV_HEADS * HEAD),
    "wo": (LAYERS, HEADS * HEAD, D),
    "w_gate": (LAYERS, D, FF),
    "w_up": (LAYERS, D, FF),
    "w_down": (LAYERS, FF, D),
}


def bump(key, n, height):
    away = (jnp.arange(n, dtype=jnp.int32) - jax.random.randint(key, (), 0, n, jnp.int32)) % n
    return jnp.where(away < n // 8, height, 1.0)


def together(key, own, strength):
    shared = jax.random.normal(key, own.shape[1:], jnp.float32)
    return (own + strength * shared) * lax.rsqrt(1 + strength * strength)


def setup_inputs(seed: int = 0, part: int = 0) -> dict:
    kx, kdy, ka, kb, kz, kf, kh, kl, *keys = jax.random.split(jax.random.key(seed), 8 + 3 * len(NAMES))
    kx, kdy, ka, kb = (jax.random.fold_in(k, part) for k in (kx, kdy, ka, kb))
    kw, km, kv = (keys[i::3] for i in range(3))
    shape = (SEQUENCES, TOKENS, D)
    much_x, much_dy = jax.random.uniform(kz, (2,), jnp.float32, 0.0, 1.0)
    loud = 2.0 ** jax.random.uniform(jax.random.fold_in(kz, 1), (), jnp.float32, -1.0, 2.0)
    layers = 2.0 ** jax.random.uniform(kl, (LAYERS, 1, 1), jnp.float32, -1.0, 1.0)
    times = {"wq": 1.0, "wk": 1.0, "wv": 2.0, "wo": layers, "w_gate": 1.0, "w_up": bump(kh, FF, 4.0), "w_down": layers}
    x = together(ka, jax.random.normal(kx, shape, jnp.float32), much_x) * bump(kf, D, 4.0)
    dy = together(kb, jax.random.normal(kdy, shape, jnp.float32), much_dy)
    drawn = {"x": x.astype(jnp.bfloat16), "dy": (loud * dy * (SEQUENCES * TOKENS) ** -0.5).astype(jnp.bfloat16)}
    for key, name in zip(kw, NAMES, strict=True):
        drawn[name] = (jax.random.normal(key, SHAPES[name], jnp.float32) * SHAPES[name][1] ** -0.5 * times[name]).astype(jnp.bfloat16)
    for key, name in zip(km, NAMES, strict=True):
        drawn[f"m_{name}"] = 0.1 * jax.random.normal(key, SHAPES[name], jnp.float32)
    for key, name in zip(kv, NAMES, strict=True):
        drawn[f"v_{name}"] = jax.random.uniform(key, SHAPES[name], jnp.float32, 0.02, 0.06)
    return drawn


def matmul(a, w):
    return jnp.dot(a, w, preferred_element_type=jnp.float32).astype(jnp.bfloat16)


def normed(h):
    wide = h.astype(jnp.float32)
    scale = lax.rsqrt(jnp.mean(wide**2, -1, keepdims=True) + 1e-6)
    return (wide * scale).astype(jnp.bfloat16)


def turned(t, theta):
    half = t.shape[-1] // 2
    angle = jnp.arange(t.shape[0], dtype=jnp.float32)[:, None] * theta ** (-jnp.arange(half, dtype=jnp.float32) / half)
    cos, sin = jnp.cos(angle)[:, None], jnp.sin(angle)[:, None]
    a, b = t[..., :half].astype(jnp.float32), t[..., half:].astype(jnp.float32)
    return jnp.concatenate([a * cos - b * sin, b * cos + a * sin], -1).astype(jnp.bfloat16)


def seen_by(q, k, v):
    tokens, kv = q.shape[0], k.shape[1]
    q = q.reshape(tokens, kv, -1, q.shape[-1])
    scores = jnp.einsum("tgsd,ugd->gstu", q.astype(jnp.float32), k.astype(jnp.float32)) * q.shape[-1] ** -0.5
    place = jnp.arange(tokens)
    weights = jax.nn.softmax(jnp.where(place[:, None] >= place, scores, -jnp.inf), -1).astype(jnp.bfloat16)
    return jnp.einsum("gstu,ugd->tgsd", weights.astype(jnp.float32), v.astype(jnp.float32)).astype(jnp.bfloat16).reshape(tokens, -1)


def layer(h, w):
    a = normed(h)
    q, k = (turned(matmul(a, w[name]).reshape(h.shape[0], -1, HEAD), THETA) for name in ("wq", "wk"))
    h = h + matmul(seen_by(q, k, matmul(a, w["wv"]).reshape(h.shape[0], -1, HEAD)), w["wo"])
    b = normed(h)
    gate = jnp.dot(b, w["w_gate"], preferred_element_type=jnp.float32)
    up = jnp.dot(b, w["w_up"], preferred_element_type=jnp.float32)
    return h + matmul((jax.nn.silu(gate) * up).astype(jnp.bfloat16), w["w_down"])


def adamw(w, m, v, g):
    m = 0.9 * m + 0.1 * g
    v = 0.95 * v + 0.05 * g * g
    step = m * lax.rsqrt(v + 1e-8) + 0.1 * w
    return (w - 0.02 * step).astype(jnp.bfloat16), m, v


def clipped(gradients, sum_of_squares, count):
    factor = jnp.minimum(1.0, 0.5 * lax.rsqrt(sum_of_squares / count + 1e-30))
    return [g * factor for g in gradients]


def stack(weights, h):
    return lax.scan(lambda h, w: (layer(h, w), None), h, weights)[0]


def reference(x, dy, wq, wk, wv, wo, w_gate, w_up, w_down, m_wq, m_wk, m_wv, m_wo, m_w_gate, m_w_up, m_w_down, v_wq, v_wk, v_wv, v_wo, v_w_gate, v_w_up, v_w_down):
    weights = dict(zip(NAMES, (wq, wk, wv, wo, w_gate, w_up, w_down), strict=True))

    def take(so_far, sequence):
        h, by_y = sequence
        _, back = jax.vjp(stack, weights, h)
        by_weights, by_h = back(by_y)
        return jax.tree.map(lambda total, term: total + term.astype(jnp.float32), so_far, by_weights), by_h

    none_yet = {name: jnp.zeros(w.shape, jnp.float32) for name, w in weights.items()}
    by_weights, by_x = lax.scan(take, none_yet, (x, dy))
    gradients = [by_weights[name].astype(jnp.bfloat16).astype(jnp.float32) for name in NAMES]
    gradients = clipped(gradients, sum(jnp.sum(g * g) for g in gradients), sum(g.size for g in gradients))
    first = (m_wq, m_wk, m_wv, m_wo, m_w_gate, m_w_up, m_w_down)
    second = (v_wq, v_wk, v_wv, v_wo, v_w_gate, v_w_up, v_w_down)
    new = [adamw(weights[name].astype(jnp.float32), m, v, g) for name, m, v, g in zip(NAMES, first, second, gradients, strict=True)]
    return tuple(one[which] for which in range(3) for one in new)
```

```python
import functools

import jax
import jax.numpy as jnp
from jax import lax
from jax.experimental import pallas as pl
from jax.experimental.pallas import tpu as pltpu
from jax.sharding import PartitionSpec as P

MESH = pl.DeviceIdType.MESH

RINGS = 4

def where_at(cycle, q, side):
    a, j = q // side, q % side
    b = (j - a + side) % side
    return a * side + b if cycle == 0 else b * side + a

class Ring:
    def __init__(self, n, rep_pairs=True):
        self.n = n
        self.side = next(s for s in range(1, n + 1) if s * s == n)
        me = lax.axis_index("dp")
        x, y = me // self.side, me % self.side
        self.me = me
        s = self.side
        self.pos = [x * s + (x + y) % s, y * s + (x + y) % s]
        self.rep = lax.axis_index("rep")
        self.core = self.rep % 2
        self.sib = self.rep + 1 - 2 * self.core
    def cyc(self, k): return k // 2
    def sgn(self, k): return 1 - 2 * (k % 2)
    def at(self, k, off):
        q = (self.pos[self.cyc(k)] + self.sgn(k) * off + self.n) % self.n if not isinstance(off, int) or off else self.pos[self.cyc(k)]
        return where_at(self.cyc(k), q, self.side)

def region(kind, ref, shape, k, block, core):
    r, c = shape
    if kind == "rows":
        rows = r // RINGS
        return ref.at[pl.ds(pl.multiple_of(block * r + k * rows, rows), rows), pl.ds(pl.multiple_of(core * (c // 2), 128), c // 2)]
    cols = c // (2 * RINGS)
    return ref.at[pl.ds(pl.multiple_of(block * r, 8), r), pl.ds(pl.multiple_of((core * RINGS + k) * cols, 128), cols)]

def gather_body(n, kinds, shapes, *refs):
    m = len(kinds)
    shards, outs = refs[:m], refs[m:2 * m]
    recv, send, dsend, drecv, lsem = refs[2 * m:]
    R = Ring(n)
    bar = pltpu.get_barrier_semaphore()
    for k in range(RINGS):
        pl.semaphore_signal(bar, inc=1, device_id={"dp": R.at(k, 1)}, device_id_type=pl.DeviceIdType.MESH)
    pl.semaphore_signal(bar, inc=1, device_id={"rep": R.sib}, device_id_type=pl.DeviceIdType.MESH)
    pl.semaphore_wait(bar, RINGS + 1)
    nxt = [R.at(k, 1) for k in range(RINGS)]

    def hop(p, k, t, src, block):
        return pltpu.make_async_remote_copy(src_ref=src, dst_ref=region(kinds[p], outs[p], shapes[p], k, block, R.core), send_sem=send.at[p],
                                            recv_sem=recv.at[p, k, t], device_id={"dp": nxt[k]}, device_id_type=pl.DeviceIdType.MESH)
    def over(p, k, block):
        r = region(kinds[p], outs[p], shapes[p], k, block, R.core)
        return pltpu.make_async_remote_copy(src_ref=r, dst_ref=r, send_sem=dsend.at[p], recv_sem=drecv.at[p], device_id={"rep": R.sib}, device_id_type=pl.DeviceIdType.MESH)
    for p in range(m):
        for k in range(RINGS):
            hop(p, k, 0, region(kinds[p], shards[p], shapes[p], k, 0, R.core), R.me).start()
        r = shapes[p][0]
        pltpu.make_async_copy(shards[p], outs[p].at[pl.ds(pl.multiple_of(R.me * r, 8), r), :], lsem.at[p]).start()

    def step(t, _):
        for p in range(m):
            for k in range(RINGS):
                block = R.at(k, -t)
                hop(p, k, t - 1, region(kinds[p], outs[p], shapes[p], k, block, R.core), block).wait_recv()
                @pl.when(t < n - 1)
                def _():
                    hop(p, k, t, region(kinds[p], outs[p], shapes[p], k, block, R.core), block).start()
                over(p, k, block).start()
        return None
    lax.fori_loop(1, n, step, None)
    for p in range(m):
        r, c = shapes[p]
        pltpu.make_async_copy(shards[p], outs[p].at[pl.ds(pl.multiple_of(R.me * r, 8), r), :], lsem.at[p]).wait()
        every = outs[p].at[pl.ds(0, (n - 1) * r), pl.ds(0, c // 2)]
        full = pltpu.make_async_remote_copy(src_ref=every, dst_ref=every, send_sem=send.at[p], recv_sem=drecv.at[p], device_id={"rep": R.sib}, device_id_type=pl.DeviceIdType.MESH)
        full.wait_send()
        full.wait_recv()
        pltpu.make_async_remote_copy(src_ref=every, dst_ref=every, send_sem=dsend.at[p], recv_sem=drecv.at[p], device_id={"rep": R.sib}, device_id_type=pl.DeviceIdType.MESH).wait_send()

def gather(n, kinds, shards, cid):
    shapes = [s.shape for s in shards]
    m = len(shards)
    return pl.pallas_call(
        functools.partial(gather_body, n, kinds, shapes),
        out_shape=[jax.ShapeDtypeStruct((s[0] * n, s[1]), jnp.bfloat16) for s in shapes],
        in_specs=[pl.BlockSpec(memory_space=pltpu.VMEM)] * m,
        out_specs=[pl.BlockSpec(memory_space=pl.ANY)] * m,
        scratch_shapes=[pltpu.SemaphoreType.DMA((m, RINGS, n)), pltpu.SemaphoreType.DMA((m,)), pltpu.SemaphoreType.DMA((m,)), pltpu.SemaphoreType.DMA((m,)),
                        pltpu.SemaphoreType.DMA((m,))],
        compiler_params=pltpu.CompilerParams(collective_id=cid, has_side_effects=True, vmem_limit_bytes=60*2**20),
        name=f"gather{cid}",
    )(*shards)

BF, F32 = jnp.bfloat16, jnp.float32

LOG2E = 1.4426950408889634
NEG = -1e30
HEAD = 128
ROWS = 256
VMEM_LIMIT = 60 * 2**20


def dot(a, b, ca, cb):
    return lax.dot_general(a, b, (((ca,), (cb,)), ((), ())), preferred_element_type=F32)


def nn(a, b):
    return dot(a, b, 1, 0)


def nt(a, b):
    return dot(a, b, 1, 1)


def row(i):
    return i, 0


def col(j):
    return 0, j


def whole(*_):
    return 0, 0


def call(body, grid, ins, outs, scratch=(), flops=0, nbytes=0, name=None):
    spec = lambda block, at: pl.BlockSpec(memory_space=pltpu.VMEM) if block is None else pl.BlockSpec(block, at)
    return pl.pallas_call(
        body, grid=grid, name=name,
        in_specs=[spec(b, at) for _, b, at in ins],
        out_specs=[spec(b, at) for _, _, b, at in outs],
        out_shape=[jax.ShapeDtypeStruct(s, d) for s, d, _, _ in outs],
        scratch_shapes=list(scratch),
        compiler_params=pltpu.CompilerParams(dimension_semantics=("arbitrary",) * len(grid), vmem_limit_bytes=VMEM_LIMIT),
        cost_estimate=pl.CostEstimate(flops=flops, bytes_accessed=nbytes, transcendentals=0),
    )(*[a for a, _, _ in ins])


def unit(h):
    return lax.rsqrt(jnp.mean(h * h, -1, keepdims=True) + 1e-6)


def normed_(h):
    w = h.astype(F32)
    return (w * unit(w)).astype(BF)


def norm_back(h, d):
    w = h.astype(F32)
    s = unit(w)
    return s * d - w * (s * s * s * jnp.mean(w * d, -1, keepdims=True))


def rotary(tokens):
    half = HEAD // 2
    angle = jnp.arange(tokens, dtype=F32)[:, None] * 10000 ** (-jnp.arange(half, dtype=F32) / half)
    c, s = jnp.cos(angle), jnp.sin(angle)
    return jnp.concatenate([c, c], 1), jnp.concatenate([-s, s], 1)


def qkv_body(h_ref, w_ref, c_ref, s_ref, a_ref, o_ref, *, turned):
    a = normed_(h_ref[...])
    a_ref[...] = a
    r = nn(a, w_ref[...]).astype(BF)
    c, s = c_ref[...], s_ref[...]
    for n in range(r.shape[1] // HEAD):
        x = r[:, n * HEAD:(n + 1) * HEAD]
        if n < turned:
            f = x.astype(F32)
            x = (f * c + pltpu.roll(f, HEAD // 2, 1) * s).astype(BF)
        o_ref[:, n * HEAD:(n + 1) * HEAD] = x


def qkv(h, w, cos, sin, kv):
    t, d = h.shape
    n = w.shape[1]
    return call(functools.partial(qkv_body, turned=n // HEAD - kv), (t // ROWS,),
                [(h, (ROWS, d), row), (w, (d, n), whole), (cos, (ROWS, HEAD), row), (sin, (ROWS, HEAD), row)],
                [((t, d), BF, (ROWS, d), row), ((t, n), BF, (ROWS, n), row)], flops=2 * t * d * n, nbytes=2 * (2 * t * d + d * n + t * n), name="qkv")


def out_body(h_ref, x_ref, w_ref, m_ref, b_ref):
    m = h_ref[...] + nn(x_ref[...], w_ref[...]).astype(BF)
    m_ref[...] = m
    b_ref[...] = normed_(m)


def out_proj(h, o, w):
    t, d = h.shape
    k = o.shape[1]
    return call(out_body, (t // ROWS,), [(h, (ROWS, d), row), (o, (ROWS, k), row), (w, (k, d), whole)],
                [((t, d), BF, (ROWS, d), row), ((t, d), BF, (ROWS, d), row)], flops=2 * t * d * k, nbytes=2 * (4 * t * d + d * k), name="out_proj")


def gu_body(b_ref, w_ref, g_ref, m_ref):
    half = m_ref.shape[1]

    def rows(i, _):
        at = pl.ds(pl.multiple_of(i * ROWS, ROWS), ROWS)
        r = nn(b_ref[at, :], w_ref[...])
        g_ref[at, :] = r
        g, u = r[:, :half], r[:, half:]
        m_ref[at, :] = (g * jax.nn.sigmoid(g) * u).astype(BF)
    lax.fori_loop(0, b_ref.shape[0] // ROWS, rows, None)


def gate_up(b, w, parts):
    t, d = b.shape
    n = w.shape[1]
    return call(gu_body, (parts,), [(b, (t, d), whole), (w, (d, n // parts), col)],
                [((t, n), F32, (t, n // parts), col), ((t, n // 2), BF, (t, n // 2 // parts), col)], flops=2 * t * d * n, nbytes=2 * (t * d + d * n + t * n * 5 // 2), name="gate_up")


def down_body(h_ref, m_ref, w_ref, o_ref):
    o_ref[...] = h_ref[...] + nn(m_ref[...], w_ref[...]).astype(BF)


def down(h, mid, w):
    t, d = h.shape
    f = mid.shape[1]
    return call(down_body, (t // ROWS,), [(h, (ROWS, d), row), (mid, (ROWS, f), row), (w, (f, d), whole)],
                [((t, d), BF, (ROWS, d), row)], flops=2 * t * d * f, nbytes=2 * (2 * t * d + d * f + t * f), name="down")[0]


STRIP = 512


def fwd_body(q_ref, k_ref, v_ref, o_ref, lse_ref, top_s, mix_s, *, scale, bk):
    bq, g = q_ref.shape[0], q_ref.shape[1] // HEAD
    iq = pl.program_id(1)
    e = scale * LOG2E
    top_s[...] = jnp.full(top_s.shape, NEG, F32)
    mix_s[...] = jnp.zeros(mix_s.shape, F32)
    ones = jnp.ones((8, bk), BF)

    def block(j, masked):
        here = pl.ds(pl.multiple_of(j * bk, bk), bk)
        k = k_ref[here, :]
        scores = [nt(k, q_ref[:, n * HEAD:(n + 1) * HEAD]) for n in range(g)]
        values = jnp.concatenate([v_ref[here, :].T, ones], axis=0)
        if masked:
            ok = (lax.broadcasted_iota(jnp.int32, (bk, bq), 1) + iq * bq) >= (lax.broadcasted_iota(jnp.int32, (bk, bq), 0) + j * bk)
        weights, keeps = [], []
        for n, s in enumerate(scores):
            if masked:
                s = jnp.where(ok, s, 2 * NEG)
            old = top_s[n:n + 1, :]
            top = jnp.maximum(old, s.max(axis=0, keepdims=True))
            top_s[n:n + 1, :] = top
            weights.append(jnp.exp2((s - top) * e).astype(BF))
            keeps.append(jnp.exp2((old - top) * e))
        for n in range(g):
            mix_s[n] = mix_s[n] * keeps[n] + nn(values, weights[n])

    full = (iq * bq) // bk
    lax.fori_loop(0, full, lambda j, _: block(j, False), None)
    lax.fori_loop(full, (iq * bq + bq + bk - 1) // bk, lambda j, _: block(j, True), None)
    for n in range(g):
        total = mix_s[n, HEAD:HEAD + 1, :]
        o_ref[:, n * HEAD:(n + 1) * HEAD] = (mix_s[n, :HEAD, :] * (1 / total)).T.astype(BF)
        lse_ref[0, n:n + 1, :] = top_s[n:n + 1, :] * scale + jnp.log(total)


def attend(qkv, kv, bq=512, bk=256):
    t, n = qkv.shape
    heads = n // HEAD - 2 * kv
    g = heads // kv
    scale = HEAD ** -0.5
    return call(functools.partial(fwd_body, scale=scale, bk=bk), (kv, t // bq),
                [(qkv, (bq, g * HEAD), lambda c, i: (i, c)), (qkv, (t, HEAD), lambda c, i: (0, heads + c)), (qkv, (t, HEAD), lambda c, i: (0, heads + kv + c))],
                [((t, heads * HEAD), BF, (bq, g * HEAD), lambda c, i: (i, c)), ((kv, g, t), F32, (1, g, bq), lambda c, i: (c, 0, i))],
                [pltpu.VMEM((8, bq), F32), pltpu.VMEM((g, HEAD + 8, bq), F32)], flops=2 * t * t * heads * HEAD, nbytes=2 * t * n, name="attend")


def bwd_body(q_ref, k_ref, v_ref, do_ref, lse_ref, delta_ref, c_ref, s_ref, cq_ref, sq_ref, dq_ref, dk_ref, dv_ref, dq_s, dk_s, dv_s, *, scale, bk):
    bq, g = q_ref.shape[0], q_ref.shape[1] // HEAD
    iq = pl.program_id(1)
    e = scale * LOG2E

    @pl.when(iq == 0)
    def _():
        dk_s[...] = jnp.zeros_like(dk_s)
        dv_s[...] = jnp.zeros_like(dv_s)
    dq_s[...] = jnp.zeros_like(dq_s)

    def block(j, masked):
        here = pl.ds(pl.multiple_of(j * bk, bk), bk)
        k, v = k_ref[here, :], v_ref[here, :]
        kt = k.T
        qs = [q_ref[:, n * HEAD:(n + 1) * HEAD] for n in range(g)]
        dos = [do_ref[:, n * HEAD:(n + 1) * HEAD] for n in range(g)]
        scores = [nt(k, x) for x in qs]
        dps = [nt(v, x) for x in dos]
        if masked:
            ok = (lax.broadcasted_iota(jnp.int32, (bk, bq), 1) + iq * bq) >= (lax.broadcasted_iota(jnp.int32, (bk, bq), 0) + j * bk)
        for n in range(g):
            p = jnp.exp2(scores[n] * e - lse_ref[0, n:n + 1, :] * LOG2E)
            if masked:
                p = jnp.where(ok, p, 0.0)
            ds = (p * (dps[n] - delta_ref[0, n:n + 1, :])).astype(BF)
            dv_s[here, :] += nn(p.astype(BF), dos[n])
            dk_s[here, :] += nn(ds, qs[n])
            dq_s[n] += nn(kt, ds)

    full = (iq * bq) // bk
    lax.fori_loop(0, full, lambda j, _: block(j, False), None)
    lax.fori_loop(full, (iq * bq + bq + bk - 1) // bk, lambda j, _: block(j, True), None)

    def back(d, c, s):
        d = d.astype(BF).astype(F32)
        return (d * c - pltpu.roll(d, HEAD // 2, 1) * s).astype(BF)
    for n in range(g):
        dq_ref[:, n * HEAD:(n + 1) * HEAD] = back((dq_s[n] * scale).T, cq_ref[...], sq_ref[...])

    @pl.when(iq == pl.num_programs(1) - 1)
    def _():
        dk_ref[...] = back(dk_s[...] * scale, c_ref[...], s_ref[...])
        dv_ref[...] = dv_s[...].astype(BF)


def attend_back(qkv, do, lse, delta, cos, sin, kv, bq=512, bk=256):
    t, n = qkv.shape
    heads = n // HEAD - 2 * kv
    g = heads // kv
    scale = HEAD ** -0.5
    qs, ks = (lambda c, i: (i, c)), (lambda c, i: (0, c))
    stat = lambda c, i: (c, 0, i)
    mine = lambda c, i: row(i)
    return call(functools.partial(bwd_body, scale=scale, bk=bk), (kv, t // bq),
                [(qkv, (bq, g * HEAD), qs), (qkv, (t, HEAD), lambda c, i: (0, heads + c)), (qkv, (t, HEAD), lambda c, i: (0, heads + kv + c)),
                 (do, (bq, g * HEAD), qs), (lse, (1, g, bq), stat), (delta, (1, g, bq), stat), (cos, (t, HEAD), whole), (sin, (t, HEAD), whole),
                 (cos, (bq, HEAD), mine), (sin, (bq, HEAD), mine)],
                [((t, heads * HEAD), BF, (bq, g * HEAD), qs), ((t, kv * HEAD), BF, (t, HEAD), ks), ((t, kv * HEAD), BF, (t, HEAD), ks)],
                [pltpu.VMEM((g, HEAD, bq), F32), pltpu.VMEM((t, HEAD), F32), pltpu.VMEM((t, HEAD), F32)], flops=5 * t * t * heads * HEAD, nbytes=6 * t * n, name="attend_back")


def dgu_body(dy_ref, w_ref, g_ref, dg_ref, dw_ref, mid_s):
    half = mid_s.shape[1]

    def rows(i, _):
        at = pl.ds(pl.multiple_of(i * ROWS, ROWS), ROWS)
        d = nt(dy_ref[at, :], w_ref[...]).astype(BF).astype(F32)
        g, u = g_ref[at, :half], g_ref[at, half:]
        s = jax.nn.sigmoid(g)
        silu = g * s
        mid_s[at, :] = (silu * u).astype(BF)
        dg_ref[at, half:] = (d * silu).astype(BF)
        dg_ref[at, :half] = (d * u * (s + silu * (1 - s))).astype(BF)
    lax.fori_loop(0, dy_ref.shape[0] // ROWS, rows, None)
    dw_ref[...] = dot(mid_s[...], dy_ref[...], 0, 0).astype(BF)


def dgu(dy, wd, gu, parts):
    t, d = dy.shape
    f = wd.shape[0]
    c = f // parts
    return call(dgu_body, (parts,), [(dy, (t, d), whole), (wd, (c, d), row), (gu, (t, 2 * c), col)],
                [((t, 2 * f), BF, (t, 2 * c), col), ((f, d), BF, (c, d), row)],
                [pltpu.VMEM((t, c), BF)], flops=4 * t * d * f, nbytes=t * f * 12, name="dgu")


def dw_body(a_ref, d_ref, o_ref, at_s):
    @pl.when(pl.program_id(0) == 0)
    def _():
        at_s[...] = a_ref[...].T

    def rows(i, _):
        at = pl.ds(pl.multiple_of(i * ROWS, ROWS), ROWS)
        o_ref[at, :] = nn(at_s[at, :], d_ref[...]).astype(BF)
    lax.fori_loop(0, at_s.shape[0] // ROWS, rows, None)


def dw(a, d, parts, name="dw"):
    t, m = a.shape
    n = d.shape[1]
    return call(dw_body, (parts,), [(a, (t, m), whole), (d, (t, n // parts), col)],
                [((m, n), BF, (m, n // parts), col)], [pltpu.VMEM((m, t), BF)], flops=2 * t * m * n, nbytes=2 * (t * m + t * n + m * n), name=name)[0]


def db_body(dg_ref, w_ref, dy_ref, h_ref, o_ref, acc):
    j = pl.program_id(0)
    last = pl.num_programs(0) - 1

    def rows(i, _):
        at = pl.ds(pl.multiple_of(i * ROWS, ROWS), ROWS)
        r = nt(dg_ref[at, :], w_ref[...])

        @pl.when(j == 0)
        def _():
            acc[at, :] = r

        @pl.when((j > 0) & (j < last))
        def _():
            acc[at, :] += r

        @pl.when(j == last)
        def _():
            d = (acc[at, :] + r).astype(BF).astype(F32)
            o_ref[at, :] = dy_ref[at, :] + norm_back(h_ref[at, :], d).astype(BF)
    lax.fori_loop(0, dy_ref.shape[0] // ROWS, rows, None)


def db(dgu, wgu, dy, h, parts):
    t, d = dy.shape
    n = dgu.shape[1]
    return call(db_body, (parts,), [(dgu, (t, n // parts), col), (wgu, (d, n // parts), col), (dy, (t, d), whole), (h, (t, d), whole)],
                [((t, d), BF, (t, d), whole)], [pltpu.VMEM((t, d), F32)], flops=2 * t * d * n, nbytes=2 * (t * n + d * n + 3 * t * d), name="db")[0]


def do_body(d_ref, w_ref, o_ref, do_ref, delta_ref):
    r = nt(d_ref[...], w_ref[...]).astype(BF)
    do_ref[...] = r
    kv, g = delta_ref.shape[:2]
    for n in range(kv * g):
        cols = slice(n * HEAD, (n + 1) * HEAD)
        x = r[:, cols].astype(F32) * o_ref[:, cols].astype(F32)
        delta_ref[n // g, n % g:n % g + 1, :] = jnp.sum(x.T, axis=0, keepdims=True)


def do_delta(d, wo, o, kv):
    t, n = d.shape
    k = o.shape[1]
    g = k // HEAD // kv
    return call(do_body, (t // ROWS,), [(d, (ROWS, n), row), (wo, (k, n), whole), (o, (ROWS, k), row)],
                [((t, k), BF, (ROWS, k), row), ((kv, g, t), F32, (kv, g, ROWS), lambda i: (0, 0, i))], flops=2 * t * n * k, nbytes=2 * (3 * t * k + n * k), name="do_delta")


def da_body(dq_ref, dk_ref, dv_ref, w_ref, d_ref, h_ref, o_ref):
    n, m = dq_ref.shape[1], dk_ref.shape[1]
    r = nt(dq_ref[...], w_ref[:, :n]) + nt(dk_ref[...], w_ref[:, n:n + m]) + nt(dv_ref[...], w_ref[:, n + m:])
    o_ref[...] = d_ref[...] + norm_back(h_ref[...], r.astype(BF).astype(F32)).astype(BF)


def da(dq, dk, dv, w, d, h):
    t, n = d.shape
    blk = lambda x: (x, (ROWS, x.shape[1]), row)
    return call(da_body, (t // ROWS,), [blk(dq), blk(dk), blk(dv), (w, w.shape, whole), blk(d), blk(h)],
                [((t, n), BF, (ROWS, n), row)], flops=2 * t * n * w.shape[1], nbytes=2 * (5 * t * n + w.size), name="da")[0]


def dqkv_body(a_ref, dq_ref, dk_ref, dv_ref, o_ref):
    at = a_ref[...].T
    n, m = dq_ref.shape[1], dk_ref.shape[1]
    o_ref[:, :n] = nn(at, dq_ref[...]).astype(BF)
    o_ref[:, n:n + m] = nn(at, dk_ref[...]).astype(BF)
    o_ref[:, n + m:] = nn(at, dv_ref[...]).astype(BF)


def dqkv(a, dq, dk, dv):
    t, d = a.shape
    n = dq.shape[1] + 2 * dk.shape[1]
    return call(dqkv_body, (d // ROWS,), [(a, (t, ROWS), col), (dq, dq.shape, whole), (dk, dk.shape, whole), (dv, dv.shape, whole)],
                [((d, n), BF, (ROWS, n), row)], flops=2 * t * d * n, nbytes=2 * (t * d + t * n + d * n), name="dqkv")[0]


PARTS = 5


def mixed(g, u):
    r = g.shape[0]
    return jnp.concatenate([g.reshape(r, PARTS, -1), u.reshape(r, PARTS, -1)], 2).reshape(r, -1)


def unmixed(m):
    r = m.shape[0]
    m = m.reshape(r, PARTS, 2, -1)
    return m[:, :, 0].reshape(r, -1), m[:, :, 1].reshape(r, -1)


def forward(h, w, cos, sin, kv=2):
    a, x = qkv(h, w[0], cos, sin, kv)
    o, lse = attend(x, kv)
    m, b = out_proj(h, o, w[1])
    gu, mid = gate_up(b, w[2], PARTS)
    return down(m, mid, w[3]), (h, a, x, o, lse, m, b, gu)


def backward(dy, w, kept, cos, sin, need, kv=2):
    h, a, x, o, lse, m, b, gu = kept
    dg, dwd = dgu(dy, w[3], gu, PARTS)
    dwgu = dw(b, dg, PARTS, "dwgu")
    dm = db(dg, w[2], dy, m, PARTS)
    do, delta = do_delta(dm, w[1], o, kv)
    dwo = dw(o, dm, 2, "dwo")
    dq, dk, dv = attend_back(x, do, lse, delta, cos, sin, kv)
    dwqkv = dqkv(a, dq, dk, dv)
    dh = da(dq, dk, dv, w[0], dm, h) if need else None
    return (dwqkv, dwo, dwgu, dwd), dh


class Piece:
    def __init__(self, kind, shape, n, lo=0, hi=None):
        self.kind, self.n = kind, n
        self.block = shape[0] // n
        self.lo, self.hi = lo, shape[1] if hi is None else hi
        self.shape = (self.block // RINGS, self.hi - self.lo) if kind == "rows" else (self.block, (self.hi - self.lo) // RINGS)

    def rows_at(self, k, block):
        r, c = self.shape
        if self.kind == "rows":
            return pl.ds(pl.multiple_of(block * self.block + k * r, 16), r), pl.ds(self.lo, c)
        return pl.ds(pl.multiple_of(block * self.block, 8), r), pl.ds(self.lo + k * c, c)

    def own(self, k):
        r, c = self.shape
        return (pl.ds(k * r, r), pl.ds(self.lo, c)) if self.kind == "rows" else (pl.ds(0, r), pl.ds(self.lo + k * c, c))

    def scratch(self):
        n = self.n
        return [pltpu.VMEM((n - 1, RINGS) + self.shape, BF), pltpu.VMEM((2, RINGS) + self.shape, BF), pltpu.SemaphoreType.DMA((n - 1, RINGS)),
                pltpu.SemaphoreType.DMA, pltpu.SemaphoreType.DMA((2, RINGS)), pltpu.SemaphoreType.DMA, pltpu.SemaphoreType.DMA]


def tiles(x):
    r, c = x.shape
    return sum(x[a : a + 8, b : b + 128] for a in range(0, r, 8) for b in range(0, c, 128))


class Scatter:
    def __init__(self, R, piece, grad, out, squares, scratch):
        self.R, self.p, self.grad, self.out, self.squares = R, piece, grad, out, squares
        self.slot, self.loc, self.recv, self.send, self.lsem, self.osem, self.fsem = scratch
        self.next = [R.at(k, 1) for k in range(RINGS)]

    def chunk(self, k, t):
        return self.grad.at[self.p.rows_at(k, self.R.at(k, -1 - t))]

    def load(self, k, t):
        s = lax.rem(t, 2) if not isinstance(t, int) else t % 2
        return pltpu.make_async_copy(self.chunk(k, t), self.loc.at[s, k], self.lsem.at[s, k])

    def hop(self, k, t, src):
        return pltpu.make_async_remote_copy(src_ref=src, dst_ref=self.slot.at[t, k], send_sem=self.send, recv_sem=self.recv.at[t, k],
                                            device_id={"dp": self.next[k]}, device_id_type=MESH)

    def first(self):
        for k in range(RINGS):
            pltpu.make_async_remote_copy(src_ref=self.chunk(k, 0), dst_ref=self.slot.at[0, k], send_sem=self.fsem, recv_sem=self.recv.at[0, k],
                                         device_id={"dp": self.next[k]}, device_id_type=MESH).start()
        for t in (1, 2):
            for k in range(RINGS):
                self.load(k, t).start()

    def add(self, t, k, total):
        s = lax.rem(t, 2)
        self.hop(k, t - 1, self.slot.at[t - 1, k]).wait_recv()
        self.load(k, t).wait()
        r, c = self.p.shape
        if self.p.kind == "rows":
            w = next(x for x in (1280, 512, 256, 128) if c % x == 0)
            def part(i, _):
                at = pl.ds(pl.multiple_of(i * w, 128), w)
                x = (self.slot[t - 1, k, :, at].astype(F32) + self.loc[s, k, :, at].astype(F32)).astype(BF)
                self.slot[t - 1, k, :, at] = x
                if total:
                    x = x.astype(F32)
                    sq = x * x
                    self.squares[...] += tiles(sq)
            lax.fori_loop(0, c // w, part, None)
        else:
            x = (self.slot[t - 1, k].astype(F32) + self.loc[s, k].astype(F32)).astype(BF)
            self.slot[t - 1, k] = x
            if total:
                x = x.astype(F32)
                sq = x * x
                self.squares[...] += tiles(sq)

    def tick(self, t):
        for k in range(RINGS):
            self.add(t, k, False)
            self.hop(k, t, self.slot.at[t - 1, k]).start()
            @pl.when(t + 2 < self.p.n)
            def _():
                self.load(k, t + 2).start()

    def last(self):
        t = self.p.n - 1
        for k in range(RINGS):
            self.add(t, k, True)
            pltpu.make_async_copy(self.slot.at[t - 1, k], self.out.at[self.p.own(k)], self.osem).start()

    def finish(self):
        n = self.p.n
        sent = self.slot.at[pl.ds(0, n - 2)]
        pltpu.make_async_remote_copy(src_ref=sent, dst_ref=sent, send_sem=self.send, recv_sem=self.recv.at[0, 0], device_id={"dp": self.next[0]}, device_id_type=MESH).wait_send()
        one = self.slot.at[0]
        pltpu.make_async_remote_copy(src_ref=one, dst_ref=one, send_sem=self.fsem, recv_sem=self.recv.at[0, 0], device_id={"dp": self.next[0]}, device_id_type=MESH).wait_send()
        pltpu.make_async_copy(one, one, self.osem).wait()


def greet(R, peers):
    bar = pltpu.get_barrier_semaphore()
    for d in peers:
        pl.semaphore_signal(bar, inc=1, device_id=d, device_id_type=MESH)
    pl.semaphore_wait(bar, len(peers))


def scatter_body(n, pieces, which, ng, *refs):
    grads, outs, squares = refs[:ng], refs[ng:2 * ng], refs[2 * ng]
    rest = refs[2 * ng + 1:]
    R = Ring(n)
    greet(R, [{"dp": R.at(k, 1)} for k in range(RINGS)])
    squares[...] = jnp.zeros_like(squares)
    per = 7
    S = [Scatter(R, p, grads[g], outs[g], squares, rest[i * per:(i + 1) * per]) for i, (p, g) in enumerate(zip(pieces, which))]
    for s in S:
        s.first()
    def step(t, _):
        for s in S:
            s.tick(t)
    lax.fori_loop(1, n - 1, step, None)
    for s in S:
        s.last()
    for s in S:
        s.finish()


def scatter(n, grads, kinds, cuts, cid):
    pieces, which = [], []
    for g, (a, kind, cut) in enumerate(zip(grads, kinds, cuts)):
        for lo, hi in zip(cut[:-1], cut[1:]):
            pieces.append(Piece(kind, a.shape, n, lo, hi)); which.append(g)
    any_ = pl.BlockSpec(memory_space=pl.ANY)
    return pl.pallas_call(
        functools.partial(scatter_body, n, pieces, which, len(grads)),
        in_specs=[any_] * len(grads),
        out_specs=[any_] * len(grads) + [pl.BlockSpec(memory_space=pltpu.VMEM)],
        out_shape=[jax.ShapeDtypeStruct((a.shape[0] // n, a.shape[1]), BF) for a in grads] + [jax.ShapeDtypeStruct((8, 128), F32)],
        scratch_shapes=[s for p in pieces for s in p.scratch()],
        compiler_params=pltpu.CompilerParams(collective_id=cid, has_side_effects=True, vmem_limit_bytes=60 * 2**20),
        name=f"scatter{cid}",
    )(*grads)


def total_body(n, x_ref, o_ref, slots, send, recv):
    me, rep = lax.axis_index("dp"), 0
    bar = pltpu.get_barrier_semaphore()
    peers = [lax.rem(me + d, n) for d in range(1, n)]
    for p in peers:
        pl.semaphore_signal(bar, inc=1, device_id={"dp": p}, device_id_type=MESH)
    pl.semaphore_wait(bar, n - 1)
    copies = [pltpu.make_async_remote_copy(src_ref=x_ref, dst_ref=slots.at[d], send_sem=send.at[d], recv_sem=recv.at[d], device_id={"dp": p}, device_id_type=MESH)
              for d, p in enumerate(peers)]
    for c in copies:
        c.start()
    for c in copies:
        c.wait()
    t = x_ref[...]
    for d in range(n - 1):
        t = t + slots[d]
    o_ref[...] = jnp.broadcast_to(jnp.sum(jnp.sum(t, axis=1, keepdims=True), axis=0, keepdims=True), o_ref.shape)


def total(n, x, cid):
    return pl.pallas_call(
        functools.partial(total_body, n),
        in_specs=[pl.BlockSpec(memory_space=pltpu.VMEM)], out_specs=pl.BlockSpec(memory_space=pltpu.VMEM),
        out_shape=jax.ShapeDtypeStruct(x.shape, F32),
        scratch_shapes=[pltpu.VMEM((n - 1,) + x.shape, F32), pltpu.SemaphoreType.DMA((n - 1,)), pltpu.SemaphoreType.DMA((n - 1,))],
        compiler_params=pltpu.CompilerParams(collective_id=cid, has_side_effects=True), name="total",
    )(x)


def adamw(w, m, v, g):
    m = 0.9 * m + 0.1 * g
    v = 0.95 * v + 0.05 * g * g
    step = m * lax.rsqrt(v + 1e-8) + 0.1 * w
    return (w - 0.02 * step).astype(BF), m, v


def solution(mesh):
    n = mesh.shape["dp"]

    def step(x, dy, *arrays):
        weights, m, v = (arrays[i : i + 7] for i in (0, 7, 14))
        layers = weights[0].shape[0]
        shards = []
        for l in range(layers):
            wq, wk, wv, wo, wg, wu, wd = (w[l] for w in weights)
            shards += [jnp.concatenate([wq, wk, wv], 1), wo, mixed(wg, wu), wd]
        kinds = ["rows", "rows", "rows", "cols"]
        full = gather(n, kinds * layers, shards, 0)
        w = [full[4 * l : 4 * l + 4] for l in range(layers)]
        cos, sin = rotary(x.shape[1])
        kv = weights[1].shape[2] // HEAD
        h, kept = x[0], []
        for l in range(layers):
            h, k = forward(h, w[l], cos, sin, kv)
            kept.append(k)
        d, mine, squares = dy[0], [None] * layers, 0
        for l in reversed(range(layers)):
            terms, d = backward(d, w[l], kept[l], cos, sin, l > 0, kv)
            ff = terms[2].shape[1]
            *got, sq = scatter(n, terms, kinds, [(0, terms[0].shape[1]), (0, terms[1].shape[1]), (0, ff // 2, ff), (0, terms[3].shape[1])], 1 + l)
            squares = squares + sq
            mine[l] = got
        squares = total(n, squares, 1 + layers)[0, 0]
        count = n * sum(w.size for w in weights)
        factor = jnp.minimum(1.0, 0.5 * lax.rsqrt(squares / count + 1e-30))
        kw = weights[1].shape[2]
        gradients = []
        for l in range(layers):
            a, o, gu, dn = mine[l]
            q = a.shape[1] - 2 * kw
            g, u = unmixed(gu)
            gradients.append([a[:, :q], a[:, q : q + kw], a[:, q + kw :], o, g, u, dn])
        gradients = [jnp.stack([gradients[l][i] for l in range(layers)]).astype(F32) * factor for i in range(7)]
        new = [adamw(w.astype(F32), m, v, g) for w, m, v, g in zip(weights, m, v, gradients, strict=True)]
        return tuple(one[which] for which in range(3) for one in new)

    states, cut = P(("rep", "dp"), None, None), P(None, "dp", None)
    return jax.shard_map(step, mesh=mesh, in_specs=(states, states) + (cut,) * 21, out_specs=(P("rep", "dp", None),) * 21, check_vma=False)
```

```python
import functools

import jax
import jax.numpy as jnp
import numpy as np
from jax import lax
from jax.experimental import pallas as pl
from jax.experimental.pallas import tpu as pltpu
from jax.sharding import PartitionSpec as P

MESH = pl.DeviceIdType.MESH
BF, F32 = jnp.bfloat16, jnp.float32
LOG2E = 1.4426950408889634
NEG = -1e30
HEAD = 128
THETA = 10000
ROWS = 256
PARTS = 5
RINGS = 4
VMEM = 62 * 2**20


class Place:
    def __init__(self, n):
        self.n = n
        self.side = s = next(i for i in range(n) if i * i == n)
        self.me = lax.axis_index("dp")
        x, y = self.me // s, self.me % s
        turn = (x + y) % s
        self.place = [x * s + turn, y * s + turn]
        rep = lax.axis_index("rep")
        self.core = rep % 2
        self.twin = {"rep": rep + 1 - 2 * self.core}

    def at(self, k, off):
        s = self.side
        q = lax.rem(self.place[k // 2] + (off if k % 2 == 0 else -off) + self.n, self.n)
        a = lax.div(q, s)
        b = lax.rem(q - a + s, s)
        return a * s + b if k < 2 else b * s + a

    def next(self, k):
        return {"dp": self.at(k, 1)}


def remote(src, dst, send, recv, device):
    return pltpu.make_async_remote_copy(src_ref=src, dst_ref=dst, send_sem=send, recv_sem=recv, device_id=device, device_id_type=MESH)


def greet(devices):
    bar = pltpu.get_barrier_semaphore()
    for d in devices:
        pl.semaphore_signal(bar, device_id=d, device_id_type=MESH)
    pl.semaphore_wait(bar, len(devices))


class Gather:
    def __init__(self, place, n, shard, full, sems):
        self.place, self.n, self.shard, self.full = place, n, shard, full
        self.recv, self.send, self.hand, self.handed, self.local = sems
        self.rounds = n - 1
        self.block = shard.shape[0]
        self.wide = shard.shape[1] // 2
        self.by_rows = self.block % (16 * RINGS) == 0

    def part(self, ref, k, block):
        core, w = self.place.core, self.wide
        if self.by_rows:
            r = self.block // RINGS
            return ref.at[pl.ds(pl.multiple_of(block * self.block + k * r, r), r), pl.ds(pl.multiple_of(core * w, HEAD), w)]
        c = w // RINGS
        return ref.at[pl.ds(pl.multiple_of(block * self.block, 8), self.block), pl.ds(pl.multiple_of(core * w + k * c, HEAD), c)]

    def hop(self, k, t, src, block):
        return remote(src, self.part(self.full, k, block), self.send, self.recv.at[k, t], self.place.next(k))

    def keep(self):
        return pltpu.make_async_copy(self.shard, self.full.at[pl.ds(pl.multiple_of(self.place.me * self.block, 8), self.block)], self.local)

    def first(self):
        for k in range(RINGS):
            self.hop(k, 0, self.part(self.shard, k, 0), self.place.me).start()
        self.keep().start()

    def tick(self, t):
        for k in range(RINGS):
            block = self.place.at(k, -t)
            here = self.part(self.full, k, block)
            self.hop(k, t - 1, here, block).wait_recv()

            @pl.when(t < self.n - 1)
            def _():
                self.hop(k, t, here, block).start()

            remote(here, here, self.hand, self.handed, self.place.twin).start()

    def last(self):
        self.keep().wait()
        half = self.full.at[pl.ds(0, (self.n - 1) * self.block), pl.ds(0, self.wide)]
        remote(half, half, self.send, self.handed, self.place.twin).wait_send()
        remote(half, half, self.hand, self.handed, self.place.twin).wait()

    def finish(self):
        pass


def gather_sems(n):
    return [pltpu.SemaphoreType.DMA((RINGS, n - 1))] + [pltpu.SemaphoreType.DMA] * 4


def scatter_shape(n, shape):
    block = shape[0] // n
    return (block // RINGS, shape[1]) if block % (16 * RINGS) == 0 else (block, shape[1] // RINGS)


def scatter_scratch(n, shape):
    s = scatter_shape(n, shape)
    dma = pltpu.SemaphoreType.DMA
    return [pltpu.VMEM((n - 1, RINGS) + s, BF), pltpu.VMEM((2, RINGS) + s, BF), dma((n - 1, RINGS)), dma((2, RINGS)), dma, dma, dma, pltpu.SemaphoreType.REGULAR]


def tiles(x):
    r, c = x.shape
    return sum(x[a : a + 8, b : b + HEAD] for a in range(0, r, 8) for b in range(0, c, HEAD))


class Scatter:
    def __init__(self, place, n, grad, out, squares, scratch, again):
        self.place, self.n, self.grad, self.out, self.squares, self.again = place, n, grad, out, squares, again
        self.slot, self.mine, self.recv, self.load, self.send, self.sent, self.kept, self.free = scratch
        self.rounds = n - 2
        self.block = grad.shape[0] // n
        self.shape = scatter_shape(n, grad.shape)
        self.by_rows = self.shape[0] < self.block

    def part(self, ref, k, block):
        r, c = self.shape
        if self.by_rows:
            return ref.at[pl.ds(pl.multiple_of(block * self.block + k * r, r), r), pl.ds(0, c)]
        return ref.at[pl.ds(pl.multiple_of(block * r, 8), r), pl.ds(k * c, c)]

    def term(self, k, t):
        return self.part(self.grad, k, self.place.at(k, -1 - t))

    def fetch(self, k, t):
        s = t % 2
        return pltpu.make_async_copy(self.term(k, t), self.mine.at[s, k], self.load.at[s, k])

    def hop(self, k, t, src, sem):
        return remote(src, self.slot.at[t, k], sem, self.recv.at[t, k], self.place.next(k))

    def first(self):
        if self.again:
            pl.semaphore_wait(self.free, RINGS)
        for k in range(RINGS):
            self.hop(k, 0, self.term(k, 0), self.sent).start()
            for t in (1, 2):
                self.fetch(k, t).start()

    def add(self, k, t):
        self.hop(k, t - 1, self.slot.at[t - 1, k], self.send).wait_recv()
        self.fetch(k, t).wait()
        s = t % 2
        r, c = self.shape
        w = next(w for w in (1280, c) if c % w == 0)

        def some(i, _):
            at = pl.ds(pl.multiple_of(i * w, HEAD), w)
            self.slot[t - 1, k, :, at] = (self.slot[t - 1, k, :, at].astype(F32) + self.mine[s, k, :, at].astype(F32)).astype(BF)

        lax.fori_loop(0, c // w, some, None)

    def tick(self, t):
        for k in range(RINGS):
            self.add(k, t)

        @pl.when(t + 2 < self.n)
        def _():
            for k in range(RINGS):
                self.fetch(k, t + 2).start()

        for k in range(RINGS):
            self.hop(k, t, self.slot.at[t - 1, k], self.send).start()

    def last(self):
        t = self.n - 1
        for k in range(RINGS):
            self.add(k, t)
            r, c = self.shape
            w = HEAD

            def some(i, _):
                x = self.slot[t - 1, k, :, pl.ds(pl.multiple_of(i * w, HEAD), w)].astype(F32)
                self.squares[...] += tiles(x * x)

            lax.fori_loop(0, c // w, some, None)
            at = (pl.ds(k * r, r), slice(None)) if self.by_rows else (slice(None), pl.ds(k * c, c))
            pltpu.make_async_copy(self.slot.at[t - 1, k], self.out.at[at], self.kept).start()

    def finish(self):
        some, one = self.slot.at[pl.ds(0, self.n - 2)], self.slot.at[0]
        remote(some, some, self.send, self.recv.at[0, 0], self.place.next(0)).wait_send()
        remote(one, one, self.sent, self.recv.at[0, 0], self.place.next(0)).wait_send()
        pltpu.make_async_copy(one, one, self.kept).wait()
        if not self.again:
            for k in range(RINGS):
                pl.semaphore_signal(self.free, device_id={"dp": self.place.at(k, -1)}, device_id_type=MESH)


class Traffic:
    def __init__(self):
        self.live, self.due, self.over = [], [], []

    def start(self, *pieces):
        for p in pieces:
            p.first()
            self.live.append((p, 1))

    def rounds(self, r, steps):
        runs = []
        for _ in range(r):
            now = self.live
            if not now:
                break
            if runs and [p for p, _ in runs[-1][0]] == [p for p, _ in now]:
                runs[-1][1] += 1
            else:
                runs.append([now, 1])
            self.due += [p for p, t in now if t == p.rounds]
            self.live = [(p, t + 1) for p, t in now if t < p.rounds]
        count = sum(len(now) * times for now, times in runs)

        def item(e, _):
            at = 0
            for now, times in runs:
                m = len(now)
                for a, (p, t) in enumerate(now):
                    @pl.when((e >= at) & (e < at + m * times) & (lax.rem(e - at + m, m) == a))
                    def _():
                        p.tick(t + (e - at) // m)
                at += m * times

        def tick(i):
            if count:
                lo, hi = lax.div(i * count, steps), lax.div((i + 1) * count, steps)

                def one(j, _):
                    @pl.when(lo + j < hi)
                    def _():
                        item(lo + j, None)

                lax.fori_loop(0, -(-count // steps), one, None)
        return tick

    def settle(self):
        for p in self.over:
            p.finish()
        for p in self.due:
            p.last()
        self.over, self.due = self.due, []

    def drain(self):
        while self.live:
            self.rounds(max(p.rounds for p, _ in self.live), 1)(0)
            self.settle()
        self.settle()
        self.settle()


def dot(a, b, ca, cb):
    return lax.dot_general(a, b, (((ca,), (cb,)), ((), ())), preferred_element_type=F32)


def nn(a, b):
    return dot(a, b, 1, 0)


def nt(a, b):
    return dot(a, b, 1, 1)


def row(i):
    return i, 0


def col(j):
    return 0, j


def whole(*_):
    return 0, 0


def run(body, grid, ins, outs, scratch=(), tick=None):
    held = [r for r, block, _ in ins if block is None]
    tiled = [x for x in ins if x[1] is not None]

    def inner(sem, *refs):
        full, rest = refs[: len(held)], refs[len(held) :]
        copies = [pltpu.make_async_copy(r, v, sem.at[i]) for i, (r, v) in enumerate(zip(held, full))]
        for c in copies:
            c.start()

        def step(*tiles):
            @pl.when(functools.reduce(lambda p, q: p & q, [pl.program_id(i) == 0 for i in range(len(grid))]))
            def _():
                for c in copies:
                    c.wait()

            some, more, given = iter(tiles), iter(full), []
            for _, block, _ in ins:
                given.append(next(more) if block is None else next(some))
            body(*given, *some, *rest, tick or (lambda i: None))

        specs = lambda arrays: [pl.BlockSpec(block, at) for _, block, at in arrays]
        pltpu.emit_pipeline(step, grid=grid, in_specs=specs(tiled), out_specs=specs(outs))(*[r for r, _, _ in tiled], *[r for r, _, _ in outs])

    pl.run_scoped(inner, pltpu.SemaphoreType.DMA((max(len(held), 1),)), *[pltpu.VMEM(r.shape, r.dtype) for r in held], *scratch)


def all_of(ref):
    return ref, None, None


def rows_of(ref):
    return ref, (ROWS, ref.shape[1]), row


def cols_of(ref, parts):
    return ref, (ref.shape[0], ref.shape[1] // parts), col


def in_rows(size, body, tick, at=0):
    n = size // ROWS

    def one(i, _):
        body(pl.ds(pl.multiple_of(i * ROWS, ROWS), ROWS))
        tick(pl.program_id(0) * n + i)

    lax.fori_loop(0, n, one, None)


def unit(h):
    return lax.rsqrt(jnp.mean(h * h, -1, keepdims=True) + 1e-6)


def normed(h):
    h = h.astype(F32)
    return (h * unit(h)).astype(BF)


def norm_back(h, d):
    h = h.astype(F32)
    s = unit(h)
    return (s * d - h * (s * s * s * jnp.mean(h * d, -1, keepdims=True))).astype(BF)


def rotary(tokens):
    half = HEAD // 2
    angle = np.arange(tokens, dtype=F32)[:, None] * np.power(np.float32(THETA), -np.arange(half, dtype=F32) / half)
    c, s = np.cos(angle), np.sin(angle)
    return jnp.asarray(np.concatenate([c, c], 1)), jnp.asarray(np.concatenate([-s, s], 1))


def heads_of(ref, g):
    return [ref[:, n * HEAD : (n + 1) * HEAD] for n in range(g)]


def qkv_body(h_ref, w_ref, c_ref, s_ref, a_ref, o_ref, tick, *, turned):
    a = normed(h_ref[...])
    a_ref[...] = a
    r = nn(a, w_ref[...]).astype(BF)
    for n in range(r.shape[1] // HEAD):
        at = slice(n * HEAD, (n + 1) * HEAD)
        x = r[:, at]
        if n < turned:
            x = x.astype(F32)
            x = (x * c_ref[...] + pltpu.roll(x, HEAD // 2, 1) * s_ref[...]).astype(BF)
        o_ref[:, at] = x
    tick(pl.program_id(0))


def qkv(h, w, cos, sin, kv, a, x, tick):
    run(functools.partial(qkv_body, turned=w.shape[1] // HEAD - kv), (h.shape[0] // ROWS,), [rows_of(h), all_of(w), rows_of(cos), rows_of(sin)],
        [rows_of(a), rows_of(x)], tick=tick)


def out_body(h_ref, x_ref, w_ref, m_ref, b_ref, tick):
    m = h_ref[...] + nn(x_ref[...], w_ref[...]).astype(BF)
    m_ref[...] = m
    b_ref[...] = normed(m)
    tick(pl.program_id(0))


def out_proj(h, o, w, m, b, tick):
    run(out_body, (h.shape[0] // ROWS,), [rows_of(h), rows_of(o), all_of(w)], [rows_of(m), rows_of(b)], tick=tick)


def gu_body(b_ref, w_ref, g_ref, m_ref, tick):
    half = m_ref.shape[1]

    def tile(at):
        r = nn(b_ref[at, :], w_ref[...])
        g_ref[at, :] = r
        g = r[:, :half]
        m_ref[at, :] = (g * jax.nn.sigmoid(g) * r[:, half:]).astype(BF)

    in_rows(b_ref.shape[0], tile, tick)


def gate_up(b, w, gu, mid, tick):
    run(gu_body, (PARTS,), [all_of(b), cols_of(w, PARTS)], [cols_of(gu, PARTS), cols_of(mid, PARTS)], tick=tick)


def down_body(h_ref, m_ref, w_ref, o_ref, tick):
    o_ref[...] = h_ref[...] + nn(m_ref[...], w_ref[...]).astype(BF)
    tick(pl.program_id(0))


def down(h, mid, w, out, tick):
    run(down_body, (h.shape[0] // ROWS,), [rows_of(h), rows_of(mid), all_of(w)], [rows_of(out)], tick=tick)


def visible(iq, j, bq, bk):
    return lax.broadcasted_iota(jnp.int32, (bk, bq), 1) - lax.broadcasted_iota(jnp.int32, (bk, bq), 0) >= j * bk - iq * bq


def key_blocks(iq, total, bq, bk, block, tick):
    full, m = iq * bq // bk, bq // bk
    before = pl.program_id(0) * m * (pl.num_programs(1) * (pl.num_programs(1) + 1) // 2) + m * (iq * (iq + 1) // 2)

    def one(j, masked):
        block(j, masked)
        tick(before + j)

    def seen(j, _):
        @pl.when(j < full)
        def _():
            one(j, False)

        @pl.when((j >= full) & (j < full + m))
        def _():
            one(j, True)

    lax.fori_loop(0, total // bk, seen, None)


def fwd_body(q_ref, k_ref, v_ref, o_ref, lse_ref, top_s, mix_s, tick, *, scale, bk):
    bq, g = q_ref.shape[0], q_ref.shape[1] // HEAD
    iq = pl.program_id(1)
    e = scale * LOG2E
    top_s[...] = jnp.full(top_s.shape, NEG, F32)
    mix_s[...] = jnp.zeros(mix_s.shape, F32)
    ones = jnp.ones((8, bk), BF)

    def block(j, masked):
        here = pl.ds(pl.multiple_of(j * bk, bk), bk)
        k = k_ref[here, :]
        scores = [nt(k, q) for q in heads_of(q_ref, g)]
        values = jnp.concatenate([v_ref[here, :].T, ones], axis=0)
        weights, keeps = [], []
        for n, s in enumerate(scores):
            if masked:
                s = jnp.where(visible(iq, j, bq, bk), s, 2 * NEG)
            mine = slice(n, n + 1)
            old = top_s[mine, :]
            top = jnp.maximum(old, s.max(axis=0, keepdims=True))
            top_s[mine, :] = top
            weights.append(jnp.exp2((s - top) * e).astype(BF))
            keeps.append(jnp.exp2((old - top) * e))
        for n in range(g):
            mix_s[n] = mix_s[n] * keeps[n] + nn(values, weights[n])

    key_blocks(iq, k_ref.shape[0], bq, bk, block, tick)
    for n in range(g):
        mine = slice(n, n + 1)
        total = mix_s[n, HEAD : HEAD + 1, :]
        o_ref[:, n * HEAD : (n + 1) * HEAD] = (mix_s[n, :HEAD, :] * (1 / total)).T.astype(BF)
        lse_ref[0, mine, :] = top_s[mine, :] * scale + jnp.log(total)


def attention_specs(x, kv, bq):
    t, n = x.shape
    heads = n // HEAD - 2 * kv
    g = heads // kv
    return (bq, g * HEAD), [(x, (bq, g * HEAD), lambda c, i: (i, c)), (x, (t, HEAD), lambda c, i: (0, heads + c)), (x, (t, HEAD), lambda c, i: (0, heads + kv + c))], \
        lambda ref: (ref, (1, g, bq), lambda c, i: (c, 0, i))


def attend(x, kv, o, lse, tick, bq=512, bk=256):
    tile, ins, stat = attention_specs(x, kv, bq)
    run(functools.partial(fwd_body, scale=HEAD**-0.5, bk=bk), (kv, x.shape[0] // bq), ins, [(o, tile, lambda c, i: (i, c)), stat(lse)],
        [pltpu.VMEM((8, bq), F32), pltpu.VMEM((tile[1] // HEAD, HEAD + 8, bq), F32)], tick)


def bwd_body(q_ref, k_ref, v_ref, do_ref, lse_ref, delta_ref, c_ref, s_ref, dq_ref, dk_ref, dv_ref, dq_s, dk_s, dv_s, tick, *, scale, bk):
    bq, g = q_ref.shape[0], q_ref.shape[1] // HEAD
    iq = pl.program_id(1)
    e = scale * LOG2E

    @pl.when(iq == 0)
    def _():
        dk_s[...] = jnp.zeros_like(dk_s)
        dv_s[...] = jnp.zeros_like(dv_s)

    dq_s[...] = jnp.zeros_like(dq_s)

    def block(j, masked):
        here = pl.ds(pl.multiple_of(j * bk, bk), bk)
        k, v = k_ref[here, :], v_ref[here, :]
        back = k.T
        qs, dos = heads_of(q_ref, g), heads_of(do_ref, g)
        scores = [nt(k, x) for x in qs]
        dps = [nt(v, x) for x in dos]
        for n in range(g):
            mine = slice(n, n + 1)
            p = jnp.exp2(scores[n] * e - lse_ref[0, mine, :] * LOG2E)
            if masked:
                p = jnp.where(visible(iq, j, bq, bk), p, 0.0)
            ds = (p * (dps[n] - delta_ref[0, mine, :])).astype(BF)
            dv_s[here, :] += nn(p.astype(BF), dos[n])
            dk_s[here, :] += nn(ds, qs[n])
            dq_s[n] += nn(back, ds)

    key_blocks(iq, k_ref.shape[0], bq, bk, block, tick)

    def unturned(d, at):
        d = d.astype(BF).astype(F32)
        return (d * c_ref[at, :] - pltpu.roll(d, HEAD // 2, 1) * s_ref[at, :]).astype(BF)

    for n in range(g):
        dq_ref[:, n * HEAD : (n + 1) * HEAD] = unturned((dq_s[n] * scale).T, pl.ds(pl.multiple_of(iq * bq, bq), bq))

    @pl.when(iq == pl.num_programs(1) - 1)
    def _():
        dk_ref[...] = unturned(dk_s[...] * scale, slice(None))
        dv_ref[...] = dv_s[...].astype(BF)


def attend_back(x, do, lse, delta, cos, sin, kv, dq, dk, dv, tick, bq=512, bk=256):
    tile, ins, stat = attention_specs(x, kv, bq)
    t = x.shape[0]
    mine = lambda ref: (ref, (t, HEAD), lambda c, i: (0, c))
    run(functools.partial(bwd_body, scale=HEAD**-0.5, bk=bk), (kv, t // bq), ins + [(do, tile, lambda c, i: (i, c)), stat(lse), stat(delta), all_of(cos), all_of(sin)],
        [(dq, tile, lambda c, i: (i, c)), mine(dk), mine(dv)], [pltpu.VMEM((tile[1] // HEAD, HEAD, bq), F32)] + [pltpu.VMEM((t, HEAD), F32)] * 2, tick)


def silu_back(g, u, d):
    s = jax.nn.sigmoid(g)
    silu = g * s
    return (silu * u).astype(BF), (d * u * (s + silu * (1 - s))).astype(BF), (d * silu).astype(BF)


def dgu_body(dy_ref, w_ref, g_ref, dg_ref, dw_ref, mid_s, tick):
    half = mid_s.shape[1]

    def tile(at):
        d = nt(dy_ref[at, :], w_ref[...]).astype(BF).astype(F32)
        mid_s[at, :], dg_ref[at, :half], dg_ref[at, half:] = silu_back(g_ref[at, :half], g_ref[at, half:], d)

    in_rows(dy_ref.shape[0], tile, tick)
    dw_ref[...] = dot(mid_s[...], dy_ref[...], 0, 0).astype(BF)


def dgu(dy, wd, gu, dg, dwd, tick):
    t, c = dy.shape[0], wd.shape[0] // PARTS
    rows = lambda ref: (ref, (c, ref.shape[1]), row)
    run(dgu_body, (PARTS,), [all_of(dy), rows(wd), cols_of(gu, PARTS)], [cols_of(dg, PARTS), rows(dwd)], [pltpu.VMEM((t, c), BF)], tick)


def last_body(dy_ref, wd_ref, b_ref, w_ref, dg_ref, dw_ref, mid_s, tick):
    half = mid_s.shape[1]

    def tile(at):
        r = nn(b_ref[at, :], w_ref[...])
        d = nt(dy_ref[at, :], wd_ref[...]).astype(BF).astype(F32)
        mid_s[at, :], dg_ref[at, :half], dg_ref[at, half:] = silu_back(r[:, :half], r[:, half:], d)

    in_rows(dy_ref.shape[0], tile, tick)
    dw_ref[...] = dot(mid_s[...], dy_ref[...], 0, 0).astype(BF)


def last_dgu(dy, wd, b, wgu, dg, dwd, tick):
    t, c = dy.shape[0], wd.shape[0] // PARTS
    rows = lambda ref: (ref, (c, ref.shape[1]), row)
    run(last_body, (PARTS,), [all_of(dy), rows(wd), all_of(b), cols_of(wgu, PARTS)], [cols_of(dg, PARTS), rows(dwd)], [pltpu.VMEM((t, c), BF)], tick)


def dw_body(a_ref, d_ref, o_ref, at_s, tick):
    @pl.when(pl.program_id(0) == 0)
    def _():
        at_s[...] = a_ref[...].T

    def tile(at):
        o_ref[at, :] = nn(at_s[at, :], d_ref[...]).astype(BF)

    in_rows(at_s.shape[0], tile, tick)


def dw(a, d, out, parts, tick):
    run(dw_body, (parts,), [all_of(a), cols_of(d, parts)], [cols_of(out, parts)], [pltpu.VMEM(a.shape[::-1], BF)], tick)


def db_body(dg_ref, w_ref, dy_ref, h_ref, o_ref, acc, tick):
    j = pl.program_id(0)
    end = pl.num_programs(0) - 1

    def tile(at):
        r = nt(dg_ref[at, :], w_ref[...])

        @pl.when(j == 0)
        def _():
            acc[at, :] = r

        @pl.when((j > 0) & (j < end))
        def _():
            acc[at, :] += r

        @pl.when(j == end)
        def _():
            o_ref[at, :] = dy_ref[at, :] + norm_back(h_ref[at, :], (acc[at, :] + r).astype(BF).astype(F32))

    in_rows(dy_ref.shape[0], tile, tick)


def db(dg, wgu, dy, h, out, tick):
    run(db_body, (PARTS,), [cols_of(dg, PARTS), cols_of(wgu, PARTS), all_of(dy), all_of(h)], [(out, out.shape, whole)], [pltpu.VMEM(dy.shape, F32)], tick)


def do_body(d_ref, w_ref, o_ref, do_ref, delta_ref, tick):
    r = nt(d_ref[...], w_ref[...]).astype(BF)
    do_ref[...] = r
    kv, g = delta_ref.shape[:2]
    for n in range(kv * g):
        at = slice(n * HEAD, (n + 1) * HEAD)
        x = r[:, at].astype(F32) * o_ref[:, at].astype(F32)
        delta_ref[n // g, n % g : n % g + 1, :] = jnp.sum(x.T, axis=0, keepdims=True)
    tick(pl.program_id(0))


def do_delta(d, wo, o, do, delta, tick):
    run(do_body, (d.shape[0] // ROWS,), [rows_of(d), all_of(wo), rows_of(o)], [rows_of(do), (delta, delta.shape[:2] + (ROWS,), lambda i: (0, 0, i))], tick=tick)


def da_body(dq_ref, dk_ref, dv_ref, w_ref, d_ref, h_ref, o_ref, tick):
    n, m = dq_ref.shape[1], dk_ref.shape[1]
    r = nt(dq_ref[...], w_ref[:, :n]) + nt(dk_ref[...], w_ref[:, n : n + m]) + nt(dv_ref[...], w_ref[:, n + m :])
    o_ref[...] = d_ref[...] + norm_back(h_ref[...], r.astype(BF).astype(F32))
    tick(pl.program_id(0))


def da(dq, dk, dv, w, d, h, out, tick):
    run(da_body, (d.shape[0] // ROWS,), [rows_of(dq), rows_of(dk), rows_of(dv), all_of(w), rows_of(d), rows_of(h)], [rows_of(out)], tick=tick)


def dqkv_body(a_ref, dq_ref, dk_ref, dv_ref, o_ref, tick):
    back = a_ref[...].T
    n, m = dq_ref.shape[1], dk_ref.shape[1]
    o_ref[:, :n] = nn(back, dq_ref[...]).astype(BF)
    o_ref[:, n : n + m] = nn(back, dk_ref[...]).astype(BF)
    o_ref[:, n + m :] = nn(back, dv_ref[...]).astype(BF)
    tick(pl.program_id(0))


def dqkv(a, dq, dk, dv, out, tick):
    run(dqkv_body, (a.shape[1] // ROWS,), [(a, (a.shape[0], ROWS), col), all_of(dq), all_of(dk), all_of(dv)], [rows_of(out)], tick=tick)


TILES, GROUP = 4, PARTS * 4
WAYS = ("a", "gu", "d")
NAMES = ("wq", "wk", "wv", "wo", "w_gate", "w_up", "w_down")


def named(names, refs):
    return dict(zip(names, refs, strict=True))


def beside(r, l, kw):
    a = r.shape[1]
    q = a // 2 - kw
    return r.at[:, pl.ds(0, a - q)], r.at[:, pl.ds(a - q, q)]


def mixture(f):
    w = f // PARTS
    return [(i, j * w, (2 * j + i) * w, w) for j in range(PARTS) for i in range(2)]


def forward_kernel(n, layers, kv, ins, outs, count, *refs):
    r = named(ins + outs, refs[:count])
    packs, sems = refs[count : count + 2], refs[count + 2 :]
    for l in range(layers):
        at = 0
        for name in NAMES[:4]:
            w = r[name].shape[2]
            packs[0][l, :, at : at + w] = r[name][l]
            at += w
        for i, a, b, w in mixture(r["w_up"].shape[2]):
            packs[1][l, :, b : b + w] = r[NAMES[4 + i]][l, :, a : a + w]
    place = Place(n)
    greet([place.next(k) for k in range(RINGS)] + [place.twin])
    pieces = [[Gather(place, n, p.at[l], r[f"w{w}{l}"], sems[5 * (3 * l + i) : 5 * (3 * l + i) + 5]) for i, (w, p) in enumerate(zip(WAYS, (*packs, r["w_down"])))]
              for l in range(layers)]
    road = Traffic()

    def arrived(*wanted):
        while any(p is q for p, _ in road.live for q in wanted):
            road.rounds(1, 1)(0)
        road.settle()

    road.start(*pieces[0])
    h = r["x"].at[0]
    for l in range(layers):
        arrived(*pieces[l])
        if l + 1 < layers:
            road.start(*pieces[l + 1])
        wqkv, wo = beside(r[f"wa{l}"], l, kv * HEAD)
        qkv(h, wqkv, r["cos"], r["sin"], kv, r[f"a{l}"], r[f"x{l}"], road.rounds(2, TILES))
        attend(r[f"x{l}"], kv, r[f"o{l}"], r[f"lse{l}"], road.rounds(4, 12))
        out_proj(h, r[f"o{l}"], wo, r[f"m{l}"], r[f"b{l}"], road.rounds(2, TILES))
        if l + 1 < layers:
            gate_up(r[f"b{l}"], r[f"wgu{l}"], r[f"gu{l}"], r[f"mid{l}"], road.rounds(4, GROUP))
            down(r[f"m{l}"], r[f"mid{l}"], r[f"wd{l}"], r[f"h{l + 1}"], road.rounds(3, TILES))
            h = r[f"h{l + 1}"]
    road.drain()


def backward_kernel(n, layers, kv, ins, outs, count, *refs):
    r = named(ins + outs, refs[:count])
    squares, slots, send, recv = refs[count : count + 4]
    held = [refs[i : i + 8] for i in range(count + 4, len(refs), 8)]
    place = Place(n)
    others = [{"dp": lax.rem(place.me + i, n)} for i in range(1, n)]
    greet(others)
    squares[...] = jnp.zeros_like(squares)
    road = Traffic()

    def piece(l, w):
        i = WAYS.index(w)
        return Scatter(place, n, r[f"t{w}{l}"], r[f"g{w}{l}"], squares, held[i], l + 1 < layers)

    d = r["dy"].at[0]
    for l in reversed(range(layers)):
        if l + 1 == layers:
            last_dgu(d, r[f"wd{l}"], r[f"b{l}"], r[f"wgu{l}"], r["dg"], r[f"td{l}"], None)
        else:
            dgu(d, r[f"wd{l}"], r[f"gu{l}"], r["dg"], r[f"td{l}"], road.rounds(6, GROUP))
        wqkv, wo = beside(r[f"wa{l}"], l, kv * HEAD)
        tqkv, to = beside(r[f"ta{l}"], l, kv * HEAD)
        road.settle()
        road.start(piece(l, "d"))
        dw(r[f"b{l}"], r["dg"], r[f"tgu{l}"], PARTS, road.rounds(5, GROUP))
        road.settle()
        road.start(piece(l, "gu"))
        db(r["dg"], r[f"wgu{l}"], d, r[f"m{l}"], r["dm"], road.rounds(4, GROUP))
        road.settle()
        do_delta(r["dm"], wo, r[f"o{l}"], r["do"], r["delta"], road.rounds(1, TILES))
        dw(r[f"o{l}"], r["dm"], to, 2, road.rounds(1, 2 * TILES))
        road.settle()
        attend_back(r[f"x{l}"], r["do"], r[f"lse{l}"], r["delta"], r["cos"], r["sin"], kv, r["dq"], r["dk"], r["dv"], road.rounds(4, 12))
        road.settle()
        dqkv(r[f"a{l}"], r["dq"], r["dk"], r["dv"], tqkv, road.rounds(1, TILES))
        road.settle()
        road.start(piece(l, "a"))
        if l:
            da(r["dq"], r["dk"], r["dv"], wqkv, r["dm"], r[f"h{l}"], r[f"d{l}"], road.rounds(2, TILES))
            d = r[f"d{l}"]
    road.drain()
    copies = [remote(squares, slots.at[i], send.at[i], recv.at[i], p) for i, p in enumerate(others)]
    for c in copies:
        c.start()
    for c in copies:
        c.wait()
    t = squares[...] + sum(slots[i] for i in range(n - 1))
    r["total"][...] = jnp.broadcast_to(jnp.sum(jnp.sum(t, axis=1, keepdims=True), axis=0, keepdims=True), t.shape)


def kernel(body, name, number, given, made, in_vmem, scratch):
    space = lambda name: pl.BlockSpec(memory_space=pltpu.VMEM if name in in_vmem else pl.ANY)
    got = pl.pallas_call(
        functools.partial(body, tuple(given), tuple(made), len(given) + len(made)),
        in_specs=[space(k) for k in given],
        out_specs=[space(k) for k in made],
        out_shape=[jax.ShapeDtypeStruct(*s) for s in made.values()],
        scratch_shapes=scratch,
        compiler_params=pltpu.CompilerParams(collective_id=number, has_side_effects=True, vmem_limit_bytes=VMEM),
        name=name,
    )(*given.values())
    return dict(zip(made, got, strict=True))


def adamw(w, m, v, g):
    m = 0.9 * m + 0.1 * g
    v = 0.95 * v + 0.05 * g * g
    step = m * lax.rsqrt(v + 1e-8) + 0.1 * w
    return (w - 0.02 * step).astype(BF), m, v


def step_kernel(count, layers, total_ref, *refs):
    grads, refs = refs[: 3 * layers], refs[3 * layers :]
    olds, news = refs[:21], refs[21:]
    factor = jnp.minimum(1.0, 0.5 * lax.rsqrt(total_ref[:1, :1] / count + 1e-30))
    for l in range(layers):
        @pl.when(pl.program_id(0) == l)
        def _():
            a, gu, d = grads[3 * l : 3 * l + 3]
            moves, at = [], 0
            for i in range(4):
                w = olds[i].shape[2]
                moves.append((i, a, 0, at, w))
                at += w
            moves += [(4 + i, gu, to, at, w) for i, to, at, w in mixture(olds[4].shape[2])] + [(6, d, 0, 0, d.shape[1])]
            for i, g, to, at, w in moves:
                for c in range(0, w, HEAD):
                    here = slice(to + c, to + c + HEAD)
                    new = adamw(*[olds[j][0, :, here].astype(F32) for j in (i, i + 7, i + 14)], g[:, at + c : at + c + HEAD].astype(F32) * factor)
                    for j, x in zip((i, i + 7, i + 14), new):
                        news[j][0, :, here] = x


def optimizer(n, total, grads, arrays):
    layers = arrays[0].shape[0]
    tile = lambda a: pl.BlockSpec((1,) + a.shape[1:], lambda l: (l, 0, 0))
    held = pl.BlockSpec(memory_space=pltpu.VMEM)
    return pl.pallas_call(
        functools.partial(step_kernel, n * sum(a.size for a in arrays[:7]), layers),
        grid=(layers,),
        in_specs=[held] * (1 + len(grads)) + [tile(a) for a in arrays],
        out_specs=[tile(a) for a in arrays],
        out_shape=[jax.ShapeDtypeStruct(a.shape, a.dtype) for a in arrays],
        compiler_params=pltpu.CompilerParams(dimension_semantics=("arbitrary",), vmem_limit_bytes=VMEM),
        name="optimizer",
    )(total, *grads, *arrays)


def solution(mesh):
    n = mesh.shape["dp"]

    def step(x, dy, *arrays):
        weights = named(NAMES, arrays[:7])
        layers, _, kw = weights["wk"].shape
        kv = kw // HEAD
        t, d = x.shape[1:]
        q, f = weights["wq"].shape[2], weights["w_up"].shape[2]
        cos, sin = rotary(t)
        shapes = {"a": (d, 2 * q + 2 * kw), "gu": (d, 2 * f), "d": (f, d)}
        made = {}
        for l in range(layers):
            made |= {f"w{w}{l}": (shapes[w], BF) for w in WAYS}
            made |= {f"a{l}": ((t, d), BF), f"x{l}": ((t, q + 2 * kw), BF), f"o{l}": ((t, q), BF), f"lse{l}": ((kv, q // kw, t), F32),
                     f"m{l}": ((t, d), BF), f"b{l}": ((t, d), BF)}
            if l + 1 < layers:
                made |= {f"gu{l}": ((t, 2 * f), F32), f"mid{l}": ((t, f), BF), f"h{l + 1}": ((t, d), BF)}
        shards = [pltpu.VMEM((layers, shapes[w][0] // n, shapes[w][1]), BF) for w in WAYS[:2]]
        kept = kernel(functools.partial(forward_kernel, n, layers, kv), "forward", 0, {"x": x, "cos": cos, "sin": sin, **weights}, made, NAMES,
                      shards + gather_sems(n) * (len(WAYS) * layers))
        given = {"dy": dy, "cos": cos, "sin": sin, **{k: a for k, a in kept.items() if not k.startswith("mid")}}
        made = {"dg": ((t, 2 * f), BF), "do": ((t, q), BF), "delta": ((kv, q // kw, t), F32), "dm": ((t, d), BF), "dq": ((t, q), BF), "dk": ((t, kw), BF), "dv": ((t, kw), BF),
                "total": ((8, HEAD), F32)}
        for l in range(layers):
            made |= {f"t{w}{l}": (shapes[w], BF) for w in WAYS} | {f"g{w}{l}": ((shapes[w][0] // n, shapes[w][1]), BF) for w in WAYS} | {f"d{l}": ((t, d), BF)}
        scratch = [pltpu.VMEM((8, HEAD), F32), pltpu.VMEM((n - 1, 8, HEAD), F32)] + [pltpu.SemaphoreType.DMA((n - 1,))] * 2
        got = kernel(functools.partial(backward_kernel, n, layers, kv), "backward", 1, given, made, ["total"], sum([scatter_scratch(n, shapes[w]) for w in WAYS], scratch))
        return tuple(optimizer(n, got["total"], [got[f"g{w}{l}"] for l in range(layers) for w in WAYS], arrays))

    states, cut = P(("rep", "dp"), None, None), P(None, "dp", None)
    return jax.shard_map(step, mesh=mesh, in_specs=(states, states) + (cut,) * 21, out_specs=(P("rep", "dp", None),) * 21, check_vma=False)
```

```python
import functools

import jax
import jax.numpy as jnp
import numpy as np
from jax import lax
from jax.experimental import pallas as pl
from jax.experimental.pallas import tpu as pltpu
from jax.sharding import PartitionSpec as P

MESH = pl.DeviceIdType.MESH
BF, F32 = jnp.bfloat16, jnp.float32
LOG2E = 1.4426950408889634
NEG = -1e30
HEAD = 128
THETA = 10000
ROWS, MORE = 256, 512
PARTS = 5
VMEM = 62 * 2**20


class Place:
    def __init__(self, n, first):
        self.side = next(i for i in range(n) if i * i == n)
        self.me = lax.axis_index("dp")
        self.xy = [lax.div(self.me, self.side), lax.rem(self.me, self.side)]
        self.first = first
        rep = lax.axis_index("rep")
        self.core = lax.rem(rep, 2)
        self.twin = {"rep": rep + 1 - 2 * self.core}

    def block(self, i, j=0):
        s = self.side
        by = (i, j) if self.first == 0 else (j, i)
        x, y = (lax.rem(c + d + s, s) for c, d in zip(self.xy, by))
        return x * s + y

    def near(self, i, j=0):
        return {"dp": self.block(i, j)}

    def around(self):
        return [self.near(*d) for d in ((1, 0), (-1, 0), (0, 1), (0, -1))]


def remote(src, dst, send, recv, device):
    return pltpu.make_async_remote_copy(src_ref=src, dst_ref=dst, send_sem=send, recv_sem=recv, device_id=device, device_id_type=MESH)


def greet(devices):
    bar = pltpu.get_barrier_semaphore()
    for d in devices:
        pl.semaphore_signal(bar, device_id=d, device_id_type=MESH)
    pl.semaphore_wait(bar, len(devices))


TWO, FOUR, THREE = range(2), range(4), range(3)


def each(count, do):
    lax.fori_loop(0, len(count), lambda i, _: do(i), None)


def lower_upper(i):
    return 2 * i - 1


class Gather:
    def __init__(self, n, shard, full, sems):
        m = len(sems) // len(TWO)
        self.ways = [(h, Place(n, h)) + tuple(sems[h * m : (h + 1) * m]) for h in TWO]
        self.place = self.ways[0][1]
        self.n, self.shard, self.full, self.local = n, shard, full, sems[-1]
        self.rows = shard.shape[0]
        self.wide = shard.shape[1] // len(TWO)
        self.by_rows = self.rows % 64 == 0

    def part(self, ref, h, block, q=None):
        i, count = len(TWO) * h + (0 if q is None else q), len(TWO) if q is None else 1
        left = self.place.core * self.wide
        if self.by_rows:
            r = self.rows // len(FOUR)
            return ref.at[pl.ds(pl.multiple_of(block * self.rows + i * r, r), count * r), pl.ds(pl.multiple_of(left, HEAD), self.wide)]
        c = self.wide // len(FOUR)
        return ref.at[pl.ds(pl.multiple_of(block * self.rows, 8), self.rows), pl.ds(pl.multiple_of(left + i * c, HEAD), count * c)]

    def send(self, h, block, device, sent, recv, q=None, src=None):
        here = self.part(self.full, h, block, q)
        remote(here if src is None else src, here, sent, recv, device).start()

    def bytes_of(self, quarters):
        if self.by_rows:
            return self.full.at[pl.ds(0, quarters * self.rows // len(FOUR)), pl.ds(0, self.wide)]
        return self.full.at[pl.ds(0, quarters // len(TWO) * self.rows), pl.ds(0, self.wide // len(TWO))]

    def wait(self, sent, recv, quarters):
        some = self.bytes_of(quarters) if quarters % len(TWO) == 0 or self.by_rows else self.full.at[pl.ds(0, quarters * self.rows), pl.ds(0, self.wide // len(FOUR))]
        each(TWO, lambda i: remote(some, some, sent, recv.at[i], self.place.twin).wait_recv())

    def hand(self, h, over, here, block):
        part = self.part(self.full, h, block)
        remote(part, part, over, here, self.place.twin).start()

    def keep(self):
        return pltpu.make_async_copy(self.shard, self.full.at[pl.ds(pl.multiple_of(self.place.me * self.rows, 8), self.rows)], self.local)

    def go0(self):
        for h, p, sent, x1, x2, y1, y2, z1, z2, over, here in self.ways:
            each(TWO, lambda i: self.send(h, p.me, p.near(lower_upper(i)), sent, x1.at[i], src=self.part(self.shard, h, 0)))
        self.keep().start()

    def go1(self):
        self.keep().wait()
        for h, p, sent, x1, x2, y1, y2, z1, z2, over, here in self.ways:
            self.wait(sent, x1, len(TWO))

            def side(i):
                d = lower_upper(i)
                self.send(h, p.block(-d), p.near(d), sent, x2.at[i], i)
                each(THREE, lambda b: self.send(h, p.block(b - 1), p.near(0, d), sent, y1.at[i]))
                self.hand(h, over, here, p.block(d))

            each(TWO, side)

    def go2(self):
        for h, p, sent, x1, x2, y1, y2, z1, z2, over, here in self.ways:
            self.wait(sent, x2, 1)
            each(TWO, lambda i: self.send(h, p.block(2), p.near(0, lower_upper(i)), sent, z1.at[i]))
            self.wait(sent, y1, len(TWO) * len(THREE))

            def side(i):
                d = lower_upper(i)

                def one(b):
                    self.send(h, p.block(b - 1, -d), p.near(0, d), sent, y2.at[i], i)
                    self.hand(h, over, here, p.block(b - 1, d))

                each(THREE, one)

            each(TWO, side)
            self.hand(h, over, here, p.block(2))

    def go3(self):
        for h, p, sent, x1, x2, y1, y2, z1, z2, over, here in self.ways:
            self.wait(sent, z1, len(TWO))

            def side(i):
                d = lower_upper(i)
                self.send(h, p.block(2, -d), p.near(0, d), sent, z2.at[i], i)
                self.hand(h, over, here, p.block(2, d))

            each(TWO, side)
            self.wait(sent, y2, len(THREE))
            each(THREE, lambda b: self.hand(h, over, here, p.block(b - 1, 2)))

    def go4(self):
        for h, p, sent, x1, x2, y1, y2, z1, z2, over, here in self.ways:
            self.wait(sent, z2, 1)
            self.hand(h, over, here, p.block(2, 2))
        some = self.bytes_of(len(TWO) * (self.n - 1))
        for h, p, sent, x1, x2, y1, y2, z1, z2, over, here in self.ways:
            remote(some, some, sent, here, p.twin).wait()
            remote(some, some, over, here, p.twin).wait_send()


def gather_sems():
    dma = pltpu.SemaphoreType.DMA
    return ([dma] + [dma((len(TWO),))] * 6 + [dma] * len(TWO)) * len(TWO) + [dma]


def chunk(n, shape):
    rows = shape[0] // n
    return (rows // 4, shape[1]) if rows % 64 == 0 else (rows, shape[1] // 4)


def scatter_scratch(n, shape):
    c, two, four = chunk(n, shape), (len(TWO),), (len(FOUR),)
    dma = pltpu.SemaphoreType.DMA
    one = [pltpu.VMEM(k + c, BF) for k in (two + four, two + two + four, two, two + two, two + four)] + [dma(k) for k in (two, two + two, two, two + two, two)] + [dma] * len(TWO)
    return one * len(TWO) + [pltpu.SemaphoreType.REGULAR]


def tiles(x):
    r, c = x.shape
    return sum(x[a : a + 8, b : b + HEAD] for a in range(0, r, 8) for b in range(0, c, HEAD))


class Scatter:
    def __init__(self, n, grad, out, squares, scratch, again):
        m = len(scratch) // len(TWO)
        self.ways = [(Place(n, h), h) + tuple(scratch[h * m : (h + 1) * m]) for h in TWO]
        self.grad, self.out, self.squares, self.again, self.free = grad, out, squares, again, scratch[-1]
        self.rows = grad.shape[0] // n
        self.chunk = chunk(n, grad.shape)
        self.by_rows = self.chunk[0] < self.rows

    def part(self, ref, block, quarter):
        r, c = self.chunk
        if self.by_rows:
            return ref.at[pl.ds(pl.multiple_of(block * self.rows + quarter * r, r), r), pl.ds(0, c)]
        return ref.at[pl.ds(pl.multiple_of(block * r, 8), r), pl.ds(pl.multiple_of(quarter * c, HEAD), c)]

    def add(self, into, *terms):
        r, c = self.chunk
        w = next(w for w in (1280, c) if c % w == 0)

        def some(i, _):
            at = pl.ds(pl.multiple_of(i * w, HEAD), w)
            into[:, at] = functools.reduce(lambda a, b: a + b, [t[:, at].astype(F32) for t in terms]).astype(BF)

        lax.fori_loop(0, c // w, some, None)

    def fetch(self, p, h, mine, sm, q, i, j):
        return pltpu.make_async_copy(self.part(self.grad, p.block(i, j), len(TWO) * h + q), mine.at[q, j], sm.at[q])

    def go0(self):
        if self.again:
            pl.semaphore_wait(self.free, len(FOUR))
        for p, h, a, b, c, d, mine, sa, sb, sc, sd, sm, send, kept in self.ways:
            each(TWO, lambda q: each(FOUR, lambda j: remote(self.part(self.grad, p.block(2, j), len(TWO) * h + q), a.at[q, j], send, sa.at[q], p.near(-lower_upper(q))).start()))
        for p, h, a, b, c, d, mine, sa, sb, sc, sd, sm, send, kept in self.ways:
            def quarter(q):
                s = -lower_upper(q)

                def one(j):
                    remote(self.part(self.grad, p.block(s, j), len(TWO) * h + 1 - q), b.at[q, 1 - q, j], send, sb.at[q, 1 - q], p.near(s)).start()
                    self.fetch(p, h, mine, sm, q, s, j).start()

                each(FOUR, one)

            each(TWO, quarter)

    def go1(self):
        for p, h, a, b, c, d, mine, sa, sb, sc, sd, sm, send, kept in self.ways:
            def quarter(q):
                s = -lower_upper(q)
                remote(a.at[q], a.at[q], send, sa.at[q], p.near(s)).wait_recv()
                pltpu.make_async_copy(mine.at[q], mine.at[q], sm.at[q]).wait()
                each(FOUR, lambda j: self.add(a.at[q, j], a.at[q, j], mine.at[q, j]))

                def one(j):
                    self.fetch(p, h, mine, sm, q, 0, j).start()
                    remote(a.at[q, j], b.at[q, q, j], send, sb.at[q, q], p.near(s)).start()

                each(FOUR, one)

            each(TWO, quarter)

    def go2(self):
        for p, h, a, b, c, d, mine, sa, sb, sc, sd, sm, send, kept in self.ways:
            def ready(q):
                pltpu.make_async_copy(mine.at[q], mine.at[q], sm.at[q]).wait()
                each(TWO, lambda i: remote(b.at[i, q], b.at[i, q], send, sb.at[i, q], p.near(1)).wait_recv())

            each(TWO, ready)

            def quarter(q):
                s = -lower_upper(q)

                def term(k, j, to, sem):
                    self.add(b.at[0, k, j], mine.at[k, j], b.at[0, k, j], b.at[1, k, j])
                    remote(b.at[0, k, j], to, send, sem, p.near(0, s)).start()

                term(q, 2, c.at[q], sc.at[q])
                term(1 - q, 1 + 2 * q, d.at[q, 1 - q], sd.at[q, 1 - q])

            each(TWO, quarter)

    def go3(self):
        for p, h, a, b, c, d, mine, sa, sb, sc, sd, sm, send, kept in self.ways:
            def quarter(q):
                s, j = -lower_upper(q), 1 + 2 * q
                remote(c.at[q], c.at[q], send, sc.at[q], p.near(0, s)).wait_recv()
                self.add(c.at[q], c.at[q], mine.at[q, j], b.at[0, q, j], b.at[1, q, j])
                remote(c.at[q], d.at[q, q], send, sd.at[q, q], p.near(0, s)).start()

            each(TWO, quarter)

    def go4(self):
        for p, h, a, b, c, d, mine, sa, sb, sc, sd, sm, send, kept in self.ways:
            def quarter(q):
                each(TWO, lambda i: remote(d.at[i, q], d.at[i, q], send, sd.at[i, q], p.near(1)).wait_recv())
                own = mine.at[q, 0]
                self.add(own, own, b.at[0, q, 0], b.at[1, q, 0], d.at[0, q], d.at[1, q])

                def some(i, _):
                    x = own[:, pl.ds(pl.multiple_of(i * HEAD, HEAD), HEAD)].astype(F32)
                    self.squares[...] += tiles(x * x)

                lax.fori_loop(0, self.chunk[1] // HEAD, some, None)
                pltpu.make_async_copy(own, self.part(self.out, 0, len(TWO) * h + q), kept).start()

            each(TWO, quarter)

    def end(self):
        for p, h, a, b, c, d, mine, sa, sb, sc, sd, sm, send, kept in self.ways:
            for x in (a, b, c, mine.at[0]):
                remote(x, x, send, sa.at[0], p.near(1)).wait_send()
            pltpu.make_async_copy(c, c, kept).wait()
        if not self.again:
            for d in self.ways[0][0].around():
                pl.semaphore_signal(self.free, device_id=d, device_id_type=MESH)


def then(*steps):
    def do():
        for step in steps:
            step()

    return do


def when(*events):
    def tick(i):
        for place, do in events:
            pl.when(i == place)(do)

    return tick


def dot(a, b, ca, cb):
    return lax.dot_general(a, b, (((ca,), (cb,)), ((), ())), preferred_element_type=F32)


def nn(a, b):
    return dot(a, b, 1, 0)


def nt(a, b):
    return dot(a, b, 1, 1)


def row(i):
    return i, 0


def col(j):
    return 0, j


def whole(*_):
    return 0, 0


def run(body, grid, ins, outs, scratch=(), tick=None):
    held = [(r, late) for r, block, late in ins if block is None]
    tiled = [x for x in ins if x[1] is not None]

    def inner(sem, *refs):
        full, rest = refs[: len(held)], refs[len(held) :]
        early, late = ([pltpu.make_async_copy(r, v, sem.at[i]) for i, ((r, k), v) in enumerate(zip(held, full)) if bool(k) == want] for want in (False, True))
        for c in early:
            c.start()

        def step(*tiles):
            @pl.when(functools.reduce(lambda p, q: p & q, [pl.program_id(i) == 0 for i in range(len(grid))]))
            def _():
                for c in late:
                    c.start()
                for c in early:
                    c.wait()

            if late:
                @pl.when(pl.program_id(0) == grid[0] - 1)
                def _():
                    for c in late:
                        c.wait()

            some, more, given = iter(tiles), iter(full), []
            for _, block, _ in ins:
                given.append(next(more) if block is None else next(some))
            body(*given, *some, *rest, tick or (lambda i: None))

        specs = lambda arrays: [pl.BlockSpec(block, at) for _, block, at in arrays]
        pltpu.emit_pipeline(step, grid=grid, in_specs=specs(tiled), out_specs=specs(outs))(*[r for r, _, _ in tiled], *[r for r, _, _ in outs])

    pl.run_scoped(inner, pltpu.SemaphoreType.DMA((max(len(held), 1),)), *[pltpu.VMEM(r.shape, r.dtype) for r, _ in held], *scratch)


def all_of(ref):
    return ref, None, None


def rows_of(ref):
    return ref, (ROWS, ref.shape[1]), row


def cols_of(ref, parts):
    return ref, (ref.shape[0], ref.shape[1] // parts), col


def in_rows(size, body, tick):
    n = size // MORE

    def one(i, _):
        body(pl.ds(pl.multiple_of(i * MORE, MORE), MORE))
        tick(pl.program_id(0) * n + i)

    lax.fori_loop(0, n, one, None)


def unit(h):
    return lax.rsqrt(jnp.mean(h * h, -1, keepdims=True) + 1e-6)


def normed(h):
    h = h.astype(F32)
    return (h * unit(h)).astype(BF)


def norm_back(h, d):
    h = h.astype(F32)
    s = unit(h)
    return (s * d - h * (s * s * s * jnp.mean(h * d, -1, keepdims=True))).astype(BF)


def rotary(tokens):
    half = HEAD // 2
    angle = np.arange(tokens, dtype=F32)[:, None] * np.power(np.float32(THETA), -np.arange(half, dtype=F32) / half)
    c, s = np.cos(angle), np.sin(angle)
    return jnp.asarray(np.concatenate([c, c], 1)), jnp.asarray(np.concatenate([-s, s], 1))


def heads_of(ref, g):
    return [ref[:, n * HEAD : (n + 1) * HEAD] for n in range(g)]


def qkv_body(h_ref, w_ref, c_ref, s_ref, a_ref, o_ref, tick, *, turned):
    a = normed(h_ref[...])
    a_ref[...] = a
    r = nn(a, w_ref[...]).astype(BF)
    for n in range(r.shape[1] // HEAD):
        at = slice(n * HEAD, (n + 1) * HEAD)
        x = r[:, at]
        if n < turned:
            x = x.astype(F32)
            x = (x * c_ref[...] + pltpu.roll(x, HEAD // 2, 1) * s_ref[...]).astype(BF)
        o_ref[:, at] = x
    tick(pl.program_id(0))


def qkv(h, w, cos, sin, kv, a, x, tick):
    run(functools.partial(qkv_body, turned=w.shape[1] // HEAD - kv), (h.shape[0] // ROWS,), [rows_of(h), all_of(w), rows_of(cos), rows_of(sin)],
        [rows_of(a), rows_of(x)], tick=tick)


def out_body(h_ref, x_ref, w_ref, m_ref, b_ref, tick):
    m = h_ref[...] + nn(x_ref[...], w_ref[...]).astype(BF)
    m_ref[...] = m
    b_ref[...] = normed(m)
    tick(pl.program_id(0))


def out_proj(h, o, w, m, b, tick):
    run(out_body, (h.shape[0] // ROWS,), [rows_of(h), rows_of(o), all_of(w)], [rows_of(m), rows_of(b)], tick=tick)


def gu_body(b_ref, w_ref, g_ref, m_ref, tick):
    half = m_ref.shape[1]

    def tile(at):
        r = nn(b_ref[at, :], w_ref[...])
        g_ref[at, :] = r
        g = r[:, :half]
        m_ref[at, :] = (g * jax.nn.sigmoid(g) * r[:, half:]).astype(BF)

    in_rows(b_ref.shape[0], tile, tick)


def gate_up(b, w, gu, mid, tick):
    run(gu_body, (PARTS,), [all_of(b), cols_of(w, PARTS)], [cols_of(gu, PARTS), cols_of(mid, PARTS)], tick=tick)


def down_body(h_ref, m_ref, w_ref, o_ref, tick):
    o_ref[...] = h_ref[...] + nn(m_ref[...], w_ref[...]).astype(BF)
    tick(pl.program_id(0))


def down(h, mid, w, out, tick):
    run(down_body, (h.shape[0] // ROWS,), [rows_of(h), rows_of(mid), all_of(w)], [rows_of(out)], tick=tick)


def visible(iq, j, bq, bk):
    return lax.broadcasted_iota(jnp.int32, (bk, bq), 1) - lax.broadcasted_iota(jnp.int32, (bk, bq), 0) >= j * bk - iq * bq


def key_blocks(iq, total, bq, bk, block, tick):
    full, m = iq * bq // bk, bq // bk
    before = pl.program_id(0) * m * (pl.num_programs(1) * (pl.num_programs(1) + 1) // 2) + m * (iq * (iq + 1) // 2)

    def one(j, masked):
        block(j, masked)
        tick(before + j)

    def seen(j, _):
        @pl.when(j < full)
        def _():
            one(j, False)

        @pl.when((j >= full) & (j < full + m))
        def _():
            one(j, True)

    lax.fori_loop(0, total // bk, seen, None)


def fwd_body(q_ref, k_ref, v_ref, o_ref, lse_ref, top_s, mix_s, tick, *, scale, bk):
    bq, g = q_ref.shape[0], q_ref.shape[1] // HEAD
    iq = pl.program_id(1)
    e = scale * LOG2E
    top_s[...] = jnp.full(top_s.shape, NEG, F32)
    mix_s[...] = jnp.zeros(mix_s.shape, F32)
    ones = jnp.ones((8, bk), BF)

    def block(j, masked):
        here = pl.ds(pl.multiple_of(j * bk, bk), bk)
        k = k_ref[here, :]
        scores = [nt(k, q) for q in heads_of(q_ref, g)]
        values = jnp.concatenate([v_ref[here, :].T, ones], axis=0)
        weights, keeps = [], []
        for n, s in enumerate(scores):
            if masked:
                s = jnp.where(visible(iq, j, bq, bk), s, 2 * NEG)
            mine = slice(n, n + 1)
            old = top_s[mine, :]
            top = jnp.maximum(old, s.max(axis=0, keepdims=True))
            top_s[mine, :] = top
            weights.append(jnp.exp2((s - top) * e).astype(BF))
            keeps.append(jnp.exp2((old - top) * e))
        for n in range(g):
            mix_s[n] = mix_s[n] * keeps[n] + nn(values, weights[n])

    key_blocks(iq, k_ref.shape[0], bq, bk, block, tick)
    for n in range(g):
        mine = slice(n, n + 1)
        total = mix_s[n, HEAD : HEAD + 1, :]
        o_ref[:, n * HEAD : (n + 1) * HEAD] = (mix_s[n, :HEAD, :] * (1 / total)).T.astype(BF)
        lse_ref[0, mine, :] = top_s[mine, :] * scale + jnp.log(total)


def attention_specs(x, kv, bq):
    t, n = x.shape
    heads = n // HEAD - 2 * kv
    g = heads // kv
    return (bq, g * HEAD), [(x, (bq, g * HEAD), lambda c, i: (i, c)), (x, (t, HEAD), lambda c, i: (0, heads + c)), (x, (t, HEAD), lambda c, i: (0, heads + kv + c))], \
        lambda ref: (ref, (1, g, bq), lambda c, i: (c, 0, i))


def attend(x, kv, o, lse, tick, bq=MORE, bk=MORE):
    tile, ins, stat = attention_specs(x, kv, bq)
    run(functools.partial(fwd_body, scale=HEAD**-0.5, bk=bk), (kv, x.shape[0] // bq), ins, [(o, tile, lambda c, i: (i, c)), stat(lse)],
        [pltpu.VMEM((8, bq), F32), pltpu.VMEM((tile[1] // HEAD, HEAD + 8, bq), F32)], tick)


def bwd_body(q_ref, k_ref, v_ref, do_ref, lse_ref, delta_ref, c_ref, s_ref, dq_ref, dk_ref, dv_ref, dq_s, dk_s, dv_s, tick, *, scale, bk):
    bq, g = q_ref.shape[0], q_ref.shape[1] // HEAD
    iq = pl.program_id(1)
    e = scale * LOG2E

    @pl.when(iq == 0)
    def _():
        dk_s[...] = jnp.zeros_like(dk_s)
        dv_s[...] = jnp.zeros_like(dv_s)

    dq_s[...] = jnp.zeros_like(dq_s)

    def block(j, masked):
        here = pl.ds(pl.multiple_of(j * bk, bk), bk)
        k, v = k_ref[here, :], v_ref[here, :]
        back = k.T
        qs, dos = heads_of(q_ref, g), heads_of(do_ref, g)
        scores = [nt(k, x) for x in qs]
        dps = [nt(v, x) for x in dos]
        for n in range(g):
            mine = slice(n, n + 1)
            p = jnp.exp2(scores[n] * e - lse_ref[0, mine, :] * LOG2E)
            if masked:
                p = jnp.where(visible(iq, j, bq, bk), p, 0.0)
            ds = (p * (dps[n] - delta_ref[0, mine, :])).astype(BF)
            dv_s[here, :] += nn(p.astype(BF), dos[n])
            dk_s[here, :] += nn(ds, qs[n])
            dq_s[n] += nn(back, ds)

    key_blocks(iq, k_ref.shape[0], bq, bk, block, tick)

    def unturned(d, at):
        d = d.astype(BF).astype(F32)
        return (d * c_ref[at, :] - pltpu.roll(d, HEAD // 2, 1) * s_ref[at, :]).astype(BF)

    for n in range(g):
        dq_ref[:, n * HEAD : (n + 1) * HEAD] = unturned((dq_s[n] * scale).T, pl.ds(pl.multiple_of(iq * bq, bq), bq))

    @pl.when(iq == pl.num_programs(1) - 1)
    def _():
        dk_ref[...] = unturned(dk_s[...] * scale, slice(None))
        dv_ref[...] = dv_s[...].astype(BF)


def attend_back(x, do, lse, delta, cos, sin, kv, dq, dk, dv, tick, bq=MORE, bk=MORE):
    tile, ins, stat = attention_specs(x, kv, bq)
    t = x.shape[0]
    mine = lambda ref: (ref, (t, HEAD), lambda c, i: (0, c))
    run(functools.partial(bwd_body, scale=HEAD**-0.5, bk=bk), (kv, t // bq), ins + [(do, tile, lambda c, i: (i, c)), stat(lse), stat(delta), all_of(cos), all_of(sin)],
        [(dq, tile, lambda c, i: (i, c)), mine(dk), mine(dv)], [pltpu.VMEM((tile[1] // HEAD, HEAD, bq), F32)] + [pltpu.VMEM((t, HEAD), F32)] * 2, tick)


def silu_back(g, u, d):
    s = jax.nn.sigmoid(g)
    silu = g * s
    return (silu * u).astype(BF), (d * u * (s + silu * (1 - s))).astype(BF), (d * silu).astype(BF)


def dgu_body(dy_ref, w_ref, g_ref, dg_ref, dw_ref, mid_s, tick):
    half = mid_s.shape[1]

    def tile(at):
        d = nt(dy_ref[at, :], w_ref[...]).astype(BF).astype(F32)
        mid_s[at, :], dg_ref[at, :half], dg_ref[at, half:] = silu_back(g_ref[at, :half], g_ref[at, half:], d)

    in_rows(dy_ref.shape[0], tile, tick)
    dw_ref[...] = dot(mid_s[...], dy_ref[...], 0, 0).astype(BF)


def dgu(dy, wd, gu, dg, dwd, tick):
    t, c = dy.shape[0], wd.shape[0] // PARTS
    rows = lambda ref: (ref, (c, ref.shape[1]), row)
    run(dgu_body, (PARTS,), [all_of(dy), rows(wd), cols_of(gu, PARTS)], [cols_of(dg, PARTS), rows(dwd)], [pltpu.VMEM((t, c), BF)], tick)


def last_body(dy_ref, wd_ref, b_ref, w_ref, dg_ref, dw_ref, mid_s, tick):
    half = mid_s.shape[1]

    def tile(at):
        r = nn(b_ref[at, :], w_ref[...])
        d = nt(dy_ref[at, :], wd_ref[...]).astype(BF).astype(F32)
        mid_s[at, :], dg_ref[at, :half], dg_ref[at, half:] = silu_back(r[:, :half], r[:, half:], d)

    in_rows(dy_ref.shape[0], tile, tick)
    dw_ref[...] = dot(mid_s[...], dy_ref[...], 0, 0).astype(BF)


def last_dgu(dy, wd, b, wgu, dg, dwd, tick):
    t, c = dy.shape[0], wd.shape[0] // PARTS
    rows = lambda ref: (ref, (c, ref.shape[1]), row)
    run(last_body, (PARTS,), [all_of(dy), rows(wd), all_of(b), cols_of(wgu, PARTS)], [cols_of(dg, PARTS), rows(dwd)], [pltpu.VMEM((t, c), BF)], tick)


def dw_body(a_ref, d_ref, o_ref, at_s, tick):
    @pl.when(pl.program_id(0) == 0)
    def _():
        at_s[...] = a_ref[...].T

    def tile(at):
        o_ref[at, :] = nn(at_s[at, :], d_ref[...]).astype(BF)

    in_rows(at_s.shape[0], tile, tick)


def dw(a, d, out, parts, tick):
    run(dw_body, (parts,), [all_of(a), cols_of(d, parts)], [cols_of(out, parts)], [pltpu.VMEM(a.shape[::-1], BF)], tick)


def db_body(dg_ref, w_ref, dy_ref, h_ref, o_ref, acc, tick):
    j = pl.program_id(0)
    end = pl.num_programs(0) - 1

    def tile(at):
        r = nt(dg_ref[at, :], w_ref[...])

        @pl.when(j == 0)
        def _():
            acc[at, :] = r

        @pl.when((j > 0) & (j < end))
        def _():
            acc[at, :] += r

        @pl.when(j == end)
        def _():
            o_ref[at, :] = dy_ref[at, :] + norm_back(h_ref[at, :], (acc[at, :] + r).astype(BF).astype(F32))

    in_rows(dy_ref.shape[0], tile, tick)


def db(dg, wgu, dy, h, out, tick):
    run(db_body, (PARTS,), [cols_of(dg, PARTS), cols_of(wgu, PARTS), (dy, None, True), (h, None, True)], [(out, out.shape, whole)], [pltpu.VMEM(dy.shape, F32)], tick)


def do_body(d_ref, w_ref, o_ref, do_ref, delta_ref, tick):
    r = nt(d_ref[...], w_ref[...]).astype(BF)
    do_ref[...] = r
    kv, g = delta_ref.shape[:2]
    for n in range(kv * g):
        at = slice(n * HEAD, (n + 1) * HEAD)
        x = r[:, at].astype(F32) * o_ref[:, at].astype(F32)
        delta_ref[n // g, n % g : n % g + 1, :] = jnp.sum(x.T, axis=0, keepdims=True)
    tick(pl.program_id(0))


def do_delta(d, wo, o, do, delta, tick):
    run(do_body, (d.shape[0] // ROWS,), [rows_of(d), all_of(wo), rows_of(o)], [rows_of(do), (delta, delta.shape[:2] + (ROWS,), lambda i: (0, 0, i))], tick=tick)


def da_body(dq_ref, dk_ref, dv_ref, w_ref, d_ref, h_ref, o_ref, tick):
    n, m = dq_ref.shape[1], dk_ref.shape[1]
    r = nt(dq_ref[...], w_ref[:, :n]) + nt(dk_ref[...], w_ref[:, n : n + m]) + nt(dv_ref[...], w_ref[:, n + m :])
    o_ref[...] = d_ref[...] + norm_back(h_ref[...], r.astype(BF).astype(F32))
    tick(pl.program_id(0))


def da(dq, dk, dv, w, d, h, out, tick):
    run(da_body, (d.shape[0] // ROWS,), [rows_of(dq), rows_of(dk), rows_of(dv), all_of(w), rows_of(d), rows_of(h)], [rows_of(out)], tick=tick)


def dqkv_body(a_ref, dq_ref, dk_ref, dv_ref, o_ref, tick):
    back = a_ref[...].T
    n, m = dq_ref.shape[1], dk_ref.shape[1]
    o_ref[:, :n] = nn(back, dq_ref[...]).astype(BF)
    o_ref[:, n : n + m] = nn(back, dk_ref[...]).astype(BF)
    o_ref[:, n + m :] = nn(back, dv_ref[...]).astype(BF)
    tick(pl.program_id(0))


def dqkv(a, dq, dk, dv, out, tick):
    run(dqkv_body, (a.shape[1] // ROWS,), [(a, (a.shape[0], ROWS), col), all_of(dq), all_of(dk), all_of(dv)], [rows_of(out)], tick=tick)


WAYS = ("a", "gu", "d")
SUMS = ("qkv", "o", "gu", "d")
NAMES = ("wq", "wk", "wv", "wo", "w_gate", "w_up", "w_down")


def named(names, refs):
    return dict(zip(names, refs, strict=True))


def beside(r, kw):
    a = r.shape[1]
    q = a // 2 - kw
    return r.at[:, pl.ds(0, a - q)], r.at[:, pl.ds(a - q, q)]


def mixture(f):
    w = f // PARTS
    return [(i, j * w, (2 * j + i) * w, w) for j in range(PARTS) for i in TWO]


def forward_kernel(n, layers, kv, ins, outs, count, *refs):
    r = named(ins + outs, refs[:count])
    packs, sems = refs[count : count + 2], refs[count + 2 :]
    for l in range(layers):
        at = 0
        for name in NAMES[:4]:
            w = r[name].shape[2]
            packs[0][l, :, at : at + w] = r[name][l]
            at += w
        for i, a, b, w in mixture(r["w_up"].shape[2]):
            packs[1][l, :, b : b + w] = r[NAMES[4 + i]][l, :, a : a + w]
    place = Place(n, 0)
    greet(place.around() + [place.twin])
    per = len(gather_sems())
    pieces = [[Gather(n, p.at[l], r[f"w{w}{l}"], sems[per * (3 * l + i) : per * (3 * l + i + 1)]) for i, (w, p) in enumerate(zip(WAYS, (*packs, r["w_down"])))]
              for l in range(layers)]
    a, gu, dn = pieces[0]
    then(a.go0, gu.go0, dn.go0, a.go1, a.go2, a.go3, gu.go1, dn.go1, a.go4)()
    h = r["x"].at[0]
    for l in range(layers):
        more = l + 1 < layers
        a, gu, dn = pieces[l]
        wqkv, wo = beside(r[f"wa{l}"], kv * HEAD)
        qkv(h, wqkv, r["cos"], r["sin"], kv, r[f"a{l}"], r[f"x{l}"], when())
        attend(r[f"x{l}"], kv, r[f"o{l}"], r[f"lse{l}"], when((1, gu.go2), *([] if more else [(3, dn.go2)])))
        out_proj(h, r[f"o{l}"], wo, r[f"m{l}"], r[f"b{l}"], when((2, gu.go3)))
        if more:
            a2, gu2, dn2 = pieces[l + 1]
            then(dn.go2, a2.go0, gu.go4)()
            gate_up(r[f"b{l}"], r[f"wgu{l}"], r[f"gu{l}"], r[f"mid{l}"], when((1, dn.go3), (2, then(a2.go1, gu2.go0, dn2.go0)), (3, dn.go4), (7, a2.go2)))
            down(r[f"m{l}"], r[f"mid{l}"], r[f"wd{l}"], r[f"h{l + 1}"], when((0, then(a2.go3, gu2.go1, dn2.go1))))
            a2.go4()
            h = r[f"h{l + 1}"]
        else:
            then(dn.go3, gu.go4, dn.go4)()


def backward_kernel(n, layers, kv, ins, outs, count, *refs):
    r = named(ins + outs, refs[:count])
    squares, slots, send, recv = refs[count : count + 4]
    held = refs[count + 4 :]
    place = Place(n, 0)
    others = [{"dp": lax.rem(place.me + i, n)} for i in range(1, n)]
    greet(others)
    squares[...] = jnp.zeros_like(squares)

    per = len(held) // len(SUMS)

    def piece(l, w):
        i = per * SUMS.index(w)
        return Scatter(n, r[f"t{w}{l}"], r[f"g{w}{l}"], squares, held[i : i + per], l + 1 < layers)

    d = r["dy"].at[0]
    before = []
    for l in reversed(range(layers)):
        p, o, gu, dn = (piece(l, w) for w in SUMS)
        if before:
            p1, o1, gu1, dn1 = before
            dgu(d, r[f"wd{l}"], r[f"gu{l}"], r["dg"], r[f"td{l}"], when((0, p1.go1), (2, then(o1.go3, gu1.go4)), (4, then(o1.go4, p1.go2)), (6, p1.go3), (8, p1.go4)))
        else:
            last_dgu(d, r[f"wd{l}"], r[f"b{l}"], r[f"wgu{l}"], r["dg"], r[f"td{l}"], when())
        wqkv, wo = beside(r[f"wa{l}"], kv * HEAD)
        then(*[q.end for q in before], dn.go0)()
        dw(r[f"b{l}"], r["dg"], r[f"tgu{l}"], PARTS, when((5, dn.go1)))
        gu.go0()
        db(r["dg"], r[f"wgu{l}"], d, r[f"m{l}"], r["dm"], when((3, dn.go2)))
        do_delta(r["dm"], wo, r[f"o{l}"], r["do"], r["delta"], when((1, gu.go1)))
        dw(r[f"o{l}"], r["dm"], r[f"to{l}"], 2, when())
        o.go0()
        attend_back(r[f"x{l}"], r["do"], r[f"lse{l}"], r["delta"], r["cos"], r["sin"], kv, r["dq"], r["dk"], r["dv"], when((3, dn.go3)))
        dqkv(r[f"a{l}"], r["dq"], r["dk"], r["dv"], r[f"tqkv{l}"], when((0, gu.go2), (1, o.go1), (3, dn.go4)))
        p.go0()
        if l:
            da(r["dq"], r["dk"], r["dv"], wqkv, r["dm"], r[f"h{l}"], r[f"d{l}"], when((2, gu.go3), (3, o.go2)))
            d = r[f"d{l}"]
        else:
            then(gu.go3, o.go2, p.go1, o.go3, gu.go4, p.go2, o.go4, p.go3, p.go4)()
        before = [p, o, gu, dn]
    then(*[q.end for q in before])()
    copies = [remote(squares, slots.at[i], send.at[i], recv.at[i], p) for i, p in enumerate(others)]
    for c in copies:
        c.start()
    for c in copies:
        c.wait()
    t = squares[...] + sum(slots[i] for i in range(n - 1))
    r["total"][...] = jnp.broadcast_to(jnp.sum(jnp.sum(t, axis=1, keepdims=True), axis=0, keepdims=True), t.shape)


def kernel(body, name, number, given, made, in_vmem, scratch):
    space = lambda name: pl.BlockSpec(memory_space=pltpu.VMEM if name in in_vmem else pl.ANY)
    got = pl.pallas_call(
        functools.partial(body, tuple(given), tuple(made), len(given) + len(made)),
        in_specs=[space(k) for k in given],
        out_specs=[space(k) for k in made],
        out_shape=[jax.ShapeDtypeStruct(*s) for s in made.values()],
        scratch_shapes=scratch,
        compiler_params=pltpu.CompilerParams(collective_id=number, has_side_effects=True, vmem_limit_bytes=VMEM),
        name=name,
    )(*given.values())
    return dict(zip(made, got, strict=True))


def adamw(w, m, v, g):
    m = 0.9 * m + 0.1 * g
    v = 0.95 * v + 0.05 * g * g
    step = m * lax.rsqrt(v + 1e-8) + 0.1 * w
    return (w - 0.02 * step).astype(BF), m, v


def step_kernel(count, layers, total_ref, *refs):
    m, k = len(SUMS), len(NAMES)
    grads, refs = refs[: m * layers], refs[m * layers :]
    olds, news = refs[: 3 * k], refs[3 * k :]
    factor = jnp.minimum(1.0, 0.5 * lax.rsqrt(total_ref[:1, :1] / count + 1e-30))
    for l in range(layers):
        @pl.when(pl.program_id(0) == l)
        def _():
            p, o, gu, d = grads[m * l : m * l + m]
            q, w = olds[0].shape[2], olds[1].shape[2]
            wide = o.shape[1]
            moves = [(0, p, 0, 0, q), (1, p, 0, q, w), (2, p, 0, q + w, w), (3, o, 0, 0, wide), (k - 1, d, 0, 0, wide)]
            for i, g, to, at, w in moves + [(4 + i, gu, to, at, w) for i, to, at, w in mixture(olds[4].shape[2])]:
                def some(c, _):
                    here, there = (pl.ds(pl.multiple_of(x + c * HEAD, HEAD), HEAD) for x in (to, at))
                    three = (i, i + k, i + 2 * k)
                    new = adamw(*[olds[j][0, :, here].astype(F32) for j in three], g[:, there].astype(F32) * factor)
                    for j, x in zip(three, new):
                        news[j][0, :, here] = x

                lax.fori_loop(0, w // HEAD, some, None)


def optimizer(n, total, grads, arrays):
    layers = arrays[0].shape[0]
    tile = lambda a: pl.BlockSpec((1,) + a.shape[1:], lambda l: (l, 0, 0))
    held = pl.BlockSpec(memory_space=pltpu.VMEM)
    return pl.pallas_call(
        functools.partial(step_kernel, n * sum(a.size for a in arrays[:7]), layers),
        grid=(layers,),
        in_specs=[held] * (1 + len(grads)) + [tile(a) for a in arrays],
        out_specs=[tile(a) for a in arrays],
        out_shape=[jax.ShapeDtypeStruct(a.shape, a.dtype) for a in arrays],
        compiler_params=pltpu.CompilerParams(dimension_semantics=("arbitrary",), vmem_limit_bytes=VMEM),
        name="optimizer",
    )(total, *grads, *arrays)


def solution(mesh):
    n = mesh.shape["dp"]

    def step(x, dy, *arrays):
        weights = named(NAMES, arrays[:7])
        layers, _, kw = weights["wk"].shape
        kv = kw // HEAD
        t, d = x.shape[1:]
        q, f = weights["wq"].shape[2], weights["w_up"].shape[2]
        cos, sin = rotary(t)
        shapes = {"a": (d, 2 * q + 2 * kw), "qkv": (d, q + 2 * kw), "o": (q, d), "gu": (d, 2 * f), "d": (f, d)}
        made = {}
        for l in range(layers):
            made |= {f"w{w}{l}": (shapes[w], BF) for w in WAYS}
            made |= {f"a{l}": ((t, d), BF), f"x{l}": ((t, q + 2 * kw), BF), f"o{l}": ((t, q), BF), f"lse{l}": ((kv, q // kw, t), F32),
                     f"m{l}": ((t, d), BF), f"b{l}": ((t, d), BF)}
            if l + 1 < layers:
                made |= {f"gu{l}": ((t, 2 * f), F32), f"mid{l}": ((t, f), BF), f"h{l + 1}": ((t, d), BF)}
        shards = [pltpu.VMEM((layers, shapes[w][0] // n, shapes[w][1]), BF) for w in WAYS[:2]]
        kept = kernel(functools.partial(forward_kernel, n, layers, kv), "forward", 0, {"x": x, "cos": cos, "sin": sin, **weights}, made, NAMES,
                      shards + gather_sems() * (len(WAYS) * layers))
        given = {"dy": dy, "cos": cos, "sin": sin, **{k: a for k, a in kept.items() if not k.startswith("mid")}}
        made = {"dg": ((t, 2 * f), BF), "do": ((t, q), BF), "delta": ((kv, q // kw, t), F32), "dm": ((t, d), BF), "dq": ((t, q), BF), "dk": ((t, kw), BF), "dv": ((t, kw), BF),
                "total": ((8, HEAD), F32)}
        for l in range(layers):
            made |= {f"t{w}{l}": (shapes[w], BF) for w in SUMS} | {f"g{w}{l}": ((shapes[w][0] // n, shapes[w][1]), BF) for w in SUMS} | {f"d{l}": ((t, d), BF)}
        scratch = [pltpu.VMEM((8, HEAD), F32), pltpu.VMEM((n - 1, 8, HEAD), F32)] + [pltpu.SemaphoreType.DMA((n - 1,))] * 2
        got = kernel(functools.partial(backward_kernel, n, layers, kv), "backward", 1, given, made, ["total"], sum([scatter_scratch(n, shapes[w]) for w in SUMS], scratch))
        return tuple(optimizer(n, got["total"], [got[f"g{w}{l}"] for l in range(layers) for w in SUMS], arrays))

    states, cut = P(("rep", "dp"), None, None), P(None, "dp", None)
    return jax.shard_map(step, mesh=mesh, in_specs=(states, states) + (cut,) * 21, out_specs=(P("rep", "dp", None),) * 21, check_vma=False)
```

```python
import functools

import jax
import jax.numpy as jnp
import numpy as np
from jax import lax
from jax.experimental import pallas as pl
from jax.experimental.pallas import tpu as pltpu
from jax.sharding import PartitionSpec as P

MESH = pl.DeviceIdType.MESH
BF, F32 = jnp.bfloat16, jnp.float32
LOG2E = 1.4426950408889634
NEG = -1e30
HEAD = 128
THETA = 10000
ROWS, MORE = 256, 512
PARTS = 5
VMEM = 62 * 2**20


class Place:
    def __init__(self, n, first):
        self.side = next(i for i in range(n) if i * i == n)
        self.me = lax.axis_index("dp")
        self.xy = [lax.div(self.me, self.side), lax.rem(self.me, self.side)]
        self.first = first
        rep = lax.axis_index("rep")
        self.core = lax.rem(rep, 2)
        self.twin = {"rep": rep + 1 - 2 * self.core}

    def block(self, i, j=0):
        s = self.side
        by = (i, j) if self.first == 0 else (j, i)
        x, y = (lax.rem(c + d + s, s) for c, d in zip(self.xy, by))
        return x * s + y

    def near(self, i, j=0):
        return {"dp": self.block(i, j)}

    def around(self):
        return [self.near(*d) for d in ((1, 0), (-1, 0), (0, 1), (0, -1))]


def remote(src, dst, send, recv, device):
    return pltpu.make_async_remote_copy(src_ref=src, dst_ref=dst, send_sem=send, recv_sem=recv, device_id=device, device_id_type=MESH)


def greet(devices):
    bar = pltpu.get_barrier_semaphore()
    for d in devices:
        pl.semaphore_signal(bar, device_id=d, device_id_type=MESH)
    pl.semaphore_wait(bar, len(devices))


TWO, FOUR, THREE = range(2), range(4), range(3)


def each(count, do):
    lax.fori_loop(0, len(count), lambda i, _: do(i), None)


def lower_upper(i):
    return 2 * i - 1


class Gather:
    def __init__(self, n, shard, full, sems):
        m = len(sems) // len(TWO)
        self.ways = [(h, Place(n, h)) + tuple(sems[h * m : (h + 1) * m]) for h in TWO]
        self.place = self.ways[0][1]
        self.n, self.shard, self.full, self.local = n, shard, full, sems[-1]
        self.rows = shard.shape[0]
        self.wide = shard.shape[1] // len(TWO)
        self.by_rows = self.rows % 64 == 0

    def part(self, ref, h, block, q=None):
        i, count = len(TWO) * h + (0 if q is None else q), len(TWO) if q is None else 1
        left = self.place.core * self.wide
        if self.by_rows:
            r = self.rows // len(FOUR)
            return ref.at[pl.ds(pl.multiple_of(block * self.rows + i * r, r), count * r), pl.ds(pl.multiple_of(left, HEAD), self.wide)]
        c = self.wide // len(FOUR)
        return ref.at[pl.ds(pl.multiple_of(block * self.rows, 8), self.rows), pl.ds(pl.multiple_of(left + i * c, HEAD), count * c)]

    def send(self, h, block, device, sent, recv, q=None, src=None):
        here = self.part(self.full, h, block, q)
        remote(here if src is None else src, here, sent, recv, device).start()

    def bytes_of(self, quarters):
        if self.by_rows:
            return self.full.at[pl.ds(0, quarters * self.rows // len(FOUR)), pl.ds(0, self.wide)]
        return self.full.at[pl.ds(0, quarters // len(TWO) * self.rows), pl.ds(0, self.wide // len(TWO))]

    def wait(self, sent, recv, quarters):
        some = self.bytes_of(quarters) if quarters % len(TWO) == 0 or self.by_rows else self.full.at[pl.ds(0, quarters * self.rows), pl.ds(0, self.wide // len(FOUR))]
        each(TWO, lambda i: remote(some, some, sent, recv.at[i], self.place.twin).wait_recv())

    def hand(self, h, over, here, block):
        part = self.part(self.full, h, block)
        remote(part, part, over, here, self.place.twin).start()

    def keep(self):
        return pltpu.make_async_copy(self.shard, self.full.at[pl.ds(pl.multiple_of(self.place.me * self.rows, 8), self.rows)], self.local)

    def go0(self):
        for h, p, sent, x1, x2, y1, y2, z1, z2, over, here in self.ways:
            each(TWO, lambda i: self.send(h, p.me, p.near(lower_upper(i)), sent, x1.at[i], src=self.part(self.shard, h, 0)))
        self.keep().start()

    def go1(self):
        self.keep().wait()
        for h, p, sent, x1, x2, y1, y2, z1, z2, over, here in self.ways:
            self.wait(sent, x1, len(TWO))

            def side(i):
                d = lower_upper(i)
                self.send(h, p.block(-d), p.near(d), sent, x2.at[i], i)
                each(THREE, lambda b: self.send(h, p.block(b - 1), p.near(0, d), sent, y1.at[i]))
                self.hand(h, over, here, p.block(d))

            each(TWO, side)

    def go2(self):
        for h, p, sent, x1, x2, y1, y2, z1, z2, over, here in self.ways:
            self.wait(sent, x2, 1)
            each(TWO, lambda i: self.send(h, p.block(2), p.near(0, lower_upper(i)), sent, z1.at[i]))
            self.wait(sent, y1, len(TWO) * len(THREE))

            def side(i):
                d = lower_upper(i)

                def one(b):
                    self.send(h, p.block(b - 1, -d), p.near(0, d), sent, y2.at[i], i)
                    self.hand(h, over, here, p.block(b - 1, d))

                each(THREE, one)

            each(TWO, side)
            self.hand(h, over, here, p.block(2))

    def go3(self):
        for h, p, sent, x1, x2, y1, y2, z1, z2, over, here in self.ways:
            self.wait(sent, z1, len(TWO))

            def side(i):
                d = lower_upper(i)
                self.send(h, p.block(2, -d), p.near(0, d), sent, z2.at[i], i)
                self.hand(h, over, here, p.block(2, d))

            each(TWO, side)
            self.wait(sent, y2, len(THREE))
            each(THREE, lambda b: self.hand(h, over, here, p.block(b - 1, 2)))

    def go4(self):
        for h, p, sent, x1, x2, y1, y2, z1, z2, over, here in self.ways:
            self.wait(sent, z2, 1)
            self.hand(h, over, here, p.block(2, 2))
        some = self.bytes_of(len(TWO) * (self.n - 1))
        for h, p, sent, x1, x2, y1, y2, z1, z2, over, here in self.ways:
            remote(some, some, sent, here, p.twin).wait()
            remote(some, some, over, here, p.twin).wait_send()


def gather_sems():
    dma = pltpu.SemaphoreType.DMA
    return ([dma] + [dma((len(TWO),))] * 6 + [dma] * len(TWO)) * len(TWO) + [dma]


def chunk(n, shape):
    rows = shape[0] // n
    return (rows // 4, shape[1]) if rows % 64 == 0 else (rows, shape[1] // 4)


def scatter_scratch(n, shape):
    c, two, four = chunk(n, shape), (len(TWO),), (len(FOUR),)
    dma = pltpu.SemaphoreType.DMA
    one = [pltpu.VMEM(k + c, BF) for k in (two + four, two + two + four, two, two + two, two + four)] + [dma(k) for k in (two, two + two, two, two + two, two)] + [dma] * len(TWO)
    return one * len(TWO) + [pltpu.SemaphoreType.REGULAR]


def tiles(x):
    r, c = x.shape
    return sum(x[a : a + 8, b : b + HEAD] for a in range(0, r, 8) for b in range(0, c, HEAD))


class Scatter:
    def __init__(self, n, grad, out, squares, scratch, again):
        m = len(scratch) // len(TWO)
        self.ways = [(Place(n, h), h) + tuple(scratch[h * m : (h + 1) * m]) for h in TWO]
        self.grad, self.out, self.squares, self.again, self.free = grad, out, squares, again, scratch[-1]
        self.rows = grad.shape[0] // n
        self.chunk = chunk(n, grad.shape)
        self.by_rows = self.chunk[0] < self.rows
        self.step = next(w for w in (1280, self.chunk[1]) if self.chunk[1] % w == 0)

    def part(self, ref, block, quarter):
        r, c = self.chunk
        if self.by_rows:
            return ref.at[pl.ds(pl.multiple_of(block * self.rows + quarter * r, r), r), pl.ds(0, c)]
        return ref.at[pl.ds(pl.multiple_of(block * r, 8), r), pl.ds(pl.multiple_of(quarter * c, HEAD), c)]

    def add(self, into, *terms):
        c, w = self.chunk[1], self.step

        def some(i, _):
            at = pl.ds(pl.multiple_of(i * w, HEAD), w)
            into[:, at] = functools.reduce(lambda a, b: a + b, [t[:, at].astype(F32) for t in terms]).astype(BF)

        lax.fori_loop(0, c // w, some, None)

    def fetch(self, p, h, mine, sm, q, i, j):
        return pltpu.make_async_copy(self.part(self.grad, p.block(i, j), len(TWO) * h + q), mine.at[q, j], sm.at[q])

    def go0(self):
        if self.again:
            pl.semaphore_wait(self.free, len(FOUR))
        for p, h, a, b, c, d, mine, sa, sb, sc, sd, sm, send, kept in self.ways:
            each(TWO, lambda q: each(FOUR, lambda j: remote(self.part(self.grad, p.block(2, j), len(TWO) * h + q), a.at[q, j], send, sa.at[q], p.near(-lower_upper(q))).start()))
        for p, h, a, b, c, d, mine, sa, sb, sc, sd, sm, send, kept in self.ways:
            def quarter(q):
                s = -lower_upper(q)

                def one(j):
                    remote(self.part(self.grad, p.block(s, j), len(TWO) * h + 1 - q), b.at[q, 1 - q, j], send, sb.at[q, 1 - q], p.near(s)).start()
                    self.fetch(p, h, mine, sm, q, s, j).start()

                each(FOUR, one)

            each(TWO, quarter)

    def go1(self):
        for p, h, a, b, c, d, mine, sa, sb, sc, sd, sm, send, kept in self.ways:
            def quarter(q):
                s = -lower_upper(q)
                remote(a.at[q], a.at[q], send, sa.at[q], p.near(s)).wait_recv()
                pltpu.make_async_copy(mine.at[q], mine.at[q], sm.at[q]).wait()
                each(FOUR, lambda j: self.add(a.at[q, j], a.at[q, j], mine.at[q, j]))

                def one(j):
                    self.fetch(p, h, mine, sm, q, 0, j).start()
                    remote(a.at[q, j], b.at[q, q, j], send, sb.at[q, q], p.near(s)).start()

                each(FOUR, one)

            each(TWO, quarter)

    def go2(self):
        for p, h, a, b, c, d, mine, sa, sb, sc, sd, sm, send, kept in self.ways:
            def ready(q):
                pltpu.make_async_copy(mine.at[q], mine.at[q], sm.at[q]).wait()
                each(TWO, lambda i: remote(b.at[i, q], b.at[i, q], send, sb.at[i, q], p.near(1)).wait_recv())

            each(TWO, ready)

            def quarter(q):
                s = -lower_upper(q)

                def term(k, j, to, sem):
                    self.add(b.at[0, k, j], mine.at[k, j], b.at[0, k, j], b.at[1, k, j])
                    remote(b.at[0, k, j], to, send, sem, p.near(0, s)).start()

                term(q, 2, c.at[q], sc.at[q])
                term(1 - q, 1 + 2 * q, d.at[q, 1 - q], sd.at[q, 1 - q])

            each(TWO, quarter)

    def go3(self):
        for p, h, a, b, c, d, mine, sa, sb, sc, sd, sm, send, kept in self.ways:
            def quarter(q):
                s, j = -lower_upper(q), 1 + 2 * q
                remote(c.at[q], c.at[q], send, sc.at[q], p.near(0, s)).wait_recv()
                self.add(c.at[q], c.at[q], mine.at[q, j], b.at[0, q, j], b.at[1, q, j])
                remote(c.at[q], d.at[q, q], send, sd.at[q, q], p.near(0, s)).start()

            each(TWO, quarter)

    def go4(self):
        for p, h, a, b, c, d, mine, sa, sb, sc, sd, sm, send, kept in self.ways:
            def quarter(q):
                each(TWO, lambda i: remote(d.at[i, q], d.at[i, q], send, sd.at[i, q], p.near(1)).wait_recv())
                own = mine.at[q, 0]
                self.add(own, own, b.at[0, q, 0], b.at[1, q, 0], d.at[0, q], d.at[1, q])

                w = self.step

                def some(i, _):
                    x = own[:, pl.ds(pl.multiple_of(i * w, HEAD), w)].astype(F32)
                    self.squares[...] += tiles(x * x)

                lax.fori_loop(0, self.chunk[1] // w, some, None)
                pltpu.make_async_copy(own, self.part(self.out, 0, len(TWO) * h + q), kept).start()

            each(TWO, quarter)

    def end(self):
        for p, h, a, b, c, d, mine, sa, sb, sc, sd, sm, send, kept in self.ways:
            for x in (a, b, c, mine.at[0]):
                remote(x, x, send, sa.at[0], p.near(1)).wait_send()
            pltpu.make_async_copy(c, c, kept).wait()
        if not self.again:
            for d in self.ways[0][0].around():
                pl.semaphore_signal(self.free, device_id=d, device_id_type=MESH)


def then(*steps):
    def do():
        for step in steps:
            step()

    return do


def when(*events):
    def tick(i):
        for place, do in events:
            pl.when(i == place)(do)

    return tick


def dot(a, b, ca, cb):
    return lax.dot_general(a, b, (((ca,), (cb,)), ((), ())), preferred_element_type=F32)


def nn(a, b):
    return dot(a, b, 1, 0)


def nt(a, b):
    return dot(a, b, 1, 1)


def row(i):
    return i, 0


def col(j):
    return 0, j


def whole(*_):
    return 0, 0


def run(body, grid, ins, outs, scratch=(), tick=None):
    held = [(r, late) for r, block, late in ins if block is None]
    tiled = [x for x in ins if x[1] is not None]

    def inner(sem, *refs):
        full, rest = refs[: len(held)], refs[len(held) :]
        copies = [(k, pltpu.make_async_copy(r, v, sem.at[i])) for i, ((r, k), v) in enumerate(zip(held, full))]
        for k, c in copies:
            if k is None:
                c.start()

        def step(*tiles):
            for at in sorted({k or 0 for k, _ in copies} | ({grid[0] - 1} if any(k for k, _ in copies) else set())):
                @pl.when(functools.reduce(lambda p, q: p & q, [pl.program_id(i) == (at if i == 0 else 0) for i in range(len(grid))]))
                def _():
                    for k, c in copies:
                        if k == at and k is not None:
                            c.start()
                    for k, c in copies:
                        if (at == 0 and k is None) or (at == grid[0] - 1 and k is not None):
                            c.wait()

            some, more, given = iter(tiles), iter(full), []
            for _, block, _ in ins:
                given.append(next(more) if block is None else next(some))
            body(*given, *some, *rest, tick or (lambda i: None))

        specs = lambda arrays: [pl.BlockSpec(r.shape, whole, pipeline_mode=pl.Buffered(1)) if block is None else pl.BlockSpec(block, at) for r, block, at in arrays]
        pltpu.emit_pipeline(step, grid=grid, in_specs=specs(tiled), out_specs=specs(outs))(*[r for r, _, _ in tiled], *[r for r, _, _ in outs])

    pl.run_scoped(inner, pltpu.SemaphoreType.DMA((max(len(held), 1),)), *[pltpu.VMEM(r.shape, r.dtype) for r, _ in held], *scratch)


def all_of(ref):
    return ref, None, None


def rows_of(ref):
    return ref, (ROWS, ref.shape[1]), row


def cols_of(ref, parts):
    return ref, (ref.shape[0], ref.shape[1] // parts), col


def in_rows(size, body, tick):
    n = size // MORE

    def one(i, _):
        body(pl.ds(pl.multiple_of(i * MORE, MORE), MORE))
        tick(pl.program_id(0) * n + i)

    lax.fori_loop(0, n, one, None)


def unit(h):
    return lax.rsqrt(jnp.mean(h * h, -1, keepdims=True) + 1e-6)


def normed(h):
    h = h.astype(F32)
    return (h * unit(h)).astype(BF)


def norm_back(h, d):
    h = h.astype(F32)
    s = unit(h)
    return (s * d - h * (s * s * s * jnp.mean(h * d, -1, keepdims=True))).astype(BF)


def rotary(tokens):
    half = HEAD // 2
    angle = np.arange(tokens, dtype=F32)[:, None] * np.power(np.float32(THETA), -np.arange(half, dtype=F32) / half)
    c, s = np.cos(angle), np.sin(angle)
    return jnp.asarray(np.concatenate([c, c], 1)), jnp.asarray(np.concatenate([-s, s], 1))


def heads_of(ref, g):
    return [ref[:, n * HEAD : (n + 1) * HEAD] for n in range(g)]


def in_tiles(size, body, tick):
    def one(i, _):
        body(pl.ds(pl.multiple_of(i * ROWS, ROWS), ROWS))
        tick(i)

    lax.fori_loop(0, size // ROWS, one, None)


def qkv(h, w, cos, sin, kv, a, x, tick):
    turned = w.shape[1] // HEAD - kv

    def tile(at):
        t = normed(h[at, :])
        a[at, :] = t
        r = nn(t, w[...]).astype(BF)
        for n in range(r.shape[1] // HEAD):
            cols = slice(n * HEAD, (n + 1) * HEAD)
            t = r[:, cols]
            if n < turned:
                t = t.astype(F32)
                t = (t * cos[at, :] + pltpu.roll(t, HEAD // 2, 1) * sin[at, :]).astype(BF)
            x[at, cols] = t

    in_tiles(h.shape[0], tile, tick)


def out_proj(h, o, w, m, b, tick):
    def tile(at):
        t = h[at, :] + nn(o[at, :], w[...]).astype(BF)
        m[at, :] = t
        b[at, :] = normed(t)

    in_tiles(h.shape[0], tile, tick)


def up_to(parts):
    return lambda j: (0, lax.min(j, parts - 1))


def cols_then(ref, parts):
    return ref, (ref.shape[0], ref.shape[1] // parts), up_to(parts)


def gu_body(w_ref, wd_ref, g_ref, mid_s, tick, *, b, m, h):
    half = w_ref.shape[1] // 2
    j = pl.program_id(0)
    end = pl.num_programs(0) - 1

    @pl.when(j < end)
    def _():
        def tile(at):
            r = nn(b[at, :], w_ref[...])
            g_ref[at, :] = r
            g = r[:, :half]
            mid_s[j, at, :] = (g * jax.nn.sigmoid(g) * r[:, half:]).astype(BF)

        in_rows(b.shape[0], tile, tick)

    @pl.when(j == end)
    def _():
        def tile(at):
            h[at, :] = m[at, :] + nn(jnp.concatenate([mid_s[i, at, :] for i in range(PARTS)], 1), wd_ref[...]).astype(BF)

        in_rows(b.shape[0], tile, tick)


def mlp(b, w, m, wd, gu, h, late, tick):
    run(functools.partial(gu_body, b=b, m=m, h=h), (PARTS + 1,), [cols_then(w, PARTS), (wd, None, late)], [cols_then(gu, PARTS)],
        [pltpu.VMEM((PARTS, b.shape[0], w.shape[1] // PARTS // 2), BF)], tick)


def visible(iq, j, bq, bk):
    return lax.broadcasted_iota(jnp.int32, (bk, bq), 1) - lax.broadcasted_iota(jnp.int32, (bk, bq), 0) >= j * bk - iq * bq


def key_blocks(c, iq, blocks, block, tick):
    before = c * (blocks * (blocks + 1) // 2) + lax.div(iq * (iq + 1), 2)

    def seen(j, _):
        @pl.when(j <= iq)
        def _():
            block(j)
            tick(before + j)

    lax.fori_loop(0, blocks, seen, None)


def attend(x, kv, o, lse, top_s, mix_s, tick, bq=MORE):
    t, n = x.shape
    heads = n // HEAD - 2 * kv
    g = heads // kv
    scale = HEAD**-0.5
    e = scale * LOG2E
    ones = jnp.ones((8, bq), BF)

    def one(step, _):
        c, iq = lax.div(step, t // bq), lax.rem(step, t // bq)
        cols = lambda at: pl.ds(pl.multiple_of(at * HEAD, HEAD), HEAD)
        rows = lambda i: pl.ds(pl.multiple_of(i * bq, bq), bq)
        top_s[...] = jnp.full(top_s.shape, NEG, F32)
        mix_s[...] = jnp.zeros(mix_s.shape, F32)

        def block(j):
            k = x[rows(j), cols(heads + c)]
            scores = [nt(k, x[rows(iq), cols(c * g + n)]) for n in range(g)]
            values = jnp.concatenate([x[rows(j), cols(heads + kv + c)].T, ones], axis=0)
            weights, keeps = [], []
            for n, s in enumerate(scores):
                s = jnp.where(visible(iq, j, bq, bq), s, 2 * NEG)
                mine = slice(n, n + 1)
                old = top_s[mine, :]
                top = jnp.maximum(old, s.max(axis=0, keepdims=True))
                top_s[mine, :] = top
                weights.append(jnp.exp2((s - top) * e).astype(BF))
                keeps.append(jnp.exp2((old - top) * e))
            for n in range(g):
                mix_s[n] = mix_s[n] * keeps[n] + nn(values, weights[n])

        key_blocks(c, iq, t // bq, block, tick)
        for n in range(g):
            mine = slice(n, n + 1)
            total = mix_s[n, HEAD : HEAD + 1, :]
            o[rows(iq), cols(c * g + n)] = (mix_s[n, :HEAD, :] * (1 / total)).T.astype(BF)
            lse[c, mine, rows(iq)] = top_s[mine, :] * scale + jnp.log(total)

    lax.fori_loop(0, kv * (t // bq), one, None)


def attention_specs(x, kv, bq):
    t, n = x.shape
    heads = n // HEAD - 2 * kv
    g = heads // kv
    return (bq, g * HEAD), [(x, (bq, g * HEAD), lambda c, i: (i, c)), (x, (t, HEAD), lambda c, i: (0, heads + c)), (x, (t, HEAD), lambda c, i: (0, heads + kv + c))], \
        lambda ref: (ref, (1, g, bq), lambda c, i: (c, 0, i))


def bwd_body(q_ref, k_ref, v_ref, do_ref, lse_ref, delta_ref, c_ref, s_ref, dq_s, dk_s, dv_s, tick, *, scale, bk, into):
    bq, g = q_ref.shape[0], q_ref.shape[1] // HEAD
    iq = pl.program_id(1)
    e = scale * LOG2E

    @pl.when(iq == 0)
    def _():
        dk_s[...] = jnp.zeros_like(dk_s)
        dv_s[...] = jnp.zeros_like(dv_s)

    dq_s[...] = jnp.zeros_like(dq_s)

    def block(j):
        here = pl.ds(pl.multiple_of(j * bk, bk), bk)
        k, v = k_ref[here, :], v_ref[here, :]
        back = k.T
        qs, dos = heads_of(q_ref, g), heads_of(do_ref, g)
        scores = [nt(k, x) for x in qs]
        dps = [nt(v, x) for x in dos]
        for n in range(g):
            mine = slice(n, n + 1)
            p = jnp.where(visible(iq, j, bq, bk), jnp.exp2(scores[n] * e - lse_ref[0, mine, :] * LOG2E), 0.0)
            ds = (p * (dps[n] - delta_ref[0, mine, :])).astype(BF)
            dv_s[here, :] += nn(p.astype(BF), dos[n])
            dk_s[here, :] += nn(ds, qs[n])
            dq_s[n] += nn(back, ds)

    key_blocks(pl.program_id(0), iq, k_ref.shape[0] // bq, block, tick)

    def unturned(d, at):
        d = d.astype(BF).astype(F32)
        return (d * c_ref[at, :] - pltpu.roll(d, HEAD // 2, 1) * s_ref[at, :]).astype(BF)

    c = pl.program_id(0)
    heads = pl.num_programs(0)
    q_at = pl.ds(pl.multiple_of(iq * bq, bq), bq)
    cols = lambda at: pl.ds(pl.multiple_of(at * HEAD, HEAD), HEAD)
    for n in range(g):
        into[q_at, cols(c * g + n)] = unturned((dq_s[n] * scale).T, q_at)

    @pl.when(iq == pl.num_programs(1) - 1)
    def _():
        into[:, cols(heads * g + c)] = unturned(dk_s[...] * scale, slice(None))
        into[:, cols(heads * (g + 1) + c)] = dv_s[...].astype(BF)


def attend_back(x, do, lse, delta, cos, sin, kv, into, tick, bq=MORE, bk=MORE):
    tile, ins, stat = attention_specs(x, kv, bq)
    t = x.shape[0]
    run(functools.partial(bwd_body, scale=HEAD**-0.5, bk=bk, into=into), (kv, t // bq), ins + [(do, tile, lambda c, i: (i, c)), stat(lse), stat(delta), all_of(cos), all_of(sin)],
        [], [pltpu.VMEM((tile[1] // HEAD, HEAD, bq), F32)] + [pltpu.VMEM((t, HEAD), F32)] * 2, tick)


def silu_back(g, u, d):
    s = jax.nn.sigmoid(g)
    silu = g * s
    return (silu * u).astype(BF), (d * u * (s + silu * (1 - s))).astype(BF), (d * silu).astype(BF)


def dgu_body(dy_ref, w_ref, g_ref, dg_ref, dw_ref, mid_s, tick):
    half = mid_s.shape[1]

    def tile(at):
        d = nt(dy_ref[at, :], w_ref[...]).astype(BF).astype(F32)
        mid_s[at, :], dg_ref[at, :half], dg_ref[at, half:] = silu_back(g_ref[at, :half], g_ref[at, half:], d)

    in_rows(dy_ref.shape[0], tile, tick)
    dw_ref[...] = dot(mid_s[...], dy_ref[...], 0, 0).astype(BF)


def dgu(dy, wd, gu, dg, dwd, tick):
    t, c = dy.shape[0], wd.shape[0] // PARTS
    rows = lambda ref: (ref, (c, ref.shape[1]), row)
    run(dgu_body, (PARTS,), [all_of(dy), rows(wd), cols_of(gu, PARTS)], [cols_of(dg, PARTS), rows(dwd)], [pltpu.VMEM((t, c), BF)], tick)


def last_body(dy_ref, wd_ref, b_ref, w_ref, dg_ref, dw_ref, mid_s, tick):
    half = mid_s.shape[1]

    def tile(at):
        r = nn(b_ref[at, :], w_ref[...])
        d = nt(dy_ref[at, :], wd_ref[...]).astype(BF).astype(F32)
        mid_s[at, :], dg_ref[at, :half], dg_ref[at, half:] = silu_back(r[:, :half], r[:, half:], d)

    in_rows(dy_ref.shape[0], tile, tick)
    dw_ref[...] = dot(mid_s[...], dy_ref[...], 0, 0).astype(BF)


def last_dgu(dy, wd, b, wgu, dg, dwd, tick):
    t, c = dy.shape[0], wd.shape[0] // PARTS
    rows = lambda ref: (ref, (c, ref.shape[1]), row)
    run(last_body, (PARTS,), [all_of(dy), rows(wd), all_of(b), cols_of(wgu, PARTS)], [cols_of(dg, PARTS), rows(dwd)], [pltpu.VMEM((t, c), BF)], tick)


def dw_body(a_ref, d_ref, o_ref, at_s, tick):
    @pl.when(pl.program_id(0) == 0)
    def _():
        at_s[...] = a_ref[...].T

    def tile(at):
        o_ref[at, :] = nn(at_s[at, :], d_ref[...]).astype(BF)

    in_rows(at_s.shape[0], tile, tick)


def dw(a, d, out, parts, tick):
    run(dw_body, (parts,), [all_of(a), cols_of(d, parts)], [cols_of(out, parts)], [pltpu.VMEM(a.shape[::-1], BF)], tick)


def db_body(dg_ref, w_ref, dy_ref, h_ref, wo_ref, x_ref, dm_ref, do_ref, delta_ref, to_ref, acc, tick):
    j = pl.program_id(0)
    end = pl.num_programs(0) - 1

    @pl.when(j < end)
    def _():
        def tile(at):
            r = nt(dg_ref[at, :], w_ref[...])

            @pl.when(j == 0)
            def _():
                acc[at, :] = r

            @pl.when(j > 0)
            def _():
                acc[at, :] += r

        in_rows(acc.shape[0], tile, tick)

    @pl.when(j == end)
    def _():
        kv, g = delta_ref.shape[:2]

        def tile(at):
            d = dy_ref[at, :] + norm_back(h_ref[at, :], acc[at, :].astype(BF).astype(F32))
            dm_ref[at, :] = d
            r = nt(d, wo_ref[...]).astype(BF)
            do_ref[at, :] = r
            for n in range(kv * g):
                cols = slice(n * HEAD, (n + 1) * HEAD)
                x = r[:, cols].astype(F32) * x_ref[at, cols].astype(F32)
                delta_ref[n // g, n % g : n % g + 1, at] = jnp.sum(x.T, axis=0, keepdims=True)

        in_rows(acc.shape[0], tile, tick)

        def term(i, _):
            at = pl.ds(pl.multiple_of(i * ROWS, ROWS), ROWS)
            to_ref[at, :] = nn(x_ref[:, at].T, dm_ref[...]).astype(BF)

        lax.fori_loop(0, to_ref.shape[0] // ROWS, term, None)


def db(dg, wgu, dy, h, wo, x, dm, do, delta, to, tick):
    late = lambda ref: (ref, None, 1)
    run(db_body, (PARTS + 1,), [cols_then(dg, PARTS), cols_then(wgu, PARTS), late(dy), late(h), late(wo), late(x)], [all_of(dm), all_of(do), all_of(delta), all_of(to)],
        [pltpu.VMEM(dy.shape, F32)], tick)


def da_body(d_ref, h_ref, o_ref, tick, *, dx, w):
    i = pl.program_id(0)
    r = nt(dx[pl.ds(pl.multiple_of(i * ROWS, ROWS), ROWS), :], w[...])
    o_ref[...] = d_ref[...] + norm_back(h_ref[...], r.astype(BF).astype(F32))
    tick(i)


def da(dx, w, d, h, out, tick):
    run(functools.partial(da_body, dx=dx, w=w), (d.shape[0] // ROWS,), [rows_of(d), rows_of(h)], [rows_of(out)], tick=tick)


def dqkv_body(o_ref, tick, *, dx, a):
    i = pl.program_id(0)
    o_ref[...] = nn(a[:, pl.ds(pl.multiple_of(i * ROWS, ROWS), ROWS)].T, dx[...]).astype(BF)
    tick(i)


def dqkv(a, dx, out, tick):
    run(functools.partial(dqkv_body, dx=dx, a=a), (out.shape[0] // ROWS,), [], [rows_of(out)], tick=tick)


WAYS = ("a", "gu", "d")
SUMS = ("qkv", "o", "gu", "d")
NAMES = ("wq", "wk", "wv", "wo", "w_gate", "w_up", "w_down")


def named(names, refs):
    return dict(zip(names, refs, strict=True))


def beside(r, kw):
    a = r.shape[1]
    q = a // 2 - kw
    return r.at[:, pl.ds(0, a - q)], r.at[:, pl.ds(a - q, q)]


def mixture(f):
    w = f // PARTS
    return [(i, j * w, (2 * j + i) * w, w) for j in range(PARTS) for i in TWO]


def forward_kernel(n, layers, kv, ins, outs, count, *refs):
    r = named(ins + outs, refs[:count])
    packs, refs = refs[count : count + 2], refs[count + 2 :]
    (h, a_s, x_s, o_s, lse_s, m_s, b_s, wqkv_s, wo_s, top_s, mix_s, fetched, out), sems = refs[:13], refs[13:]
    fetch = lambda i, src, dst: pltpu.make_async_copy(src, dst, fetched.at[i])
    first = fetch(0, r["x"].at[0], h)
    first.start()
    for l in range(layers):
        at = 0
        for name in NAMES[:4]:
            w = r[name].shape[2]
            packs[0][l, :, at : at + w] = r[name][l]
            at += w
        for i, a, b, w in mixture(r["w_up"].shape[2]):
            packs[1][l, :, b : b + w] = r[NAMES[4 + i]][l, :, a : a + w]
    place = Place(n, 0)
    greet(place.around() + [place.twin])
    per = len(gather_sems())
    pieces = [[Gather(n, p.at[l], r[f"w{w}{l}"], sems[per * (3 * l + i) : per * (3 * l + i + 1)]) for i, (w, p) in enumerate(zip(WAYS, (*packs, r["w_down"])))]
              for l in range(layers)]
    a, gu, dn = pieces[0]
    then(a.go0, gu.go0, dn.go0, a.go1, a.go2, a.go3, gu.go1, dn.go1, a.go4)()
    kept = dict(zip("axombh", (a_s, x_s, o_s, m_s, b_s, h))) | {"lse": lse_s}
    leave = lambda i, l: pltpu.make_async_copy(kept[i], r[f"{i}{l}"], out.at[list(kept).index(i)])
    first.wait()
    for l in range(layers):
        more = l + 1 < layers
        a, gu, dn = pieces[l]
        wqkv, wo = beside(r[f"wa{l}"], kv * HEAD)
        two = fetch(0, wqkv, wqkv_s), fetch(1, wo, wo_s)
        for c in two:
            c.start()
        if l:
            for i in kept:
                if i != "h":
                    leave(i, l - 1).wait()
        two[0].wait()
        qkv(h, wqkv_s, r["cos"], r["sin"], kv, a_s, x_s, when())
        for i in "ax":
            leave(i, l).start()
        attend(x_s, kv, o_s, lse_s, top_s, mix_s, when((1, gu.go2)) if more else when((0, dn.go2), (2, gu.go2)))
        for i in ("o", "lse"):
            leave(i, l).start()
        two[1].wait()
        out_proj(h, o_s, wo_s, m_s, b_s, when((2, gu.go3) if more else (0, dn.go3)))
        for i in "mb":
            leave(i, l).start()
        if more:
            if l:
                leave("h", l).wait()
            a2, gu2, dn2 = pieces[l + 1]
            then(dn.go2, a2.go0, gu2.go0, dn2.go0, gu.go4)()
            mlp(b_s, r[f"wgu{l}"], m_s, r[f"wd{l}"], r[f"gu{l}"], h, 2,
                when((1, then(dn.go3, a2.go1)), (3, dn.go4), (7, then(a2.go2, dn2.go1)), (2 * PARTS, then(a2.go3, gu2.go1))))
            leave("h", l + 1).start()
            a2.go4()
        else:
            then(gu.go3, dn.go4, gu.go4)()
    for i in kept:
        leave(i, layers - 1).wait()


def backward_kernel(n, layers, kv, ins, outs, count, *refs):
    r = named(ins + outs, refs[:count])
    squares, slots, send, recv = refs[count : count + 4]
    held = refs[count + 4 :]
    place = Place(n, 0)
    others = [{"dp": lax.rem(place.me + i, n)} for i in range(1, n)]
    greet(others)
    squares[...] = jnp.zeros_like(squares)

    per = len(held) // len(SUMS)

    def piece(l, w):
        i = per * SUMS.index(w)
        return Scatter(n, r[f"t{w}{l}"], r[f"g{w}{l}"], squares, held[i : i + per], l + 1 < layers)

    d = r["dy"].at[0]
    before = []
    for l in reversed(range(layers)):
        p, o, gu, dn = (piece(l, w) for w in SUMS)
        if before:
            p1, o1, gu1, dn1 = before
            dgu(d, r[f"wd{l}"], r[f"gu{l}"], r["dg"], r[f"td{l}"],
                when((0, then(dn1.go4, o1.go2)), (2, p1.go1), (5, then(gu1.go4, o1.go3)), (6, p1.go2), (8, then(o1.go4, p1.go3))))
            p1.go4()
        else:
            last_dgu(d, r[f"wd{l}"], r[f"b{l}"], r[f"wgu{l}"], r["dg"], r[f"td{l}"], when())
        wqkv, wo = beside(r[f"wa{l}"], kv * HEAD)
        then(*[q.end for q in before], dn.go0)()
        dw(r[f"b{l}"], r["dg"], r[f"tgu{l}"], PARTS, when((5, dn.go1)))
        gu.go0()
        db(r["dg"], r[f"wgu{l}"], d, r[f"m{l}"], wo, r[f"o{l}"], r["dm"], r["do"], r["delta"], r[f"to{l}"], when((4, dn.go2), (2 * PARTS, gu.go1)))
        o.go0()

        def attention(dx, a, w, sem):
            copies = [pltpu.make_async_copy(x, y, sem.at[i]) for i, (x, y) in enumerate(((r[f"a{l}"], a), (wqkv, w))[: 2 if l else 1])]
            for c in copies:
                c.start()
            attend_back(r[f"x{l}"], r["do"], r[f"lse{l}"], r["delta"], r["cos"], r["sin"], kv, dx, when((3, dn.go3)))
            for c in copies:
                c.wait()
            dqkv(a, dx, r[f"tqkv{l}"], when((2, gu.go2), (3, o.go1)) if l else when())
            p.go0()
            if l:
                da(dx, w, r["dm"], r[f"h{l}"], r[f"d{l}"], when((3, gu.go3)))

        pl.run_scoped(attention, pltpu.VMEM(r[f"x{l}"].shape, BF), pltpu.VMEM(r[f"a{l}"].shape, BF), pltpu.VMEM(wqkv.shape, BF), pltpu.SemaphoreType.DMA((2,)))
        if l:
            d = r[f"d{l}"]
        else:
            then(gu.go2, o.go1, dn.go4, p.go1, gu.go3, o.go2, p.go2, gu.go4, o.go3, p.go3, o.go4, p.go4)()
        before = [p, o, gu, dn]
    then(*[q.end for q in before])()
    copies = [remote(squares, slots.at[i], send.at[i], recv.at[i], p) for i, p in enumerate(others)]
    for c in copies:
        c.start()
    for c in copies:
        c.wait()
    t = squares[...] + sum(slots[i] for i in range(n - 1))
    r["total"][...] = jnp.broadcast_to(jnp.sum(jnp.sum(t, axis=1, keepdims=True), axis=0, keepdims=True), t.shape)


def kernel(body, name, number, given, made, in_vmem, scratch):
    space = lambda name: pl.BlockSpec(memory_space=pltpu.VMEM if name in in_vmem else pl.ANY)
    got = pl.pallas_call(
        functools.partial(body, tuple(given), tuple(made), len(given) + len(made)),
        in_specs=[space(k) for k in given],
        out_specs=[space(k) for k in made],
        out_shape=[jax.ShapeDtypeStruct(*s) for s in made.values()],
        scratch_shapes=scratch,
        compiler_params=pltpu.CompilerParams(collective_id=number, has_side_effects=True, vmem_limit_bytes=VMEM),
        name=name,
    )(*given.values())
    return dict(zip(made, got, strict=True))


def adamw(w, m, v, g):
    m = 0.9 * m + 0.1 * g
    v = 0.95 * v + 0.05 * g * g
    step = m * lax.rsqrt(v + 1e-8) + 0.1 * w
    return (w - 0.02 * step).astype(BF), m, v


def step_kernel(count, layers, total_ref, *refs):
    m, k = len(SUMS), len(NAMES)
    grads, refs = refs[: m * layers], refs[m * layers :]
    olds, news = refs[: 3 * k], refs[3 * k :]
    factor = jnp.minimum(1.0, 0.5 * lax.rsqrt(total_ref[:1, :1] / count + 1e-30))
    for l in range(layers):
        @pl.when(pl.program_id(0) == l)
        def _():
            p, o, gu, d = grads[m * l : m * l + m]
            q, w = olds[0].shape[2], olds[1].shape[2]
            wide = o.shape[1]
            moves = [(0, p, 0, 0, q), (1, p, 0, q, w), (2, p, 0, q + w, w), (3, o, 0, 0, wide), (k - 1, d, 0, 0, wide)]
            for i, g, to, at, w in moves + [(4 + i, gu, to, at, w) for i, to, at, w in mixture(olds[4].shape[2])]:
                def some(c, _):
                    here, there = (pl.ds(pl.multiple_of(x + c * HEAD, HEAD), HEAD) for x in (to, at))
                    three = (i, i + k, i + 2 * k)
                    new = adamw(*[olds[j][0, :, here].astype(F32) for j in three], g[:, there].astype(F32) * factor)
                    for j, x in zip(three, new):
                        news[j][0, :, here] = x

                lax.fori_loop(0, w // HEAD, some, None)


def optimizer(n, total, grads, arrays):
    layers = arrays[0].shape[0]
    tile = lambda a: pl.BlockSpec((1,) + a.shape[1:], lambda l: (l, 0, 0))
    held = pl.BlockSpec(memory_space=pltpu.VMEM)
    return pl.pallas_call(
        functools.partial(step_kernel, n * sum(a.size for a in arrays[:7]), layers),
        grid=(layers,),
        in_specs=[held] * (1 + len(grads)) + [tile(a) for a in arrays],
        out_specs=[tile(a) for a in arrays],
        out_shape=[jax.ShapeDtypeStruct(a.shape, a.dtype) for a in arrays],
        compiler_params=pltpu.CompilerParams(dimension_semantics=("arbitrary",), vmem_limit_bytes=VMEM),
        name="optimizer",
    )(total, *grads, *arrays)


def solution(mesh):
    n = mesh.shape["dp"]

    def step(x, dy, *arrays):
        weights = named(NAMES, arrays[:7])
        layers, _, kw = weights["wk"].shape
        kv = kw // HEAD
        t, d = x.shape[1:]
        q, f = weights["wq"].shape[2], weights["w_up"].shape[2]
        cos, sin = rotary(t)
        shapes = {"a": (d, 2 * q + 2 * kw), "qkv": (d, q + 2 * kw), "o": (q, d), "gu": (d, 2 * f), "d": (f, d)}
        lse, made = (kv, q // kw, t), {}
        for l in range(layers):
            made |= {f"w{w}{l}": (shapes[w], BF) for w in WAYS}
            made |= {f"a{l}": ((t, d), BF), f"x{l}": ((t, q + 2 * kw), BF), f"o{l}": ((t, q), BF), f"lse{l}": (lse, F32),
                     f"m{l}": ((t, d), BF), f"b{l}": ((t, d), BF)}
            if l + 1 < layers:
                made |= {f"gu{l}": ((t, 2 * f), F32), f"h{l + 1}": ((t, d), BF)}
        vm = lambda *shape: pltpu.VMEM(shape, BF)
        shards = [vm(layers, shapes[w][0] // n, shapes[w][1]) for w in WAYS[:2]]
        work = [vm(t, d), vm(t, d), vm(t, q + 2 * kw), vm(t, q), pltpu.VMEM(lse, F32), vm(t, d), vm(t, d), vm(*shapes["qkv"]), vm(*shapes["o"]),
                pltpu.VMEM((8, MORE), F32), pltpu.VMEM((q // kw, HEAD + 8, MORE), F32), pltpu.SemaphoreType.DMA((2,)), pltpu.SemaphoreType.DMA((7,))]
        kept = kernel(functools.partial(forward_kernel, n, layers, kv), "forward", 0, {"x": x, "cos": cos, "sin": sin, **weights}, made, NAMES + ("cos", "sin"),
                      shards + work + gather_sems() * (len(WAYS) * layers))
        given = {"dy": dy, "cos": cos, "sin": sin, **kept}
        made = {"dg": ((t, 2 * f), BF), "do": ((t, q), BF), "delta": (lse, F32), "dm": ((t, d), BF),
                "total": ((8, HEAD), F32)}
        for l in range(layers):
            made |= {f"t{w}{l}": (shapes[w], BF) for w in SUMS} | {f"g{w}{l}": ((shapes[w][0] // n, shapes[w][1]), BF) for w in SUMS} | {f"d{l}": ((t, d), BF)}
        scratch = [pltpu.VMEM((8, HEAD), F32), pltpu.VMEM((n - 1, 8, HEAD), F32)] + [pltpu.SemaphoreType.DMA((n - 1,))] * 2
        got = kernel(functools.partial(backward_kernel, n, layers, kv), "backward", 1, given, made, ["total"], sum([scatter_scratch(n, shapes[w]) for w in SUMS], scratch))
        return tuple(optimizer(n, got["total"], [got[f"g{w}{l}"] for l in range(layers) for w in SUMS], arrays))

    states, cut = P(("rep", "dp"), None, None), P(None, "dp", None)
    return jax.shard_map(step, mesh=mesh, in_specs=(states, states) + (cut,) * 21, out_specs=(P("rep", "dp", None),) * 21, check_vma=False)
```

```python
import functools

import jax
import jax.numpy as jnp
import numpy as np
from jax import lax
from jax.experimental import pallas as pl
from jax.experimental.pallas import tpu as pltpu
from jax.sharding import PartitionSpec as P

MESH = pl.DeviceIdType.MESH
BF, F32 = jnp.bfloat16, jnp.float32
LOG2E = 1.4426950408889634
NEG = -1e30
HEAD = 128
THETA = 10000
ROWS, MORE = 256, 512
PARTS = 5
VMEM = 62 * 2**20


class Place:
    def __init__(self, n, first):
        self.side = next(i for i in range(n) if i * i == n)
        self.me = lax.axis_index("dp")
        self.xy = [lax.div(self.me, self.side), lax.rem(self.me, self.side)]
        self.first = first
        rep = lax.axis_index("rep")
        self.core = lax.rem(rep, 2)
        self.twin = {"rep": rep + 1 - 2 * self.core}

    def block(self, i, j=0):
        s = self.side
        by = (i, j) if self.first == 0 else (j, i)
        x, y = (lax.rem(c + d + s, s) for c, d in zip(self.xy, by))
        return x * s + y

    def near(self, i, j=0):
        return {"dp": self.block(i, j)}

    def around(self):
        return [self.near(*d) for d in ((1, 0), (-1, 0), (0, 1), (0, -1))]


def remote(src, dst, send, recv, device):
    return pltpu.make_async_remote_copy(src_ref=src, dst_ref=dst, send_sem=send, recv_sem=recv, device_id=device, device_id_type=MESH)


def greet(devices, meanwhile=lambda: None):
    bar = pltpu.get_barrier_semaphore()
    for d in devices:
        pl.semaphore_signal(bar, device_id=d, device_id_type=MESH)
    meanwhile()
    pl.semaphore_wait(bar, len(devices))


TWO, FOUR, THREE = range(2), range(4), range(3)


def each(count, do):
    lax.fori_loop(0, len(count), lambda i, _: do(i), None)


def lower_upper(i):
    return 2 * i - 1


class Gather:
    def __init__(self, n, shard, full, sems):
        m = len(sems) // len(TWO)
        self.ways = [(h, Place(n, h)) + tuple(sems[h * m : (h + 1) * m]) for h in TWO]
        self.place = self.ways[0][1]
        self.n, self.shard, self.full, self.local = n, shard, full, sems[-1]
        self.rows = shard.shape[0]
        self.wide = shard.shape[1] // len(TWO)
        self.by_rows = self.rows % 64 == 0

    def part(self, ref, h, block, q=None):
        i, count = len(TWO) * h + (0 if q is None else q), len(TWO) if q is None else 1
        left = self.place.core * self.wide
        if self.by_rows:
            r = self.rows // len(FOUR)
            return ref.at[pl.ds(pl.multiple_of(block * self.rows + i * r, r), count * r), pl.ds(pl.multiple_of(left, HEAD), self.wide)]
        c = self.wide // len(FOUR)
        return ref.at[pl.ds(pl.multiple_of(block * self.rows, 8), self.rows), pl.ds(pl.multiple_of(left + i * c, HEAD), count * c)]

    def send(self, h, block, device, sent, recv, q=None, src=None):
        here = self.part(self.full, h, block, q)
        remote(here if src is None else src, here, sent, recv, device).start()

    def bytes_of(self, quarters):
        if self.by_rows:
            return self.full.at[pl.ds(0, quarters * self.rows // len(FOUR)), pl.ds(0, self.wide)]
        return self.full.at[pl.ds(0, quarters // len(TWO) * self.rows), pl.ds(0, self.wide // len(TWO))]

    def wait(self, sent, recv, quarters):
        some = self.bytes_of(quarters) if quarters % len(TWO) == 0 or self.by_rows else self.full.at[pl.ds(0, quarters * self.rows), pl.ds(0, self.wide // len(FOUR))]
        each(TWO, lambda i: remote(some, some, sent, recv.at[i], self.place.twin).wait_recv())

    def hand(self, h, over, here, block):
        part = self.part(self.full, h, block)
        remote(part, part, over, here, self.place.twin).start()

    def keep(self):
        return pltpu.make_async_copy(self.shard, self.full.at[pl.ds(pl.multiple_of(self.place.me * self.rows, 8), self.rows)], self.local)

    def go0(self):
        for h, p, sent, x1, x2, y1, y2, z1, z2, over, here in self.ways:
            each(TWO, lambda i: self.send(h, p.me, p.near(lower_upper(i)), sent, x1.at[i], src=self.part(self.shard, h, 0)))
        self.keep().start()

    def go1(self):
        self.keep().wait()
        for h, p, sent, x1, x2, y1, y2, z1, z2, over, here in self.ways:
            self.wait(sent, x1, len(TWO))

            def side(i):
                d = lower_upper(i)
                self.send(h, p.block(-d), p.near(d), sent, x2.at[i], i)
                each(THREE, lambda b: self.send(h, p.block(b - 1), p.near(0, d), sent, y1.at[i]))
                self.hand(h, over, here, p.block(d))

            each(TWO, side)

    def go2(self):
        for h, p, sent, x1, x2, y1, y2, z1, z2, over, here in self.ways:
            self.wait(sent, x2, 1)
            each(TWO, lambda i: self.send(h, p.block(2), p.near(0, lower_upper(i)), sent, z1.at[i]))
            self.wait(sent, y1, len(TWO) * len(THREE))

            def side(i):
                d = lower_upper(i)

                def one(b):
                    self.send(h, p.block(b - 1, -d), p.near(0, d), sent, y2.at[i], i)
                    self.hand(h, over, here, p.block(b - 1, d))

                each(THREE, one)

            each(TWO, side)
            self.hand(h, over, here, p.block(2))

    def go3(self):
        for h, p, sent, x1, x2, y1, y2, z1, z2, over, here in self.ways:
            self.wait(sent, z1, len(TWO))

            def side(i):
                d = lower_upper(i)
                self.send(h, p.block(2, -d), p.near(0, d), sent, z2.at[i], i)
                self.hand(h, over, here, p.block(2, d))

            each(TWO, side)
            self.wait(sent, y2, len(THREE))
            each(THREE, lambda b: self.hand(h, over, here, p.block(b - 1, 2)))

    def go4(self):
        for h, p, sent, x1, x2, y1, y2, z1, z2, over, here in self.ways:
            self.wait(sent, z2, 1)
            self.hand(h, over, here, p.block(2, 2))
        some = self.bytes_of(len(TWO) * (self.n - 1))
        for h, p, sent, x1, x2, y1, y2, z1, z2, over, here in self.ways:
            remote(some, some, sent, here, p.twin).wait()
            remote(some, some, over, here, p.twin).wait_send()


def gather_sems():
    dma = pltpu.SemaphoreType.DMA
    return ([dma] + [dma((len(TWO),))] * 6 + [dma] * len(TWO)) * len(TWO) + [dma]


def chunk(n, shape):
    rows = shape[0] // n
    return (rows // 4, shape[1]) if rows % 64 == 0 else (rows, shape[1] // 4)


def scatter_scratch(n, shape):
    c, two, four = chunk(n, shape), (len(TWO),), (len(FOUR),)
    dma = pltpu.SemaphoreType.DMA
    one = [pltpu.VMEM(k + c, BF) for k in (two + four, two + two + four, two, two + two, two + four)] + [dma(k) for k in (two, two + two, two, two + two, two)] + [dma] * len(TWO)
    return one * len(TWO) + [pltpu.SemaphoreType.REGULAR]


def tiles(x):
    r, c = x.shape
    return sum(x[a : a + 8, b : b + HEAD] for a in range(0, r, 8) for b in range(0, c, HEAD))


class Scatter:
    def __init__(self, n, grad, out, squares, scratch, again):
        m = len(scratch) // len(TWO)
        self.ways = [(Place(n, h), h) + tuple(scratch[h * m : (h + 1) * m]) for h in TWO]
        self.grad, self.out, self.squares, self.again, self.free = grad, out, squares, again, scratch[-1]
        self.rows = grad.shape[0] // n
        self.chunk = chunk(n, grad.shape)
        self.by_rows = self.chunk[0] < self.rows
        self.step = next(w for w in (1280, self.chunk[1]) if self.chunk[1] % w == 0)

    def part(self, ref, block, quarter):
        r, c = self.chunk
        if self.by_rows:
            return ref.at[pl.ds(pl.multiple_of(block * self.rows + quarter * r, r), r), pl.ds(0, c)]
        return ref.at[pl.ds(pl.multiple_of(block * r, 8), r), pl.ds(pl.multiple_of(quarter * c, HEAD), c)]

    def add(self, into, *terms):
        c, w = self.chunk[1], self.step

        def some(i, _):
            at = pl.ds(pl.multiple_of(i * w, HEAD), w)
            into[:, at] = functools.reduce(lambda a, b: a + b, [t[:, at].astype(F32) for t in terms]).astype(BF)

        lax.fori_loop(0, c // w, some, None)

    def fetch(self, p, h, mine, sm, q, i, j):
        return pltpu.make_async_copy(self.part(self.grad, p.block(i, j), len(TWO) * h + q), mine.at[q, j], sm.at[q])

    def go0(self):
        if self.again:
            pl.semaphore_wait(self.free, len(FOUR))
        for p, h, a, b, c, d, mine, sa, sb, sc, sd, sm, send, kept in self.ways:
            each(TWO, lambda q: each(FOUR, lambda j: remote(self.part(self.grad, p.block(2, j), len(TWO) * h + q), a.at[q, j], send, sa.at[q], p.near(-lower_upper(q))).start()))
        for p, h, a, b, c, d, mine, sa, sb, sc, sd, sm, send, kept in self.ways:
            def quarter(q):
                s = -lower_upper(q)

                def one(j):
                    remote(self.part(self.grad, p.block(s, j), len(TWO) * h + 1 - q), b.at[q, 1 - q, j], send, sb.at[q, 1 - q], p.near(s)).start()
                    self.fetch(p, h, mine, sm, q, s, j).start()

                each(FOUR, one)

            each(TWO, quarter)

    def go1(self):
        for p, h, a, b, c, d, mine, sa, sb, sc, sd, sm, send, kept in self.ways:
            def quarter(q):
                s = -lower_upper(q)
                remote(a.at[q], a.at[q], send, sa.at[q], p.near(s)).wait_recv()
                pltpu.make_async_copy(mine.at[q], mine.at[q], sm.at[q]).wait()
                each(FOUR, lambda j: self.add(a.at[q, j], a.at[q, j], mine.at[q, j]))

                def one(j):
                    self.fetch(p, h, mine, sm, q, 0, j).start()
                    remote(a.at[q, j], b.at[q, q, j], send, sb.at[q, q], p.near(s)).start()

                each(FOUR, one)

            each(TWO, quarter)

    def go2(self):
        for p, h, a, b, c, d, mine, sa, sb, sc, sd, sm, send, kept in self.ways:
            def ready(q):
                pltpu.make_async_copy(mine.at[q], mine.at[q], sm.at[q]).wait()
                each(TWO, lambda i: remote(b.at[i, q], b.at[i, q], send, sb.at[i, q], p.near(1)).wait_recv())

            each(TWO, ready)

            def quarter(q):
                s = -lower_upper(q)

                def term(k, j, to, sem):
                    self.add(b.at[0, k, j], mine.at[k, j], b.at[0, k, j], b.at[1, k, j])
                    remote(b.at[0, k, j], to, send, sem, p.near(0, s)).start()

                term(q, 2, c.at[q], sc.at[q])
                term(1 - q, 1 + 2 * q, d.at[q, 1 - q], sd.at[q, 1 - q])

            each(TWO, quarter)

    def go3(self):
        for p, h, a, b, c, d, mine, sa, sb, sc, sd, sm, send, kept in self.ways:
            def quarter(q):
                s, j = -lower_upper(q), 1 + 2 * q
                remote(c.at[q], c.at[q], send, sc.at[q], p.near(0, s)).wait_recv()
                self.add(c.at[q], c.at[q], mine.at[q, j], b.at[0, q, j], b.at[1, q, j])
                remote(c.at[q], d.at[q, q], send, sd.at[q, q], p.near(0, s)).start()

            each(TWO, quarter)

    def go4(self):
        for p, h, a, b, c, d, mine, sa, sb, sc, sd, sm, send, kept in self.ways:
            def quarter(q):
                each(TWO, lambda i: remote(d.at[i, q], d.at[i, q], send, sd.at[i, q], p.near(1)).wait_recv())
                own = mine.at[q, 0]
                self.add(own, own, b.at[0, q, 0], b.at[1, q, 0], d.at[0, q], d.at[1, q])

                w = self.step

                def some(i, _):
                    x = own[:, pl.ds(pl.multiple_of(i * w, HEAD), w)].astype(F32)
                    self.squares[...] += tiles(x * x)

                lax.fori_loop(0, self.chunk[1] // w, some, None)
                pltpu.make_async_copy(own, self.part(self.out, 0, len(TWO) * h + q), kept).start()

            each(TWO, quarter)

    def end(self):
        for p, h, a, b, c, d, mine, sa, sb, sc, sd, sm, send, kept in self.ways:
            for x in (a, b, c, mine.at[0]):
                remote(x, x, send, sa.at[0], p.near(1)).wait_send()
            pltpu.make_async_copy(c, c, kept).wait()
        if not self.again:
            for d in self.ways[0][0].around():
                pl.semaphore_signal(self.free, device_id=d, device_id_type=MESH)


def then(*steps):
    def do():
        for step in steps:
            step()

    return do


def when(*events):
    def tick(i):
        for place, do in events:
            pl.when(i == place)(do)

    return tick


def dot(a, b, ca, cb):
    return lax.dot_general(a, b, (((ca,), (cb,)), ((), ())), preferred_element_type=F32)


def nn(a, b):
    return dot(a, b, 1, 0)


def nt(a, b):
    return dot(a, b, 1, 1)


def row(i):
    return i, 0


def col(j):
    return 0, j


def whole(*_):
    return 0, 0


def run(body, grid, ins, outs, scratch=(), tick=None):
    held = [(r, late) for r, block, late in ins if block is None]
    tiled = [x for x in ins if x[1] is not None]

    def inner(sem, *refs):
        full, rest = refs[: len(held)], refs[len(held) :]
        copies = [(k, pltpu.make_async_copy(r, v, sem.at[i])) for i, ((r, k), v) in enumerate(zip(held, full))]
        for k, c in copies:
            if k is None:
                c.start()

        def step(*tiles):
            for at in sorted({k or 0 for k, _ in copies} | ({grid[0] - 1} if any(k for k, _ in copies) else set())):
                @pl.when(functools.reduce(lambda p, q: p & q, [pl.program_id(i) == (at if i == 0 else 0) for i in range(len(grid))]))
                def _():
                    for k, c in copies:
                        if k == at and k is not None:
                            c.start()
                    for k, c in copies:
                        if (at == 0 and k is None) or (at == grid[0] - 1 and k is not None):
                            c.wait()

            some, more, given = iter(tiles), iter(full), []
            for _, block, _ in ins:
                given.append(next(more) if block is None else next(some))
            body(*given, *some, *rest, tick or (lambda i: None))

        specs = lambda arrays: [pl.BlockSpec(r.shape, whole, pipeline_mode=pl.Buffered(1)) if block is None else pl.BlockSpec(block, at) for r, block, at in arrays]
        pltpu.emit_pipeline(step, grid=grid, in_specs=specs(tiled), out_specs=specs(outs))(*[r for r, _, _ in tiled], *[r for r, _, _ in outs])

    pl.run_scoped(inner, pltpu.SemaphoreType.DMA((max(len(held), 1),)), *[pltpu.VMEM(r.shape, r.dtype) for r, _ in held], *scratch)


def all_of(ref):
    return ref, None, None


def rows_of(ref):
    return ref, (ROWS, ref.shape[1]), row


def cols_of(ref, parts):
    return ref, (ref.shape[0], ref.shape[1] // parts), col


def in_rows(size, body, tick):
    n = size // MORE

    def one(i, _):
        body(pl.ds(pl.multiple_of(i * MORE, MORE), MORE))
        tick(pl.program_id(0) * n + i)

    lax.fori_loop(0, n, one, None)


def unit(h):
    return lax.rsqrt(jnp.mean(h * h, -1, keepdims=True) + 1e-6)


def normed(h):
    h = h.astype(F32)
    return (h * unit(h)).astype(BF)


def norm_back(h, d):
    h = h.astype(F32)
    s = unit(h)
    return (s * d - h * (s * s * s * jnp.mean(h * d, -1, keepdims=True))).astype(BF)


def rotary(tokens):
    half = HEAD // 2
    angle = np.arange(tokens, dtype=F32)[:, None] * np.power(np.float32(THETA), -np.arange(half, dtype=F32) / half)
    c, s = np.cos(angle), np.sin(angle)
    return jnp.asarray(np.concatenate([c, c], 1)), jnp.asarray(np.concatenate([-s, s], 1))


def heads_of(ref, g):
    return [ref[:, n * HEAD : (n + 1) * HEAD] for n in range(g)]


def in_tiles(size, body, tick):
    def one(i, _):
        body(pl.ds(pl.multiple_of(i * ROWS, ROWS), ROWS))
        tick(i)

    lax.fori_loop(0, size // ROWS, one, None)


def qkv(h, w, cos, sin, kv, a, x, tick):
    turned = w.shape[1] // HEAD - kv

    def tile(at):
        t = normed(h[at, :])
        a[at, :] = t
        r = nn(t, w[...]).astype(BF)
        for n in range(r.shape[1] // HEAD):
            cols = slice(n * HEAD, (n + 1) * HEAD)
            t = r[:, cols]
            if n < turned:
                t = t.astype(F32)
                t = (t * cos[at, :] + pltpu.roll(t, HEAD // 2, 1) * sin[at, :]).astype(BF)
            x[at, cols] = t

    in_tiles(h.shape[0], tile, tick)


def out_proj(h, o, w, m, b, tick):
    def tile(at):
        t = h[at, :] + nn(o[at, :], w[...]).astype(BF)
        m[at, :] = t
        b[at, :] = normed(t)

    in_tiles(h.shape[0], tile, tick)


def up_to(parts):
    return lambda j: (0, lax.min(j, parts - 1))


def cols_then(ref, parts):
    return ref, (ref.shape[0], ref.shape[1] // parts), up_to(parts)


def gu_body(w_ref, wd_ref, g_ref, mid_s, tick, *, b, m, h):
    half = w_ref.shape[1] // 2
    j = pl.program_id(0)
    end = pl.num_programs(0) - 1

    @pl.when(j < end)
    def _():
        def tile(at):
            r = nn(b[at, :], w_ref[...])
            g_ref[at, :] = r
            g = r[:, :half]
            mid_s[j, at, :] = (g * jax.nn.sigmoid(g) * r[:, half:]).astype(BF)

        in_rows(b.shape[0], tile, tick)

    @pl.when(j == end)
    def _():
        def tile(at):
            h[at, :] = m[at, :] + nn(jnp.concatenate([mid_s[i, at, :] for i in range(PARTS)], 1), wd_ref[...]).astype(BF)

        in_rows(b.shape[0], tile, tick)


def mlp(b, w, m, wd, gu, h, late, tick):
    run(functools.partial(gu_body, b=b, m=m, h=h), (PARTS + 1,), [cols_then(w, PARTS), (wd, None, late)], [cols_then(gu, PARTS)],
        [pltpu.VMEM((PARTS, b.shape[0], w.shape[1] // PARTS // 2), BF)], tick)


def visible(iq, j, bq, bk):
    return lax.broadcasted_iota(jnp.int32, (bk, bq), 1) - lax.broadcasted_iota(jnp.int32, (bk, bq), 0) >= j * bk - iq * bq


def key_blocks(c, iq, blocks, block, tick):
    before = c * (blocks * (blocks + 1) // 2) + lax.div(iq * (iq + 1), 2)

    def seen(j, _):
        @pl.when(j <= iq)
        def _():
            block(j)
            tick(before + j)

    lax.fori_loop(0, blocks, seen, None)


def attend(x, kv, o, lse, top_s, mix_s, tick, bq=MORE):
    t, n = x.shape
    heads = n // HEAD - 2 * kv
    g = heads // kv
    scale = HEAD**-0.5
    e = scale * LOG2E
    ones = jnp.ones((8, bq), BF)

    def one(step, _):
        c, iq = lax.div(step, t // bq), lax.rem(step, t // bq)
        cols = lambda at: pl.ds(pl.multiple_of(at * HEAD, HEAD), HEAD)
        rows = lambda i: pl.ds(pl.multiple_of(i * bq, bq), bq)
        top_s[...] = jnp.full(top_s.shape, NEG, F32)
        mix_s[...] = jnp.zeros(mix_s.shape, F32)

        def block(j):
            k = x[rows(j), cols(heads + c)]
            scores = [nt(k, x[rows(iq), cols(c * g + n)]) for n in range(g)]
            values = jnp.concatenate([x[rows(j), cols(heads + kv + c)].T, ones], axis=0)
            weights, keeps = [], []
            for n, s in enumerate(scores):
                s = jnp.where(visible(iq, j, bq, bq), s, 2 * NEG)
                mine = slice(n, n + 1)
                old = top_s[mine, :]
                top = jnp.maximum(old, s.max(axis=0, keepdims=True))
                top_s[mine, :] = top
                weights.append(jnp.exp2((s - top) * e).astype(BF))
                keeps.append(jnp.exp2((old - top) * e))
            for n in range(g):
                mix_s[n] = mix_s[n] * keeps[n] + nn(values, weights[n])

        key_blocks(c, iq, t // bq, block, tick)
        for n in range(g):
            mine = slice(n, n + 1)
            total = mix_s[n, HEAD : HEAD + 1, :]
            o[rows(iq), cols(c * g + n)] = (mix_s[n, :HEAD, :] * (1 / total)).T.astype(BF)
            lse[c, mine, rows(iq)] = top_s[mine, :] * scale + jnp.log(total)

    lax.fori_loop(0, kv * (t // bq), one, None)


def attention_specs(x, kv, bq):
    t, n = x.shape
    heads = n // HEAD - 2 * kv
    g = heads // kv
    return (bq, g * HEAD), [(x, (bq, g * HEAD), lambda c, i: (i, c)), (x, (t, HEAD), lambda c, i: (0, heads + c)), (x, (t, HEAD), lambda c, i: (0, heads + kv + c))], \
        lambda ref: (ref, (1, g, bq), lambda c, i: (c, 0, i))


def bwd_body(q_ref, k_ref, v_ref, do_ref, lse_ref, delta_ref, c_ref, s_ref, dq_s, dk_s, dv_s, tick, *, scale, bk, into):
    bq, g = q_ref.shape[0], q_ref.shape[1] // HEAD
    iq = pl.program_id(1)
    e = scale * LOG2E

    @pl.when(iq == 0)
    def _():
        dk_s[...] = jnp.zeros_like(dk_s)
        dv_s[...] = jnp.zeros_like(dv_s)

    dq_s[...] = jnp.zeros_like(dq_s)

    def block(j):
        here = pl.ds(pl.multiple_of(j * bk, bk), bk)
        k, v = k_ref[here, :], v_ref[here, :]
        back = k.T
        qs, dos = heads_of(q_ref, g), heads_of(do_ref, g)
        scores = [nt(k, x) for x in qs]
        dps = [nt(v, x) for x in dos]
        for n in range(g):
            mine = slice(n, n + 1)
            p = jnp.where(visible(iq, j, bq, bk), jnp.exp2(scores[n] * e - lse_ref[0, mine, :] * LOG2E), 0.0)
            ds = (p * (dps[n] - delta_ref[0, mine, :])).astype(BF)
            dv_s[here, :] += nn(p.astype(BF), dos[n])
            dk_s[here, :] += nn(ds, qs[n])
            dq_s[n] += nn(back, ds)

    key_blocks(pl.program_id(0), iq, k_ref.shape[0] // bq, block, tick)

    def unturned(d, at):
        d = d.astype(BF).astype(F32)
        return (d * c_ref[at, :] - pltpu.roll(d, HEAD // 2, 1) * s_ref[at, :]).astype(BF)

    c = pl.program_id(0)
    heads = pl.num_programs(0)
    q_at = pl.ds(pl.multiple_of(iq * bq, bq), bq)
    cols = lambda at: pl.ds(pl.multiple_of(at * HEAD, HEAD), HEAD)
    for n in range(g):
        into[q_at, cols(c * g + n)] = unturned((dq_s[n] * scale).T, q_at)

    @pl.when(iq == pl.num_programs(1) - 1)
    def _():
        into[:, cols(heads * g + c)] = unturned(dk_s[...] * scale, slice(None))
        into[:, cols(heads * (g + 1) + c)] = dv_s[...].astype(BF)


def attend_back(x, do, lse, delta, cos, sin, kv, into, tick, bq=MORE, bk=MORE):
    tile, ins, stat = attention_specs(x, kv, bq)
    t = x.shape[0]
    run(functools.partial(bwd_body, scale=HEAD**-0.5, bk=bk, into=into), (kv, t // bq), ins + [(do, tile, lambda c, i: (i, c)), stat(lse), stat(delta), all_of(cos), all_of(sin)],
        [], [pltpu.VMEM((tile[1] // HEAD, HEAD, bq), F32)] + [pltpu.VMEM((t, HEAD), F32)] * 2, tick)


def silu_back(g, u, d):
    s = jax.nn.sigmoid(g)
    silu = g * s
    return (silu * u).astype(BF), (d * u * (s + silu * (1 - s))).astype(BF), (d * silu).astype(BF)


def dgu_body(dy_ref, w_ref, g_ref, dg_ref, dw_ref, mid_s, tick):
    half = mid_s.shape[1]

    def tile(at):
        d = nt(dy_ref[at, :], w_ref[...]).astype(BF).astype(F32)
        mid_s[at, :], dg_ref[at, :half], dg_ref[at, half:] = silu_back(g_ref[at, :half], g_ref[at, half:], d)

    in_rows(dy_ref.shape[0], tile, tick)
    dw_ref[...] = dot(mid_s[...], dy_ref[...], 0, 0).astype(BF)


def dgu(dy, wd, gu, dg, dwd, tick):
    t, c = dy.shape[0], wd.shape[0] // PARTS
    rows = lambda ref: (ref, (c, ref.shape[1]), row)
    run(dgu_body, (PARTS,), [all_of(dy), rows(wd), cols_of(gu, PARTS)], [cols_of(dg, PARTS), rows(dwd)], [pltpu.VMEM((t, c), BF)], tick)


def last_body(dy_ref, wd_ref, b_ref, w_ref, dg_ref, dw_ref, mid_s, tick):
    half = mid_s.shape[1]

    def tile(at):
        r = nn(b_ref[at, :], w_ref[...])
        d = nt(dy_ref[at, :], wd_ref[...]).astype(BF).astype(F32)
        mid_s[at, :], dg_ref[at, :half], dg_ref[at, half:] = silu_back(r[:, :half], r[:, half:], d)

    in_rows(dy_ref.shape[0], tile, tick)
    dw_ref[...] = dot(mid_s[...], dy_ref[...], 0, 0).astype(BF)


def last_dgu(dy, wd, b, wgu, dg, dwd, tick):
    t, c = dy.shape[0], wd.shape[0] // PARTS
    rows = lambda ref: (ref, (c, ref.shape[1]), row)
    run(last_body, (PARTS,), [all_of(dy), rows(wd), all_of(b), cols_of(wgu, PARTS)], [cols_of(dg, PARTS), rows(dwd)], [pltpu.VMEM((t, c), BF)], tick)


def dw_body(a_ref, d_ref, o_ref, at_s, tick):
    @pl.when(pl.program_id(0) == 0)
    def _():
        at_s[...] = a_ref[...].T

    def tile(at):
        o_ref[at, :] = nn(at_s[at, :], d_ref[...]).astype(BF)

    in_rows(at_s.shape[0], tile, tick)


def dw(a, d, out, parts, tick):
    run(dw_body, (parts,), [all_of(a), cols_of(d, parts)], [cols_of(out, parts)], [pltpu.VMEM(a.shape[::-1], BF)], tick)


def db_body(dg_ref, w_ref, dy_ref, h_ref, wo_ref, x_ref, dm_ref, do_ref, delta_ref, to_ref, acc, tick):
    j = pl.program_id(0)
    end = pl.num_programs(0) - 1

    @pl.when(j < end)
    def _():
        def tile(at):
            r = nt(dg_ref[at, :], w_ref[...])

            @pl.when(j == 0)
            def _():
                acc[at, :] = r

            @pl.when(j > 0)
            def _():
                acc[at, :] += r

        in_rows(acc.shape[0], tile, tick)

    @pl.when(j == end)
    def _():
        kv, g = delta_ref.shape[:2]

        def tile(at):
            d = dy_ref[at, :] + norm_back(h_ref[at, :], acc[at, :].astype(BF).astype(F32))
            dm_ref[at, :] = d
            r = nt(d, wo_ref[...]).astype(BF)
            do_ref[at, :] = r
            for n in range(kv * g):
                cols = slice(n * HEAD, (n + 1) * HEAD)
                x = r[:, cols].astype(F32) * x_ref[at, cols].astype(F32)
                delta_ref[n // g, n % g : n % g + 1, at] = jnp.sum(x.T, axis=0, keepdims=True)

        in_rows(acc.shape[0], tile, tick)

        def term(i, _):
            at = pl.ds(pl.multiple_of(i * ROWS, ROWS), ROWS)
            to_ref[at, :] = nn(x_ref[:, at].T, dm_ref[...]).astype(BF)

        lax.fori_loop(0, to_ref.shape[0] // ROWS, term, None)


def db(dg, wgu, dy, h, wo, x, dm, do, delta, to, tick):
    late = lambda ref: (ref, None, 1)
    run(db_body, (PARTS + 1,), [cols_then(dg, PARTS), cols_then(wgu, PARTS), late(dy), late(h), late(wo), late(x)], [all_of(dm), all_of(do), all_of(delta), all_of(to)],
        [pltpu.VMEM(dy.shape, F32)], tick)


def da_body(d_ref, h_ref, o_ref, tick, *, dx, w):
    i = pl.program_id(0)
    r = nt(dx[pl.ds(pl.multiple_of(i * ROWS, ROWS), ROWS), :], w[...])
    o_ref[...] = d_ref[...] + norm_back(h_ref[...], r.astype(BF).astype(F32))
    tick(i)


def da(dx, w, d, h, out, tick):
    run(functools.partial(da_body, dx=dx, w=w), (d.shape[0] // ROWS,), [rows_of(d), rows_of(h)], [rows_of(out)], tick=tick)


def dqkv_body(o_ref, tick, *, dx, a):
    i = pl.program_id(0)
    o_ref[...] = nn(a[:, pl.ds(pl.multiple_of(i * ROWS, ROWS), ROWS)].T, dx[...]).astype(BF)
    tick(i)


def dqkv(a, dx, out, tick):
    run(functools.partial(dqkv_body, dx=dx, a=a), (out.shape[0] // ROWS,), [], [rows_of(out)], tick=tick)


WAYS = ("a", "gu", "d")
SUMS = ("qkv", "o", "gu", "d")
NAMES = ("wq", "wk", "wv", "wo", "w_gate", "w_up", "w_down")


def named(names, refs):
    return dict(zip(names, refs, strict=True))


def beside(r, kw):
    a = r.shape[1]
    q = a // 2 - kw
    return r.at[:, pl.ds(0, a - q)], r.at[:, pl.ds(a - q, q)]


def mixture(f):
    w = f // PARTS
    return [(i, j * w, (2 * j + i) * w, w) for j in range(PARTS) for i in TWO]


def forward_kernel(n, layers, kv, ins, outs, count, *refs):
    r = named(ins + outs, refs[:count])
    packs, refs = refs[count : count + 2], refs[count + 2 :]
    (h, a_s, x_s, o_s, lse_s, m_s, b_s, wqkv_s, wo_s, top_s, mix_s, fetched, out), sems = refs[:13], refs[13:]
    fetch = lambda i, src, dst: pltpu.make_async_copy(src, dst, fetched.at[i])
    first = fetch(0, r["x"].at[0], h)
    first.start()
    def pack():
        for l in range(layers):
            at = 0
            for name in NAMES[:4]:
                w = r[name].shape[2]
                packs[0][l, :, at : at + w] = r[name][l]
                at += w
            for i, a, b, w in mixture(r["w_up"].shape[2]):
                packs[1][l, :, b : b + w] = r[NAMES[4 + i]][l, :, a : a + w]

    place = Place(n, 0)
    greet(place.around() + [place.twin], pack)
    per = len(gather_sems())
    pieces = [[Gather(n, p.at[l], r[f"w{w}{l}"], sems[per * (3 * l + i) : per * (3 * l + i + 1)]) for i, (w, p) in enumerate(zip(WAYS, (*packs, r["w_down"])))]
              for l in range(layers)]
    a, gu, dn = pieces[0]
    then(a.go0, gu.go0, dn.go0, a.go1, a.go2, a.go3, gu.go1, dn.go1, a.go4)()
    kept = dict(zip("axombh", (a_s, x_s, o_s, m_s, b_s, h))) | {"lse": lse_s}
    leave = lambda i, l: pltpu.make_async_copy(kept[i], r[f"{i}{l}"], out.at[list(kept).index(i)])
    first.wait()
    for l in range(layers):
        more = l + 1 < layers
        a, gu, dn = pieces[l]
        wqkv, wo = beside(r[f"wa{l}"], kv * HEAD)
        two = fetch(0, wqkv, wqkv_s), fetch(1, wo, wo_s)
        for c in two:
            c.start()
        if l:
            for i in kept:
                if i != "h":
                    leave(i, l - 1).wait()
        two[0].wait()
        qkv(h, wqkv_s, r["cos"], r["sin"], kv, a_s, x_s, when())
        for i in "ax":
            leave(i, l).start()
        attend(x_s, kv, o_s, lse_s, top_s, mix_s, when((1, gu.go2)) if more else when((0, dn.go2), (2, gu.go2)))
        for i in ("o", "lse"):
            leave(i, l).start()
        two[1].wait()
        out_proj(h, o_s, wo_s, m_s, b_s, when((2, gu.go3) if more else (0, dn.go3)))
        for i in "mb":
            leave(i, l).start()
        if more:
            if l:
                leave("h", l).wait()
            a2, gu2, dn2 = pieces[l + 1]
            then(dn.go2, a2.go0, gu2.go0, dn2.go0, gu.go4)()
            mlp(b_s, r[f"wgu{l}"], m_s, r[f"wd{l}"], r[f"gu{l}"], h, 2,
                when((1, then(dn.go3, a2.go1)), (3, dn.go4), (7, then(a2.go2, dn2.go1)), (2 * PARTS, then(a2.go3, gu2.go1))))
            leave("h", l + 1).start()
            a2.go4()
        else:
            then(gu.go3, dn.go4, gu.go4)()
    for i in kept:
        leave(i, layers - 1).wait()


def backward_kernel(n, layers, kv, ins, outs, count, *refs):
    r = named(ins + outs, refs[:count])
    squares, slots, send, recv = refs[count : count + 4]
    held = refs[count + 4 :]
    place = Place(n, 0)
    others = [{"dp": lax.rem(place.me + i, n)} for i in range(1, n)]
    greet(others)
    squares[...] = jnp.zeros_like(squares)

    per = len(held) // len(SUMS)

    def piece(l, w):
        i = per * SUMS.index(w)
        return Scatter(n, r[f"t{w}{l}"], r[f"g{w}{l}"], squares, held[i : i + per], l + 1 < layers)

    d = r["dy"].at[0]
    before = []
    for l in reversed(range(layers)):
        p, o, gu, dn = (piece(l, w) for w in SUMS)
        if before:
            p1, o1, gu1, dn1 = before
            dgu(d, r[f"wd{l}"], r[f"gu{l}"], r["dg"], r[f"td{l}"],
                when((0, then(dn1.go4, o1.go2)), (2, p1.go1), (5, then(gu1.go4, o1.go3)), (6, p1.go2), (8, then(o1.go4, p1.go3))))
            p1.go4()
        else:
            last_dgu(d, r[f"wd{l}"], r[f"b{l}"], r[f"wgu{l}"], r["dg"], r[f"td{l}"], when())
        wqkv, wo = beside(r[f"wa{l}"], kv * HEAD)
        then(*[q.end for q in before], dn.go0)()
        dw(r[f"b{l}"], r["dg"], r[f"tgu{l}"], PARTS, when((5, dn.go1)))
        gu.go0()
        db(r["dg"], r[f"wgu{l}"], d, r[f"m{l}"], wo, r[f"o{l}"], r["dm"], r["do"], r["delta"], r[f"to{l}"], when((4, dn.go2), (2 * PARTS, gu.go1)))
        o.go0()

        def attention(dx, a, w, sem):
            copies = [pltpu.make_async_copy(x, y, sem.at[i]) for i, (x, y) in enumerate(((r[f"a{l}"], a), (wqkv, w))[: 2 if l else 1])]
            for c in copies:
                c.start()
            attend_back(r[f"x{l}"], r["do"], r[f"lse{l}"], r["delta"], r["cos"], r["sin"], kv, dx, when((3, dn.go3)))
            for c in copies:
                c.wait()
            dqkv(a, dx, r[f"tqkv{l}"], when((2, gu.go2), (3, o.go1)) if l else when())
            p.go0()
            if l:
                da(dx, w, r["dm"], r[f"h{l}"], r[f"d{l}"], when((3, gu.go3)))

        pl.run_scoped(attention, pltpu.VMEM(r[f"x{l}"].shape, BF), pltpu.VMEM(r[f"a{l}"].shape, BF), pltpu.VMEM(wqkv.shape, BF), pltpu.SemaphoreType.DMA((2,)))
        if l:
            d = r[f"d{l}"]
        else:
            then(gu.go2, o.go1, dn.go4, p.go1, gu.go3, o.go2, p.go2, gu.go4, o.go3, p.go3, o.go4, p.go4)()
        before = [p, o, gu, dn]
    then(*[q.end for q in before])()
    copies = [remote(squares, slots.at[i], send.at[i], recv.at[i], p) for i, p in enumerate(others)]
    for c in copies:
        c.start()
    for c in copies:
        c.wait()
    t = squares[...] + sum(slots[i] for i in range(n - 1))
    r["total"][...] = jnp.broadcast_to(jnp.sum(jnp.sum(t, axis=1, keepdims=True), axis=0, keepdims=True), t.shape)


def kernel(body, name, number, given, made, in_vmem, scratch):
    space = lambda name: pl.BlockSpec(memory_space=pltpu.VMEM if name in in_vmem else pl.ANY)
    got = pl.pallas_call(
        functools.partial(body, tuple(given), tuple(made), len(given) + len(made)),
        in_specs=[space(k) for k in given],
        out_specs=[space(k) for k in made],
        out_shape=[jax.ShapeDtypeStruct(*s) for s in made.values()],
        scratch_shapes=scratch,
        compiler_params=pltpu.CompilerParams(collective_id=number, has_side_effects=True, vmem_limit_bytes=VMEM),
        name=name,
    )(*given.values())
    return dict(zip(made, got, strict=True))


def adamw(w, m, v, g):
    m = 0.9 * m + 0.1 * g
    v = 0.95 * v + 0.05 * g * g
    step = m * lax.rsqrt(v + 1e-8) + 0.1 * w
    return (w - 0.02 * step).astype(BF), m, v


def step_kernel(count, layers, total_ref, *refs):
    m, k = len(SUMS), len(NAMES)
    grads, refs = refs[: m * layers], refs[m * layers :]
    olds, news = refs[: 3 * k], refs[3 * k :]
    factor = jnp.minimum(1.0, 0.5 * lax.rsqrt(total_ref[:1, :1] / count + 1e-30))
    for l in range(layers):
        @pl.when(pl.program_id(0) == l)
        def _():
            p, o, gu, d = grads[m * l : m * l + m]
            q, w = olds[0].shape[2], olds[1].shape[2]
            wide = o.shape[1]
            moves = [(0, p, 0, 0, q), (1, p, 0, q, w), (2, p, 0, q + w, w), (3, o, 0, 0, wide), (k - 1, d, 0, 0, wide)]
            for i, g, to, at, w in moves + [(4 + i, gu, to, at, w) for i, to, at, w in mixture(olds[4].shape[2])]:
                def some(c, _):
                    here, there = (pl.ds(pl.multiple_of(x + c * HEAD, HEAD), HEAD) for x in (to, at))
                    three = (i, i + k, i + 2 * k)
                    new = adamw(*[olds[j][0, :, here].astype(F32) for j in three], g[:, there].astype(F32) * factor)
                    for j, x in zip(three, new):
                        news[j][0, :, here] = x

                lax.fori_loop(0, w // HEAD, some, None)


def optimizer(n, total, grads, arrays):
    layers = arrays[0].shape[0]
    tile = lambda a: pl.BlockSpec((1,) + a.shape[1:], lambda l: (l, 0, 0))
    held = pl.BlockSpec(memory_space=pltpu.VMEM)
    return pl.pallas_call(
        functools.partial(step_kernel, n * sum(a.size for a in arrays[:7]), layers),
        grid=(layers,),
        in_specs=[held] * (1 + len(grads)) + [tile(a) for a in arrays],
        out_specs=[tile(a) for a in arrays],
        out_shape=[jax.ShapeDtypeStruct(a.shape, a.dtype) for a in arrays],
        compiler_params=pltpu.CompilerParams(dimension_semantics=("arbitrary",), vmem_limit_bytes=VMEM),
        name="optimizer",
    )(total, *grads, *arrays)


def solution(mesh):
    n = mesh.shape["dp"]

    def step(x, dy, *arrays):
        weights = named(NAMES, arrays[:7])
        layers, _, kw = weights["wk"].shape
        kv = kw // HEAD
        t, d = x.shape[1:]
        q, f = weights["wq"].shape[2], weights["w_up"].shape[2]
        cos, sin = rotary(t)
        shapes = {"a": (d, 2 * q + 2 * kw), "qkv": (d, q + 2 * kw), "o": (q, d), "gu": (d, 2 * f), "d": (f, d)}
        lse, made = (kv, q // kw, t), {}
        for l in range(layers):
            made |= {f"w{w}{l}": (shapes[w], BF) for w in WAYS}
            made |= {f"a{l}": ((t, d), BF), f"x{l}": ((t, q + 2 * kw), BF), f"o{l}": ((t, q), BF), f"lse{l}": (lse, F32),
                     f"m{l}": ((t, d), BF), f"b{l}": ((t, d), BF)}
            if l + 1 < layers:
                made |= {f"gu{l}": ((t, 2 * f), F32), f"h{l + 1}": ((t, d), BF)}
        vm = lambda *shape: pltpu.VMEM(shape, BF)
        shards = [vm(layers, shapes[w][0] // n, shapes[w][1]) for w in WAYS[:2]]
        work = [vm(t, d), vm(t, d), vm(t, q + 2 * kw), vm(t, q), pltpu.VMEM(lse, F32), vm(t, d), vm(t, d), vm(*shapes["qkv"]), vm(*shapes["o"]),
                pltpu.VMEM((8, MORE), F32), pltpu.VMEM((q // kw, HEAD + 8, MORE), F32), pltpu.SemaphoreType.DMA((2,)), pltpu.SemaphoreType.DMA((7,))]
        kept = kernel(functools.partial(forward_kernel, n, layers, kv), "forward", 0, {"x": x, "cos": cos, "sin": sin, **weights}, made, NAMES + ("cos", "sin"),
                      shards + work + gather_sems() * (len(WAYS) * layers))
        given = {"dy": dy, "cos": cos, "sin": sin, **kept}
        made = {"dg": ((t, 2 * f), BF), "do": ((t, q), BF), "delta": (lse, F32), "dm": ((t, d), BF),
                "total": ((8, HEAD), F32)}
        for l in range(layers):
            made |= {f"t{w}{l}": (shapes[w], BF) for w in SUMS} | {f"g{w}{l}": ((shapes[w][0] // n, shapes[w][1]), BF) for w in SUMS} | {f"d{l}": ((t, d), BF)}
        scratch = [pltpu.VMEM((8, HEAD), F32), pltpu.VMEM((n - 1, 8, HEAD), F32)] + [pltpu.SemaphoreType.DMA((n - 1,))] * 2
        got = kernel(functools.partial(backward_kernel, n, layers, kv), "backward", 1, given, made, ["total"], sum([scatter_scratch(n, shapes[w]) for w in SUMS], scratch))
        return tuple(optimizer(n, got["total"], [got[f"g{w}{l}"] for l in range(layers) for w in SUMS], arrays))

    states, cut = P(("rep", "dp"), None, None), P(None, "dp", None)
    return jax.shard_map(step, mesh=mesh, in_specs=(states, states) + (cut,) * 21, out_specs=(P("rep", "dp", None),) * 21, check_vma=False)
```
